128 devices in a mesh: seq: 2 (over z_lo), ctx: 8 (over y, core), exp: 8 (over z_hi, x).
Axes of the slice: x: 4, y: 4, z: 4 (z_hi: 2, z_lo: 2; z = z_hi * 2 + z_lo), core: 2. Of those that a mesh axis runs over, the one named last changes fastest.
Arguments:
- tokens: bfloat16 [2, 8192, 7168], P('seq', ('ctx', 'exp')), may hold values from -8 to 8
- routing: int32 [2, 8192, 8], P('seq', ('ctx', 'exp')), may hold values from 0 to 255, as said below
- router_weight: bfloat16 [7168, 256], replicated, may hold values from -0.0625 to 0.0625
- w_gate: bfloat16 [16, 7168, 2048], P(('seq', 'exp'), None, 'ctx'), may hold values from -0.0625 to 0.0625
- w_up: bfloat16 [16, 7168, 2048], P(('seq', 'exp'), None, 'ctx'), may hold values from -0.0625 to 0.0625
- w_down: bfloat16 [16, 2048, 7168], P(('seq', 'exp'), 'ctx'), may hold values from -0.125 to 0.125
Outputs:
- routed: bfloat16 [2, 8192, 7168], P('seq', ('ctx', 'exp'))
- balance: float32 [2, 256], P('seq')
The draws below stay inside these ranges and needn't reach their ends.
Inputs may be any that keep to these rules, and one draw needn't show every extreme that they name: `routing`: each token names 8 different experts. The rows of one device name any one expert at least 3 and at most 5 times; in every draw one expert below 16 is named exactly 5 times by the rows of every device.
All inputs are finite; a program needn't handle non-finite values.
Results may differ from the reference program's by a relative error of at most 0.014.
Values may be sent and summed in bfloat16 or wider, within the bound.
A program may use at most 128 MiB of HBM per device.

```python
import jax
import jax.numpy as jnp
from jax import lax

D = 7168
FF = 2048
EXPERTS = 256
TOP = 8
TOK_DEV = 128
FLIGHT = 16
SEQS = 2
LENGTH = 8192
CAPACITY = 5
N_SEQ = 2
N_CTX = 8
N_EXP = 8


def draw_tokens(key, part):
    key_jitter, key_direction = jax.random.split(key, 2)
    positions = jnp.arange(LENGTH, dtype=jnp.float32) / (LENGTH - 1)
    direction = jax.random.normal(key_direction, (SEQS, 1, D), jnp.float32)
    jitter_part = jax.random.normal(key_jitter, (SEQS, LENGTH, D), jnp.float32)
    strength = 0.3 + 0.6 * positions
    values = jitter_part + strength[None, :, None] * direction
    return jnp.clip(values, -8.0, 8.0).astype(jnp.bfloat16)


def draw_routing(key, part):
    blocks = SEQS * LENGTH // TOK_DEV
    classes = EXPERTS // TOP
    mean_load = TOK_DEV * TOP // EXPERTS
    reach = mean_load // 4
    key_pick, key_shift, key_order, key_lift, key_perm = jax.random.split(key, 5)
    full_expert = jax.random.randint(key_pick, (), 0, FLIGHT).astype(jnp.int32)
    shifts = jax.random.randint(key_shift, (blocks, classes // 2), -reach, reach + 1).astype(jnp.int32)
    shifts = shifts.at[:, 0].set(reach)
    counts = jnp.stack([mean_load + shifts, mean_load - shifts], axis=2).reshape(blocks, classes)
    bounds = jnp.cumsum(counts, axis=1).astype(jnp.int32)
    ranks = jnp.arange(TOK_DEV, dtype=jnp.int32)
    class_of_rank = jnp.sum((ranks[None, :, None] >= bounds[:, None, :]).astype(jnp.int32), axis=2).astype(jnp.int32)
    orders = jax.vmap(lambda sub: jax.random.permutation(sub, TOK_DEV))(jax.random.split(key_order, blocks)).astype(jnp.int32)
    token_class = jnp.take_along_axis(class_of_rank, orders, axis=1)
    lifts = jax.random.randint(key_lift, (blocks, TOK_DEV), 0, TOP).astype(jnp.int32)
    base = token_class + classes * lifts
    perms = jax.vmap(lambda sub: jax.random.permutation(sub, EXPERTS))(jax.random.split(key_perm, blocks)).astype(jnp.int32)
    where_full = jnp.argmax(perms == full_expert, axis=1).astype(jnp.int32)
    first_entry = perms[:, 0]
    positions = jnp.arange(EXPERTS, dtype=jnp.int32)[None, :]
    perms = jnp.where(positions == 0, full_expert, jnp.where(positions == where_full[:, None], first_entry[:, None], perms))
    offsets = jnp.arange(TOP, dtype=jnp.int32) * classes
    picks = (base[:, :, None] + offsets[None, None, :]) % EXPERTS
    chosen = jnp.take_along_axis(perms, picks.reshape(blocks, TOK_DEV * TOP), axis=1)
    return chosen.reshape(SEQS, LENGTH, TOP).astype(jnp.int32)


def block_scale(stream_key, dims, cuts, low, top_value):
    def one(position, shards_of):
        steps = jax.random.uniform(jax.random.fold_in(jax.random.fold_in(stream_key, 6), position), (shards_of,), jnp.float32, low / len(cuts), top_value / len(cuts))
        return jnp.repeat(jnp.exp(steps), dims[position] // shards_of).reshape((-1,) + (1,) * (len(dims) - position - 1))

    factor_of = one(*cuts[0])
    for cut in cuts[1:]:
        factor_of = factor_of * one(*cut)
    return factor_of


def scatter_about(stream_key, shape, width, most, shards=(), kind=jnp.bfloat16):
    factor_of = block_scale(stream_key, shape, shards, -0.22, 0.18) if shards else 1.0
    drawn = jax.random.normal(stream_key, shape, jnp.float32) * width * factor_of
    return jnp.minimum(jnp.maximum(drawn, -most), most).astype(kind)


def setup_inputs(seed: int = 0) -> dict:
    splits = jax.random.split(jax.random.key(seed), 7)
    tokens = draw_tokens(jax.random.fold_in(splits[6], 71), 0)
    routing = draw_routing(jax.random.fold_in(splits[6], 71), 0)
    router_weight = scatter_about(splits[2], (D, EXPERTS), D ** -0.5, 0.0625)
    w_gate = scatter_about(splits[3], (FLIGHT, D, FF), D ** -0.5, 0.0625, ((0, 16), (2, 8)))
    w_up = scatter_about(splits[4], (FLIGHT, D, FF), D ** -0.5, 0.0625, ((0, 16), (2, 8)))
    w_down = scatter_about(splits[5], (FLIGHT, FF, D), FF ** -0.5, 0.125, ((0, 16), (1, 8)))
    return dict(tokens=tokens, routing=routing, router_weight=router_weight, w_gate=w_gate, w_up=w_up, w_down=w_down)


route_scale = 2.5


def expert_block(row_block, gate_weight, up_weight, down_weight):
    gate_proj = jnp.dot(row_block, gate_weight, preferred_element_type=jnp.float32)
    up_proj = jnp.dot(row_block, up_weight, preferred_element_type=jnp.float32)
    hidden = (jax.nn.silu(gate_proj) * up_proj).astype(jnp.bfloat16)
    block_width = FF // N_CTX
    combined = jnp.zeros((row_block.shape[0], D), jnp.float32)
    for column in range(N_CTX):
        lower = column * block_width
        partial_value = jnp.dot(hidden[:, lower:lower + block_width], down_weight[lower:lower + block_width], preferred_element_type=jnp.float32)
        rounded = lax.optimization_barrier(partial_value.astype(jnp.bfloat16))
        combined = combined + rounded.astype(jnp.float32)
    return combined.astype(jnp.bfloat16)


def reference(tokens, routing, router_weight, w_gate, w_up, w_down):
    flight = N_SEQ * N_EXP
    blocks = SEQS * LENGTH // TOK_DEV
    per_block = TOK_DEV * TOP
    flat_tokens = tokens.reshape(SEQS * LENGTH, D)
    routes = routing.reshape(SEQS * LENGTH, TOP)
    logits = jnp.dot(flat_tokens, router_weight, preferred_element_type=jnp.float32)
    scores = jax.nn.sigmoid(logits)
    affinity = scores / jnp.sum(scores, axis=1, keepdims=True)
    picked = jnp.take_along_axis(scores, routes, axis=1)
    gate_weights = picked / jnp.sum(picked, axis=1, keepdims=True) * route_scale
    prob_sum = jnp.sum(affinity.reshape(SEQS, LENGTH, EXPERTS), axis=1)
    seq_of_row = (jnp.arange(SEQS * LENGTH, dtype=jnp.int32) // LENGTH)[:, None]
    load = jnp.zeros((SEQS, EXPERTS), jnp.float32).at[jnp.broadcast_to(seq_of_row, routes.shape), routes].add(1.0)
    balance = load * (EXPERTS / (TOP * LENGTH)) * (prob_sum / LENGTH) * EXPERTS

    block_routes = routes.reshape(blocks, per_block)
    expert_iota = jnp.arange(flight, dtype=jnp.int32)[None, None, :]
    onehot = (block_routes[:, :, None] == expert_iota).astype(jnp.int32)
    slot_rank = jnp.sum((jnp.cumsum(onehot, axis=1) - onehot) * onehot, axis=2)
    is_live = block_routes < flight
    block_ids = jnp.arange(blocks, dtype=jnp.int32)[:, None]
    row_index = block_routes * (blocks * CAPACITY) + block_ids * CAPACITY + slot_rank
    spare = flight * blocks * CAPACITY
    target = jnp.where(is_live, row_index, spare)
    owner = block_ids * TOK_DEV + jnp.arange(per_block, dtype=jnp.int32)[None, :] // TOP
    source_row = jnp.zeros((spare + 1,), jnp.int32).at[target.reshape(-1)].set(owner.reshape(-1))
    filled = jnp.zeros((spare + 1,), jnp.int32).at[target.reshape(-1)].set(1)
    source_row = source_row[:spare].reshape(flight, blocks * CAPACITY)
    filled = filled[:spare].reshape(flight, blocks * CAPACITY)

    def one_expert(inputs):
        rows_of, filled_of, gate_weight, up_weight, down_weight = inputs
        row_block = jnp.where(filled_of[:, None] > 0, flat_tokens[rows_of], jnp.zeros((), flat_tokens.dtype))
        return expert_block(row_block, gate_weight, up_weight, down_weight)

    expert_out = lax.map(one_expert, (source_row, filled, w_gate, w_up, w_down))
    expert_out = expert_out.reshape(spare, D)
    live_gates = jnp.where(is_live, gate_weights.reshape(blocks, per_block), 0.0).reshape(SEQS * LENGTH, TOP)
    gather_index = jnp.where(is_live, row_index, 0).reshape(SEQS * LENGTH, TOP)
    combined = jnp.zeros((SEQS * LENGTH, D), jnp.float32)
    for column in range(TOP):
        combined = combined + live_gates[:, column:column + 1] * expert_out[gather_index[:, column]]
    routed = combined.astype(jnp.bfloat16).reshape(SEQS, LENGTH, D)
    return routed, balance
```

```python
import jax
import jax.numpy as jnp
from jax import lax
from jax.experimental import pallas as pl
from jax.experimental.pallas import tpu as pltpu
from jax.sharding import PartitionSpec as P

MESH = pl.DeviceIdType.MESH
F32 = jnp.float32
BF16 = jnp.bfloat16

TOKS = 128
D = 7168
EXPERTS = 256
TOP = 8
FLIGHT = 16
CAP = 5
PAD = 8
HID = 256
ROWS = FLIGHT * CAP
LENGTH = 8192
HALF = D // 2

NC, C = 7, 1024
NM, CM = 7, 512
LEAD = 2


def dot(a, b):
    return jnp.dot(a, b, preferred_element_type=F32)


def iota(shape, dim):
    return lax.broadcasted_iota(jnp.int32, shape, dim)


def kernel(
    tok_h, routes_ref, rw_h, wg_h, wu_h, wd_h,
    out_h, bal_ref,
    tok, rw, wg, wu, wd, disp, sel, exd, ghi, glo, logits,
    asend, arecv, xb, accg, accu, hb,
    t3, t2, t1, s1, s2, f1, f2, rsend, rrecv, outb,
    sta, str_, stb,
    load_sem, out_sem, wdx_sem, a_send, a_recv, g_send, g1, g2, g3a, g3b, gd,
    h_sem, b_send, b_s1, b_s2, b_f1, b_f2, r_send, r_recv, sta_send, sta_recv, stb_send, stb_recv,
):
    s = lax.axis_index("seq")
    cx = lax.axis_index("ctx")
    ex = lax.axis_index("exp")
    core = lax.rem(cx, 2)
    other = 1 - core
    y = lax.div(cx, 2)
    zh = lax.div(ex, 4)
    xx = lax.rem(ex, 4)
    me = s * 8 + ex

    def at_y(step, which=None):
        return (s, lax.rem(y + step, 4) * 2 + (core if which is None else which), ex)

    up, down, far = at_y(1), at_y(3), at_y(2)
    peer = (s, y * 2 + other, ex)

    plane = []
    for dx in range(4):
        for dh in range(2):
            for dl in range(2):
                ps = lax.rem(s + dl, 2)
                pe = lax.rem(zh + dh, 2) * 4 + lax.rem(xx + dx, 4)
                plane.append((ps, pe, ps * 8 + pe))

    def rcopy(src, dst, ssem, rsem, dev):
        return pltpu.make_async_remote_copy(
            src_ref=src, dst_ref=dst, send_sem=ssem, recv_sem=rsem, device_id=dev, device_id_type=MESH
        )

    def load(src, dst, k):
        return pltpu.make_async_copy(src, dst, load_sem.at[k])

    mine = pl.ds(pl.multiple_of(core * HALF, 128), HALF)
    theirs = pl.ds(pl.multiple_of(other * HALF, 128), HALF)
    loads = [
        load(tok_h, tok, 0),
        load(rw_h, rw, 1),
        load(wg_h, wg, 2),
        load(wu_h, wu, 3),
        load(wd_h.at[:, mine], wd.at[core], 4),
    ]
    for cp in loads:
        cp.start()

    barrier = pltpu.get_barrier_semaphore()
    friends = [(ps, y * 2 + core, pe) for ps, pe, _ in plane[1:]]
    friends += [(ps, y * 2 + other, pe) for ps, pe, _ in plane]
    friends += [up, down, far]
    for dev in friends:
        pl.semaphore_signal(barrier, inc=1, device_id=dev, device_id_type=MESH)

    routes = routes_ref[...]
    lane = iota((TOKS, TOKS), 1)
    sub = iota((TOKS, TOKS), 0)
    hit = jnp.zeros((TOKS, TOKS), F32)
    for k in range(TOP):
        hit = hit + jnp.where(routes[:, k : k + 1] == (lane >> 3), 1.0, 0.0)
    before = jnp.where(lane < sub, 1.0, 0.0).astype(BF16)
    rank = dot(before, hit.astype(BF16))
    place = jnp.where(rank == (lane & 7).astype(F32), hit, 0.0)
    ghi[...] = place.astype(BF16)
    disp[...] = place.T.astype(BF16)
    si, sl = iota((ROWS, TOKS), 0), iota((ROWS, TOKS), 1)
    sel[...] = jnp.where((si == (sl >> 3) * CAP + (sl & 7)) & ((sl & 7) < CAP), 1.0, 0.0).astype(BF16)
    ei, el = iota((TOKS, ROWS), 1), iota((TOKS, ROWS), 0)
    exd[...] = jnp.where((ei == (el >> 3) * CAP + (el & 7)) & ((el & 7) < CAP), 1.0, 0.0).astype(BF16)
    logits[...] = jnp.zeros_like(logits)
    accg[...] = jnp.zeros_like(accg)
    accu[...] = jnp.zeros_like(accu)

    pl.semaphore_wait(barrier, len(friends))
    wdx = rcopy(wd_h.at[:, theirs], wd.at[core], wdx_sem.at[0], wdx_sem.at[1], peer)
    wdx.start()
    loads[0].wait()

    def a_copy(j, i):
        ps, pe, pm = plane[i]
        return rcopy(asend.at[j, pm], arecv.at[j, me], a_send.at[j], a_recv.at[j], (ps, cx, pe))

    def dispatch(j, carry):
        cols = pl.ds(pl.multiple_of(j * C, 128), C)
        rows = dot(disp[...], tok[:, cols])
        asend[j] = rows.reshape(FLIGHT, PAD, C).astype(BF16)
        for i in range(1, 16):
            a_copy(j, i).start()
        arecv[j, me] = asend[j, me]
        return carry

    lax.fori_loop(0, NC, dispatch, 0)
    for cp in loads[1:4]:
        cp.wait()

    def a_wait(j):
        w = rcopy(asend.at[j, pl.ds(0, 15)], arecv.at[j, pl.ds(0, 15)], a_send.at[j], a_recv.at[j], peer)
        w.wait_recv()

    hc = C // 2

    def g_own_up(j):
        return rcopy(xb.at[j, core], xb.at[j, 2 + core], g_send.at[0, j], g1.at[j], up)

    def g_own_down(j):
        return rcopy(xb.at[j, core], xb.at[j, 4 + core], g_send.at[1, j], g2.at[j], down)

    def g_far_up(j):
        return rcopy(
            xb.at[j, 2 + core, :, pl.ds(0, hc)], xb.at[j, 6 + core, :, pl.ds(0, hc)], g_send.at[2, j], g3a.at[j], up
        )

    def g_far_down(j):
        return rcopy(
            xb.at[j, 4 + core, :, pl.ds(hc, hc)], xb.at[j, 6 + core, :, pl.ds(hc, hc)], g_send.at[3, j], g3b.at[j], down
        )

    def g_peer(j, rel):
        return rcopy(
            xb.at[j, 2 * rel + core], xb.at[j, 2 * rel + core], g_send.at[4 + rel, j], gd.at[rel, j], peer
        )

    def g_peer_wait(j, rel):
        rcopy(
            xb.at[j, 2 * rel + core], xb.at[j, 2 * rel + other], g_send.at[4 + rel, j], gd.at[rel, j], peer
        ).wait_recv()

    def gather(i, carry):
        @pl.when(i < NC)
        def _():
            j = i
            a_wait(j)
            got = arecv[j].astype(F32).reshape(TOKS, C).astype(BF16)
            xb[j, core] = dot(sel[...], got).astype(BF16)
            g_own_up(j).start()
            g_own_down(j).start()
            g_peer(j, 0).start()
            cols = pl.ds(pl.multiple_of(j * C, 128), C)
            logits[...] += dot(tok[:, cols], rw[cols, :])

        @pl.when(i >= 3)
        def _():
            j = i - 3
            for rel in range(4):
                g_peer_wait(j, rel)
            rows = pl.ds(pl.multiple_of(j * C, 128), C)
            for rel in range(4):
                at = slice(rel * 2 * ROWS, (rel + 1) * 2 * ROWS)
                v = xb[j, 2 * rel : 2 * rel + 2].reshape(2 * ROWS, C)
                accg[at, :] += dot(v, wg[rows, :])
                accu[at, :] += dot(v, wu[rows, :])

        @pl.when((i >= 1) & (i < NC + 1))
        def _():
            j = i - 1
            g_own_up(j).wait_recv()
            g_far_up(j).start()
            g_peer(j, 1).start()
            g_own_down(j).wait_recv()
            g_far_down(j).start()
            g_peer(j, 2).start()

        @pl.when((i >= 2) & (i < NC + 2))
        def _():
            j = i - 2
            g_far_up(j).wait_recv()
            g_far_down(j).wait_recv()
            g_peer(j, 3).start()

        return carry

    lax.fori_loop(0, NC + 3, gather, 0)

    gate = accg[...]
    hb[core] = (gate * jax.nn.sigmoid(gate) * accu[...]).astype(BF16)
    hx = rcopy(hb.at[core], hb.at[core], h_sem.at[0], h_sem.at[1], peer)
    hx.start()
    loads[4].wait()
    wdx.wait_recv()
    rcopy(hb.at[core], hb.at[other], h_sem.at[0], h_sem.at[1], peer).wait_recv()

    hm = CM // 2

    def down_rows(rel, cols):
        at = slice(rel * 2 * ROWS, (rel + 1) * 2 * ROWS)
        return dot(hb[0, at, :], wd[0, :, cols]) + dot(hb[1, at, :], wd[1, :, cols])

    def b_far_up(m):
        return rcopy(t3.at[m, 0], s1.at[m], b_send.at[0, m], b_s1.at[m], up)

    def b_far_down(m):
        return rcopy(t3.at[m, 1], s2.at[m], b_send.at[1, m], b_s2.at[m], down)

    def b_up(m):
        return rcopy(t2.at[m], f1.at[m], b_send.at[2, m], b_f1.at[m], up)

    def b_down(m):
        return rcopy(t1.at[m], f2.at[m], b_send.at[3, m], b_f2.at[m], down)

    def r_copy(m, rel, i):
        ps, pe, pm = plane[i]
        cc = core if rel == 0 else other
        return rcopy(
            rsend.at[m, cc, pm], rrecv.at[core * NM + m, me], r_send.at[rel, m], r_recv.at[core * NM + m], (ps, y * 2 + cc, pe)
        )

    def out_copy(half, m):
        cols = pl.ds(pl.multiple_of(half * HALF + m * CM, 128), CM)
        return pltpu.make_async_copy(outb.at[:, cols], out_h.at[:, cols], out_sem.at[half, m])

    def st_a(i, rel):
        ps, pe, pm = plane[i]
        cc = core if rel == 0 else other
        return rcopy(sta.at[0], str_.at[core * 16 + me], sta_send, sta_recv, (ps, y * 2 + cc, pe))

    def st_b(dev):
        return rcopy(sta.at[1], stb.at[y], stb_send, stb_recv, dev)

    def statistics():
        scores = jax.nn.sigmoid(logits[...])
        eye = iota((TOKS, EXPERTS), 1)
        named = jnp.zeros((TOKS, EXPERTS), F32)
        for k in range(TOP):
            named = named + jnp.where(routes_ref[:, k : k + 1] == eye, 1.0, 0.0)
        affinity = scores / jnp.sum(scores, axis=1, keepdims=True)
        sta[0, 0:1, :] = jnp.sum(affinity, axis=0, keepdims=True)
        sta[0, 1:2, :] = jnp.sum(named, axis=0, keepdims=True)
        total = jnp.sum(jnp.where(named > 0.0, scores, 0.0), axis=1, keepdims=True)
        weights = scores / total * 2.5
        spread = jnp.where(iota((EXPERTS, TOKS), 0) == (iota((EXPERTS, TOKS), 1) >> 3), 1.0, 0.0)
        wide = jnp.dot(weights, spread, preferred_element_type=F32, precision=lax.Precision.HIGHEST)
        g = jnp.where(ghi[...].astype(F32) > 0.0, wide, 0.0)
        hi = g.astype(BF16)
        ghi[...] = hi
        glo[...] = (g - hi.astype(F32)).astype(BF16)
        for rel in range(2):
            for i in range(16):
                if plane_same_seq(i) and (rel, i) != (0, 0):
                    st_a(i, rel).start()

    def plane_same_seq(i):
        return i % 2 == 0

    def statistics_next():
        rcopy(str_.at[pl.ds(0, 15)], str_.at[pl.ds(0, 15)], sta_send, sta_recv, peer).wait_recv()
        str_[core * 16 + me] = sta[0]
        acc = jnp.zeros((2, EXPERTS), F32)
        for cc in range(2):
            for e in range(8):
                acc = acc + str_[cc * 16 + s * 8 + e]
        sta[1] = acc
        stb[y] = acc
        for dev in (up, down, far):
            st_b(dev).start()

    def backward(i, carry):
        @pl.when(i < NM)
        def _():
            m = i
            cols = pl.ds(pl.multiple_of(m * CM, 128), CM)
            v = down_rows(3, cols).astype(BF16)
            t3[m, 0] = v[:, :hm]
            t3[m, 1] = v[:, hm:]
            b_far_up(m).start()
            b_far_down(m).start()

        @pl.when((i >= LEAD) & (i < NM + LEAD))
        def _():
            m = i - LEAD
            cols = pl.ds(pl.multiple_of(m * CM, 128), CM)
            v = down_rows(2, cols)
            b_far_up(m).wait_recv()
            t2[m, :, :hm] = (v[:, :hm] + s1[m].astype(F32)).astype(BF16)
            t2[m, :, hm:] = v[:, hm:].astype(BF16)
            b_up(m).start()
            v = down_rows(1, cols)
            b_far_down(m).wait_recv()
            t1[m, :, :hm] = v[:, :hm].astype(BF16)
            t1[m, :, hm:] = (v[:, hm:] + s2[m].astype(F32)).astype(BF16)
            b_down(m).start()

        @pl.when(i == LEAD)
        def _():
            statistics()

        @pl.when(i == NM)
        def _():
            statistics_next()

        @pl.when((i >= LEAD + 1) & (i < NM + LEAD + 1))
        def _():
            m = i - LEAD - 1
            cols = pl.ds(pl.multiple_of(m * CM, 128), CM)
            v = down_rows(0, cols)
            b_up(m).wait_recv()
            b_down(m).wait_recv()
            v = (v + f1[m].astype(F32) + f2[m].astype(F32)).astype(BF16)
            for cc in range(2):
                w = dot(exd[...], v[cc * ROWS : (cc + 1) * ROWS, :])
                rsend[m, cc] = w.reshape(FLIGHT, PAD, CM).astype(BF16)
            for i2 in range(16):
                for rel in range(2):
                    if (rel, i2) != (0, 0):
                        r_copy(m, rel, i2).start()
            rrecv[core * NM + m, me] = rsend[m, core, me]

        @pl.when(i >= LEAD + 3)
        def _():
            m = i - LEAD - 3
            a, b = core * NM + m, other * NM + m
            rcopy(
                rrecv.at[a, pl.ds(0, 15)], rrecv.at[a, pl.ds(0, 15)], r_send.at[0, m], r_recv.at[a], peer
            ).wait_recv()
            rcopy(rrecv.at[b], rrecv.at[b], r_send.at[1, m], r_recv.at[b], peer).wait_recv()
            for half in range(2):
                v = rrecv[half * NM + m].astype(F32).reshape(TOKS, CM).astype(BF16)
                cols = pl.ds(pl.multiple_of(half * HALF + m * CM, 128), CM)
                outb[:, cols] = (dot(ghi[...], v) + dot(glo[...], v)).astype(BF16)
                out_copy(half, m).start()

        return carry

    lax.fori_loop(0, NM + LEAD + 3, backward, 0)

    rcopy(stb.at[pl.ds(0, 3)], stb.at[pl.ds(0, 3)], stb_send, stb_recv, peer).wait_recv()
    tot = stb[0] + stb[1] + stb[2] + stb[3]
    bal_ref[...] = tot[1:2, :] * (EXPERTS / (TOP * LENGTH)) * (tot[0:1, :] / LENGTH) * EXPERTS

    wdx.wait_send()
    hx.wait_send()
    rcopy(str_.at[pl.ds(0, 15)], str_.at[pl.ds(0, 15)], sta_send, sta_recv, peer).wait_send()
    rcopy(stb.at[pl.ds(0, 3)], stb.at[pl.ds(0, 3)], stb_send, stb_recv, peer).wait_send()

    def drain(j, carry):
        rcopy(asend.at[j, pl.ds(0, 15)], arecv.at[j, pl.ds(0, 15)], a_send.at[j], a_recv.at[j], peer).wait_send()
        g_own_up(j).wait_send()
        g_own_down(j).wait_send()
        g_far_up(j).wait_send()
        g_far_down(j).wait_send()
        for rel in range(4):
            g_peer(j, rel).wait_send()
        b_far_up(j).wait_send()
        b_far_down(j).wait_send()
        b_up(j).wait_send()
        b_down(j).wait_send()
        rcopy(rrecv.at[0], rrecv.at[0], r_send.at[1, j], r_recv.at[0], peer).wait_send()
        rcopy(
            rrecv.at[0, pl.ds(0, 15)], rrecv.at[0, pl.ds(0, 15)], r_send.at[0, j], r_recv.at[0], peer
        ).wait_send()
        for half in range(2):
            out_copy(half, j).wait()
        return carry

    lax.fori_loop(0, NM, drain, 0)


def on_device(tokens, routing, router_weight, w_gate, w_up, w_down):
    any_ = pl.BlockSpec(memory_space=pl.ANY)
    vmem = pl.BlockSpec(memory_space=pltpu.VMEM)
    V = pltpu.VMEM
    dma = pltpu.SemaphoreType.DMA
    out, bal = pl.pallas_call(
        kernel,
        out_shape=(
            jax.ShapeDtypeStruct((TOKS, D), BF16),
            jax.ShapeDtypeStruct((1, EXPERTS), F32),
        ),
        in_specs=[any_, vmem, any_, any_, any_, any_],
        out_specs=(any_, vmem),
        scratch_shapes=[
            V((TOKS, D), BF16),
            V((D, EXPERTS), BF16),
            V((D, HID), BF16),
            V((D, HID), BF16),
            V((2, HID, HALF), BF16),
            V((TOKS, TOKS), BF16),
            V((ROWS, TOKS), BF16),
            V((TOKS, ROWS), BF16),
            V((TOKS, TOKS), BF16),
            V((TOKS, TOKS), BF16),
            V((TOKS, EXPERTS), F32),
            V((NC, FLIGHT, PAD, C), BF16),
            V((NC, FLIGHT, PAD, C), BF16),
            V((NC, 8, ROWS, C), BF16),
            V((8 * ROWS, HID), F32),
            V((8 * ROWS, HID), F32),
            V((2, 8 * ROWS, HID), BF16),
            V((NM, 2, 2 * ROWS, CM // 2), BF16),
            V((NM, 2 * ROWS, CM), BF16),
            V((NM, 2 * ROWS, CM), BF16),
            V((NM, 2 * ROWS, CM // 2), BF16),
            V((NM, 2 * ROWS, CM // 2), BF16),
            V((NM, 2 * ROWS, CM), BF16),
            V((NM, 2 * ROWS, CM), BF16),
            V((NM, 2, FLIGHT, PAD, CM), BF16),
            V((2 * NM, FLIGHT, PAD, CM), BF16),
            V((TOKS, D), BF16),
            V((2, 2, EXPERTS), F32),
            V((32, 2, EXPERTS), F32),
            V((4, 2, EXPERTS), F32),
            dma((5,)),
            dma((2, NM)),
            dma((2,)),
            dma((NC,)),
            dma((NC,)),
            dma((8, NC)),
            dma((NC,)),
            dma((NC,)),
            dma((NC,)),
            dma((NC,)),
            dma((4, NC)),
            dma((2,)),
            dma((4, NM)),
            dma((NM,)),
            dma((NM,)),
            dma((NM,)),
            dma((NM,)),
            dma((2, NM)),
            dma((2 * NM,)),
            dma(()),
            dma(()),
            dma(()),
            dma(()),
        ],
        compiler_params=pltpu.CompilerParams(
            collective_id=0, has_side_effects=True, vmem_limit_bytes=62 * 1024 * 1024
        ),
    )(tokens[0], routing[0], router_weight, w_gate[0], w_up[0], w_down[0])
    return out[None], bal


def solution(mesh):
    placed = (
        P("seq", ("ctx", "exp"), None),
        P("seq", ("ctx", "exp"), None),
        P(),
        P(("seq", "exp"), None, "ctx"),
        P(("seq", "exp"), None, "ctx"),
        P(("seq", "exp"), "ctx", None),
    )
    return jax.shard_map(
        on_device,
        mesh=mesh,
        in_specs=placed,
        out_specs=(P("seq", ("ctx", "exp"), None), P("seq", None)),
        check_vma=False,
    )
```

```python
import jax
import jax.numpy as jnp
from jax import lax
from jax.experimental import pallas as pl
from jax.experimental.pallas import tpu as pltpu
from jax.sharding import PartitionSpec as P

MESH = pl.DeviceIdType.MESH
F32 = jnp.float32
BF16 = jnp.bfloat16

TOKS = 128
D = 7168
EXPERTS = 256
TOP = 8
FLIGHT = 16
CAP = 5
PAD = 8
HID = 256
ROWS = FLIGHT * CAP
LENGTH = 8192
HALF = D // 2

NC, C = 14, 512
NM, CM = 14, 256
NR = 12
NP = NC - NR
MSG = 24
AHEAD = 4
NEAR = 3
LAG = 6
LATE = 6
FIRST = 9
LEAD = 3
SUM = 3
BACK = 9


def dot(a, b):
    return jnp.dot(a, b, preferred_element_type=F32)


def iota(shape, dim):
    return lax.broadcasted_iota(jnp.int32, shape, dim)


def stage(cond, name):
    def wrap(body):
        @pl.when(cond)
        def _():
            with jax.named_scope(name):
                body()

    return wrap


def kernel(
    tok_h, routes_ref, rw_h, wg_h, wu_h, wd_h,
    out_ref, bal_ref,
    tok, rw, wg, wu, wd, disp, sel, exd, pack, unpack, yb, ys, yr, ghi, glo, logits,
    asend, arecv, xb, accg, accu, hb,
    t3, s3, nu, nd, f1, f2, rsend, rrecv,
    sta, str_, stb,
    load_sem, wdx_sem, a_send, a_recv, g_send, g1, g3, gd,
    h_sem, b_send, b_s, b_f, r_send, r_recv, st_send, st_recv, y_send, y1, y3, ym,
):
    s = lax.axis_index("seq")
    cx = lax.axis_index("ctx")
    ex = lax.axis_index("exp")
    core = lax.rem(cx, 2)
    other = 1 - core
    y = lax.div(cx, 2)
    zh = lax.div(ex, 4)
    xx = lax.rem(ex, 4)
    me = s * 8 + ex

    def at_y(step):
        return (s, lax.rem(y + step, 4) * 2 + core, ex)

    up, down, far = at_y(1), at_y(3), at_y(2)
    peer = (s, y * 2 + other, ex)

    plane = []
    for dx in range(4):
        for dh in range(2):
            for dl in range(2):
                ps = lax.rem(s + dl, 2)
                pe = lax.rem(zh + dh, 2) * 4 + lax.rem(xx + dx, 4)
                plane.append((ps, pe, ps * 8 + pe))

    def rcopy(src, dst, ssem, rsem, dev):
        return pltpu.make_async_remote_copy(
            src_ref=src, dst_ref=dst, send_sem=ssem, recv_sem=rsem, device_id=dev, device_id_type=MESH
        )

    mine = pl.ds(pl.multiple_of(core * HALF, 128), HALF)
    theirs = pl.ds(pl.multiple_of(other * HALF, 128), HALF)
    pairs = [(tok_h, tok), (rw_h, rw), (wg_h, wg), (wu_h, wu), (wd_h.at[:, mine], wd.at[core])]
    loads = [pltpu.make_async_copy(src, dst, load_sem.at[k]) for k, (src, dst) in enumerate(pairs)]
    for cp in loads:
        cp.start()

    barrier = pltpu.get_barrier_semaphore()
    friends = [(ps, y * 2 + core, pe) for ps, pe, _ in plane[1:]]
    friends += [(ps, y * 2 + other, pe) for ps, pe, _ in plane]
    friends += [up, down, far]
    for dev in friends:
        pl.semaphore_signal(barrier, inc=1, device_id=dev, device_id_type=MESH)

    lane = iota((TOKS, TOKS), 1)
    sub = iota((TOKS, TOKS), 0)
    hit = jnp.zeros((TOKS, TOKS), F32)
    for k in range(TOP):
        hit = hit + jnp.where(routes_ref[k : k + 1, :] == (sub >> 3), 1.0, 0.0)
    before = jnp.where(sub < lane, 1.0, 0.0).astype(BF16)
    rank = dot(hit.astype(BF16), before)
    place = jnp.where(rank == (sub & 7).astype(F32), hit, 0.0)
    disp[...] = place.astype(BF16)
    ghi[...] = place.T.astype(BF16)
    si, sl = iota((ROWS, TOKS), 0), iota((ROWS, TOKS), 1)
    sel[...] = jnp.where((si == (sl >> 3) * CAP + (sl & 7)) & ((sl & 7) < CAP), 1.0, 0.0).astype(BF16)
    ei, el = iota((TOKS, ROWS), 1), iota((TOKS, ROWS), 0)
    exd[...] = jnp.where((ei == (el >> 3) * CAP + (el & 7)) & ((el & 7) < CAP), 1.0, 0.0).astype(BF16)
    logits[...] = jnp.zeros_like(logits)
    accg[...] = jnp.zeros_like(accg)
    accu[...] = jnp.zeros_like(accu)

    with jax.named_scope("w_bar"):
        pl.semaphore_wait(barrier, len(friends))
        loads[0].wait()

    def a_copy(j, i):
        ps, pe, pm = plane[i]
        return rcopy(asend.at[j, pm], arecv.at[j, me], a_send, a_recv.at[j], (ps, cx, pe))

    def dispatch(j):
        cols = pl.ds(pl.multiple_of(j * C, 128), C)
        rows = dot(disp[...], tok[:, cols])
        asend[j] = rows.reshape(FLIGHT, PAD, C).astype(BF16)
        for i in range(1, 16):
            a_copy(j, i).start()
        arecv[j, me] = asend[j, me]

    def dispatch_first(j, carry):
        with jax.named_scope("disp"):
            dispatch(j)
        return carry

    hc = C // 2
    left, right = pl.ds(0, hc), pl.ds(hc, hc)

    def y_near(p, step):
        return rcopy(yb.at[p, 0], yb.at[p, 1 if step == 1 else 2], y_send.at[0], y1.at[p], up if step == 1 else down)

    def y_far(p, step):
        half, rel, dev = (left, 1, up) if step == 1 else (right, 2, down)
        return rcopy(yb.at[p, rel, :, half], yb.at[p, 3, :, half], y_send.at[0], y3.at[p], dev)

    with jax.named_scope("pre"):
        compact = dot(sel[...], disp[...]).astype(BF16)
        for p in range(NP):
            cols = slice((NR + p) * C, (NR + p + 1) * C)
            yb[p, 0] = dot(compact, tok[:, cols]).astype(BF16)
            y_near(p, 1).start()
            y_near(p, 3).start()

    lax.fori_loop(0, AHEAD, dispatch_first, 0)
    wdx = rcopy(wd_h.at[:, theirs], wd.at[core], wdx_sem.at[0], wdx_sem.at[1], peer)
    wdx.start()
    with jax.named_scope("w_wts"):
        for rel in range(4):
            q = iota((MSG * FLIGHT, ROWS), 1)
            q = ((q * 205) >> 10) * (MSG - CAP) + q + CAP * rel
            pack[rel] = jnp.where(q == iota((MSG * FLIGHT, ROWS), 0), 1.0, 0.0).astype(BF16)
            q = iota((ROWS, MSG * FLIGHT), 0)
            q = ((q * 205) >> 10) * (MSG - CAP) + q + CAP * rel
            unpack[rel] = jnp.where(q == iota((ROWS, MSG * FLIGHT), 1), 1.0, 0.0).astype(BF16)
        for cp in loads[1:4]:
            cp.wait()
    with jax.named_scope("w_y1"):
        for p in range(NP):
            two = yb.at[p, pl.ds(0, 2)]
            rcopy(two, two, y_send.at[0], y1.at[p], peer).wait_recv()
            y_far(p, 1).start()
            y_far(p, 3).start()

    def y_message(p, i):
        ps, pe, pm = plane[i]
        return rcopy(ys.at[p, pm], yr.at[p, me], y_send.at[1], ym.at[p], (ps, cx, pe))

    def y_messages():
        for p in range(NP):
            with jax.named_scope("w_y3"):
                rcopy(yb.at[p, 0], yb.at[p, 0], y_send.at[0], y3.at[p], peer).wait_recv()
            v = dot(pack[0], yb[p, 0])
            for rel in range(1, 4):
                v = v + dot(pack[rel], yb[p, rel])
            ys[p] = v.reshape(FLIGHT, MSG, C).astype(BF16)
            for i in range(1, 16):
                y_message(p, i).start()
            yr[p, me] = ys[p, me]
            cols = slice((NR + p) * C, (NR + p + 1) * C)
            logits[...] += dot(tok[:, cols], rw[cols, :])

    def y_arrived():
        for p in range(NP):
            with jax.named_scope("w_ym"):
                most = yr.at[p, pl.ds(0, 15)]
                rcopy(most, most, y_send.at[1], ym.at[p], peer).wait_recv()
            got = yr[p].astype(F32).reshape(FLIGHT * MSG, C).astype(BF16)
            for rel in range(4):
                xb[NR + p, 2 * rel + core] = dot(unpack[rel], got).astype(BF16)
                g_peer(NR + p, rel).start()

    def g_own_up(j):
        return rcopy(xb.at[j, core], xb.at[j, 2 + core], g_send.at[0], g1.at[j], up)

    def g_own_down(j):
        return rcopy(xb.at[j, core], xb.at[j, 4 + core], g_send.at[1], g1.at[j], down)

    def g_far_up(j):
        return rcopy(xb.at[j, 2 + core, :, left], xb.at[j, 6 + core, :, left], g_send.at[2], g3.at[j], up)

    def g_far_down(j):
        return rcopy(xb.at[j, 4 + core, :, right], xb.at[j, 6 + core, :, right], g_send.at[3], g3.at[j], down)

    def g_peer(j, rel):
        at = 2 * rel + core
        return rcopy(xb.at[j, at], xb.at[j, at], g_send.at[4 + rel], gd.at[rel // 3, j], peer)

    def g_peer_wait(j, rel):
        blocks = xb.at[j, pl.ds(0, 1 if rel == 3 else 3)]
        rcopy(blocks, blocks, g_send.at[4], gd.at[rel // 3, j], peer).wait_recv()

    def multiply(j, rel):
        rows = pl.ds(pl.multiple_of(j * C, 128), C)
        at = slice(rel * 2 * ROWS, (rel + 1) * 2 * ROWS)
        v = xb[j, 2 * rel : 2 * rel + 2].reshape(2 * ROWS, C)
        accg[at, :] += dot(v, wg[rows, :])
        accu[at, :] += dot(v, wu[rows, :])

    def relay(j):
        g_far_up(j).start()
        g_far_down(j).start()

    def relay_arrived(j):
        rcopy(xb.at[j, 0], xb.at[j, 0], g_send.at[0], g3.at[j], peer).wait_recv()
        g_peer(j, 3).start()

    def multiply_far(j):
        g_peer_wait(j, 3)
        multiply(j, 3)

    def gather(i, carry):
        @stage(i + AHEAD < NR, "disp")
        def _():
            dispatch(i + AHEAD)

        @stage(i < NR, "fa")
        def _():
            j = i
            with jax.named_scope("w_a"):
                rcopy(
                    asend.at[j, pl.ds(0, 15)], arecv.at[j, pl.ds(0, 15)], a_send, a_recv.at[j], peer
                ).wait_recv()
            got = arecv[j].astype(F32).reshape(TOKS, C).astype(BF16)
            xb[j, core] = dot(sel[...], got).astype(BF16)
            g_own_up(j).start()
            g_own_down(j).start()
            g_peer(j, 0).start()
            cols = pl.ds(pl.multiple_of(j * C, 128), C)
            logits[...] += dot(tok[:, cols], rw[cols, :])

        @stage((i >= LAG) & (i < NR), "ff")
        def _():
            relay(i - LAG)

        @stage((i >= NEAR) & (i < NR + NEAR), "fn")
        def _():
            j = i - NEAR
            with jax.named_scope("w_g1"):
                two = xb.at[j, pl.ds(0, 2)]
                rcopy(two, two, g_send.at[0], g1.at[j], peer).wait_recv()
            g_peer(j, 1).start()
            g_peer(j, 2).start()

        @stage(i == NR, "ff")
        def _():
            for j in range(NR - LAG, NR - NEAR + 1):
                relay(j)

        @stage(i == NR - AHEAD, "ymsg")
        def _():
            y_messages()

        @stage(i == NR + 2, "yarr")
        def _():
            y_arrived()

        @stage((i > NR) & (i < NR + NEAR), "ff")
        def _():
            relay(i - NEAR)

        @stage((i >= NEAR + 2), "fm")
        def _():
            j = i - NEAR - 2
            with jax.named_scope("w_d"):
                g_peer_wait(j, 0)
            for rel in range(3):
                multiply(j, rel)

        @stage((i >= LAG + 2) & (i < LAG + 2 + NR - LATE), "fc")
        def _():
            with jax.named_scope("w_g3"):
                relay_arrived(i - LAG - 2)

        @stage((i >= LAG + 4) & (i < LAG + 4 + NR - LATE), "fmf")
        def _():
            multiply_far(i - LAG - 4)

        @stage(i >= NR + NEAR + 2, "fmf")
        def _():
            multiply_far(i - NEAR - 2)

        return carry

    lax.fori_loop(0, NC + NEAR + 2, gather, 0)

    def hidden(lo, n, k):
        at = pl.ds(lo, n)
        gate = accg[at, :]
        hb[core, at, :] = (gate * jax.nn.sigmoid(gate) * accu[at, :]).astype(BF16)
        h_copy(lo, n, k, core).start()

    def h_copy(lo, n, k, slot):
        at = pl.ds(lo, n)
        return rcopy(hb.at[core, at, :], hb.at[slot, at, :], h_sem.at[0, k], h_sem.at[1, k], peer)

    near_rows, far_rows = 6 * ROWS, 2 * ROWS
    with jax.named_scope("hn"):
        hidden(0, near_rows, 0)
    with jax.named_scope("w_h"):
        loads[4].wait()
        wdx.wait_recv()
        h_copy(0, near_rows, 0, other).wait_recv()

    def chunk(m):
        return pl.ds(pl.multiple_of(m * CM, 128), CM)

    def down_rows(lo, n, m):
        at = slice(lo * ROWS, (lo + n) * ROWS)
        cols = chunk(m)
        return dot(hb[0, at, :], wd[0, :, cols]) + dot(hb[1, at, :], wd[1, :, cols])

    def b_up(m, k):
        return rcopy(nu.at[m, k], f1.at[m, k], b_send.at[k], b_f.at[m], up)

    def b_down(m, k):
        return rcopy(nd.at[m, k], f2.at[m, k], b_send.at[2 + k], b_f.at[m], down)

    def b_far_up(m):
        return rcopy(t3.at[0, m], s3.at[0, m], b_send.at[4], b_s.at[m], up)

    def b_far_down(m):
        return rcopy(t3.at[1, m], s3.at[1, m], b_send.at[5], b_s.at[m], down)

    def independent(m):
        nd[m, 0] = down_rows(2, 1, m).astype(BF16)
        b_down(m, 0).start()
        nu[m, 1] = down_rows(5, 1, m).astype(BF16)
        b_up(m, 1).start()

    def late(j):
        with jax.named_scope("w_g3"):
            relay_arrived(j)

    def step(q, carry):
        with jax.named_scope("ind"):
            independent(q)

        @stage(q >= 1, "late")
        def _():
            late(NR - LATE - 1 + q)

        @stage(q >= 3, "fmf")
        def _():
            multiply_far(NR - LATE - 3 + q)

        return carry

    lax.fori_loop(0, LATE + 1, step, 0)
    with jax.named_scope("fmf"):
        multiply_far(NR - 2)
        multiply_far(NR - 1)
    with jax.named_scope("hf"):
        hidden(near_rows, far_rows, 1)
    with jax.named_scope("ind"):
        for q in range(LATE + 1, FIRST):
            independent(q)
    with jax.named_scope("w_hf"):
        h_copy(near_rows, far_rows, 1, other).wait_recv()

    def r_copy(m, rel, i):
        ps, pe, pm = plane[i]
        cc = core if rel == 0 else other
        return rcopy(rsend.at[m, cc, pm], rrecv.at[m, core * 16 + me], r_send.at[rel], r_recv.at[m], (ps, y * 2 + cc, pe))

    def st_a(i, rel):
        ps, pe, pm = plane[i]
        cc = core if rel == 0 else other
        return rcopy(sta.at[0], str_.at[core * 16 + me], st_send.at[0], st_recv.at[0], (ps, y * 2 + cc, pe))

    def st_b(dev):
        return rcopy(sta.at[1], stb.at[y], st_send.at[1], st_recv.at[1], dev)

    all_a = rcopy(str_.at[pl.ds(0, 15)], str_.at[pl.ds(0, 15)], st_send.at[0], st_recv.at[0], peer)
    all_b = rcopy(stb.at[pl.ds(0, 3)], stb.at[pl.ds(0, 3)], st_send.at[1], st_recv.at[1], peer)

    def statistics():
        scores = jax.nn.sigmoid(logits[...])
        eye = iota((EXPERTS, TOKS), 0)
        named = jnp.zeros((EXPERTS, TOKS), F32)
        for k in range(TOP):
            named = named + jnp.where(routes_ref[k : k + 1, :] == eye, 1.0, 0.0)
        named = named.T
        affinity = scores / jnp.sum(scores, axis=1, keepdims=True)
        sta[0, 0:1, :] = jnp.sum(affinity, axis=0, keepdims=True)
        sta[0, 1:2, :] = jnp.sum(named, axis=0, keepdims=True)
        total = jnp.sum(jnp.where(named > 0.0, scores, 0.0), axis=1, keepdims=True)
        weights = scores / total * 2.5
        spread = jnp.where(iota((EXPERTS, TOKS), 0) == (iota((EXPERTS, TOKS), 1) >> 3), 1.0, 0.0)
        wide = jnp.dot(weights, spread, preferred_element_type=F32, precision=lax.Precision.HIGHEST)
        g = jnp.where(ghi[...].astype(F32) > 0.0, wide, 0.0)
        hi = g.astype(BF16)
        ghi[...] = hi
        glo[...] = (g - hi.astype(F32)).astype(BF16)
        for rel in range(2):
            for i in range(0, 16, 2):
                if (rel, i) != (0, 0):
                    st_a(i, rel).start()

    def statistics_next():
        all_a.wait_recv()
        str_[core * 16 + me] = sta[0]
        acc = jnp.zeros((2, EXPERTS), F32)
        for cc in range(2):
            for e in range(8):
                acc = acc + str_[cc * 16 + s * 8 + e]
        sta[1] = acc
        stb[y] = acc
        for dev in (up, down, far):
            st_b(dev).start()

    def backward(i, carry):
        @stage(i < NM, "bt")
        def _():
            m = i
            v = down_rows(6, 2, m)
            t3[0, m] = v[:ROWS].astype(BF16)
            t3[1, m] = v[ROWS:].astype(BF16)
            b_far_up(m).start()
            b_far_down(m).start()

        @stage((lax.rem(i, 2) == 1) & (i < 2 * (NM - FIRST)), "bi")
        def _():
            independent(FIRST + lax.div(i, 2))

        @stage((i >= LEAD) & (i < NM + LEAD), "bb")
        def _():
            m = i - LEAD
            v = down_rows(3, 2, m)
            with jax.named_scope("w_s"):
                rcopy(nu.at[m], nu.at[m], b_send.at[0], b_s.at[m], peer).wait_recv()
            nu[m, 0] = (v[ROWS:] + s3[0, m].astype(F32)).astype(BF16)
            b_up(m, 0).start()
            nd[m, 1] = (v[:ROWS] + s3[1, m].astype(F32)).astype(BF16)
            b_down(m, 1).start()

        @stage(i == LEAD + 2, "stat")
        def _():
            statistics()

        @stage(i == NM // 2, "stat")
        def _():
            statistics_next()

        @stage((i >= LEAD + SUM) & (i < NM + LEAD + SUM), "bc")
        def _():
            m = i - LEAD - SUM
            v = down_rows(0, 2, m)
            with jax.named_scope("w_f"):
                four = nu.at[pl.ds(0, 2)]
                rcopy(four, four, b_send.at[0], b_f.at[m], peer).wait_recv()
            for cc in range(2):
                at = slice(cc * ROWS, (cc + 1) * ROWS)
                r = (v[at] + f1[m, cc].astype(F32) + f2[m, cc].astype(F32)).astype(BF16)
                w = dot(exd[...], r)
                rsend[m, cc] = w.reshape(FLIGHT, PAD, CM).astype(BF16)
            for i2 in range(16):
                for rel in range(2):
                    if (rel, i2) != (0, 0):
                        r_copy(m, rel, i2).start()
            rrecv[m, core * 16 + me] = rsend[m, core, me]

        @stage(i >= LEAD + BACK, "br")
        def _():
            m = i - LEAD - BACK
            with jax.named_scope("w_r"):
                most = rrecv.at[m, pl.ds(0, 31)]
                rcopy(most, most, r_send.at[0], r_recv.at[m], peer).wait_recv()
            for half in range(2):
                v = rrecv[m, half * 16 : half * 16 + 16].astype(F32).reshape(TOKS, CM).astype(BF16)
                cols = pl.ds(pl.multiple_of(half * HALF + m * CM, 128), CM)
                out_ref[:, cols] = (dot(ghi[...], v) + dot(glo[...], v)).astype(BF16)

        return carry

    lax.fori_loop(0, NM + LEAD + BACK, backward, 0)

    with jax.named_scope("fin"):
        all_b.wait_recv()
        tot = stb[0] + stb[1] + stb[2] + stb[3]
        bal_ref[...] = tot[1:2, :] * (EXPERTS / (TOP * LENGTH)) * (tot[0:1, :] / LENGTH) * EXPERTS

        wdx.wait_send()
        h_copy(0, near_rows, 0, core).wait_send()
        h_copy(near_rows, far_rows, 1, core).wait_send()
        all_a.wait_send()
        all_b.wait_send()

        def left_(src, sem):
            rcopy(src, src, sem, r_recv.at[0], peer).wait_send()

        left_(asend.at[:, pl.ds(0, 15)], a_send)
        some = pl.ds(0, NR)
        left_(xb.at[some, core], g_send.at[0])
        left_(xb.at[some, core], g_send.at[1])
        left_(xb.at[some, core, :, left], g_send.at[2])
        left_(xb.at[some, core, :, left], g_send.at[3])
        left_(yb.at[:, pl.ds(0, 3)], y_send.at[0])
        left_(ys.at[:, pl.ds(0, 15)], y_send.at[1])
        for rel in range(4):
            left_(xb.at[:, core], g_send.at[4 + rel])
        for k in range(6):
            left_(t3.at[0], b_send.at[k])
        left_(rsend.at[:, 0, pl.ds(0, 15)], r_send.at[0])
        left_(rsend.at[:, 0], r_send.at[1])


def on_device(tokens, routing, router_weight, w_gate, w_up, w_down):
    hbm = pl.BlockSpec(memory_space=pltpu.HBM)
    vmem = pl.BlockSpec(memory_space=pltpu.VMEM)
    V = pltpu.VMEM
    dma = pltpu.SemaphoreType.DMA
    out, bal = pl.pallas_call(
        kernel,
        out_shape=(
            jax.ShapeDtypeStruct((TOKS, D), BF16),
            jax.ShapeDtypeStruct((1, EXPERTS), F32),
        ),
        in_specs=[hbm, vmem, hbm, hbm, hbm, hbm],
        out_specs=(vmem, vmem),
        scratch_shapes=[
            V((TOKS, D), BF16),
            V((D, EXPERTS), BF16),
            V((D, HID), BF16),
            V((D, HID), BF16),
            V((2, HID, HALF), BF16),
            V((TOKS, TOKS), BF16),
            V((ROWS, TOKS), BF16),
            V((TOKS, ROWS), BF16),
            V((4, MSG * FLIGHT, ROWS), BF16),
            V((4, ROWS, MSG * FLIGHT), BF16),
            V((NP, 4, ROWS, C), BF16),
            V((NP, FLIGHT, MSG, C), BF16),
            V((NP, FLIGHT, MSG, C), BF16),
            V((TOKS, TOKS), BF16),
            V((TOKS, TOKS), BF16),
            V((TOKS, EXPERTS), F32),
            V((NR, FLIGHT, PAD, C), BF16),
            V((NR, FLIGHT, PAD, C), BF16),
            V((NC, 8, ROWS, C), BF16),
            V((8 * ROWS, HID), F32),
            V((8 * ROWS, HID), F32),
            V((2, 8 * ROWS, HID), BF16),
            V((2, NM, ROWS, CM), BF16),
            V((2, NM, ROWS, CM), BF16),
            V((NM, 2, ROWS, CM), BF16),
            V((NM, 2, ROWS, CM), BF16),
            V((NM, 2, ROWS, CM), BF16),
            V((NM, 2, ROWS, CM), BF16),
            V((NM, 2, FLIGHT, PAD, CM), BF16),
            V((NM, 2 * FLIGHT, PAD, CM), BF16),
            V((2, 2, EXPERTS), F32),
            V((32, 2, EXPERTS), F32),
            V((4, 2, EXPERTS), F32),
            dma((5,)),
            dma((2,)),
            dma(()),
            dma((NR,)),
            dma((8,)),
            dma((NR,)),
            dma((NR,)),
            dma((2, NC)),
            dma((2, 2)),
            dma((6,)),
            dma((NM,)),
            dma((NM,)),
            dma((2,)),
            dma((NM,)),
            dma((2,)),
            dma((2,)),
            dma((2,)),
            dma((NP,)),
            dma((NP,)),
            dma((NP,)),
        ],
        compiler_params=pltpu.CompilerParams(
            collective_id=0, has_side_effects=True, vmem_limit_bytes=52 * 1024 * 1024
        ),
    )(tokens[0], routing[0].T, router_weight, w_gate[0], w_up[0], w_down[0])
    return out[None], bal


def solution(mesh):
    placed = (
        P("seq", ("ctx", "exp"), None),
        P("seq", ("ctx", "exp"), None),
        P(),
        P(("seq", "exp"), None, "ctx"),
        P(("seq", "exp"), None, "ctx"),
        P(("seq", "exp"), "ctx", None),
    )
    return jax.shard_map(
        on_device,
        mesh=mesh,
        in_specs=placed,
        out_specs=(P("seq", ("ctx", "exp"), None), P("seq", None)),
        check_vma=False,
    )
```

```python
import jax
import jax.numpy as jnp
from jax import lax
from jax.experimental import pallas as pl
from jax.experimental.pallas import tpu as pltpu
from jax.sharding import PartitionSpec as P

MESH = pl.DeviceIdType.MESH
F32 = jnp.float32
BF16 = jnp.bfloat16

TOKS = 128
D = 7168
EXPERTS = 256
TOP = 8
FLIGHT = 16
CAP = 5
PAD = 8
HID = 256
ROWS = FLIGHT * CAP
LENGTH = 8192
HALF = D // 2

NC, C = 14, 512
NM, CM = 14, 256
NR = 12
NP = NC - NR
MSG = 24
AHEAD = 6
NEAR = 3
LAG = 6
FAR = 10
EARLY = 3
NL = 3
NB = NM - NL
PLACE = 8 * CAP
FIRST = 7
LEAD = 3
SUM = 3
BACK = 9


SLOT = ((0, 1), (2, 4), (5, 3), (6, 7))


def dot(a, b):
    return jnp.dot(a, b, preferred_element_type=F32)


def iota(shape, dim):
    return lax.broadcasted_iota(jnp.int32, shape, dim)


def stage(cond, name):
    def wrap(body):
        @pl.when(cond)
        def _():
            with jax.named_scope(name):
                body()

    return wrap


def kernel(
    tok_h, routes_ref, rw_h, wg_h, wu_h, wd_h,
    out_ref, bal_ref,
    tok, rw, wg, wu, wd, disp, sel, exd, pack, unpack, yb, ys, yr, ghi, glo, logits,
    asend, arecv, xb, accg, accu, hb,
    t3, s3, nu, nd, f1, f2, rsend, rrecv, sort, hp, ls, lr, lp, hs, hr, vbuf, khi, klo,
    sta, str_, stb,
    load_sem, wdx_sem, a_send, a_recv, g_send, g1, g3, gd,
    h_sem, b_send, b_s, b_f, r_send, r_recv, st_send, st_recv, y_send, y1, y3, ym, l_send, lm, lh,
):
    s = lax.axis_index("seq")
    cx = lax.axis_index("ctx")
    ex = lax.axis_index("exp")
    core = lax.rem(cx, 2)
    other = 1 - core
    y = lax.div(cx, 2)
    zh = lax.div(ex, 4)
    xx = lax.rem(ex, 4)
    me = s * 8 + ex

    def at_y(step):
        return (s, lax.rem(y + step, 4) * 2 + core, ex)

    up, down, far = at_y(1), at_y(3), at_y(2)
    peer = (s, y * 2 + other, ex)

    plane = []
    for dx in range(4):
        for dh in range(2):
            for dl in range(2):
                ps = lax.rem(s + dl, 2)
                pe = lax.rem(zh + dh, 2) * 4 + lax.rem(xx + dx, 4)
                plane.append((ps, pe, ps * 8 + pe))

    def rcopy(src, dst, ssem, rsem, dev):
        return pltpu.make_async_remote_copy(
            src_ref=src, dst_ref=dst, send_sem=ssem, recv_sem=rsem, device_id=dev, device_id_type=MESH
        )

    mine = pl.ds(pl.multiple_of(core * HALF, 128), HALF)
    theirs = pl.ds(pl.multiple_of(other * HALF, 128), HALF)
    pairs = [(tok_h, tok), (rw_h, rw), (wg_h, wg), (wu_h, wu), (wd_h.at[:, mine], wd.at[core])]
    loads = [pltpu.make_async_copy(src, dst, load_sem.at[k]) for k, (src, dst) in enumerate(pairs)]
    for cp in loads:
        cp.start()

    barrier = pltpu.get_barrier_semaphore()
    friends = [(ps, y * 2 + core, pe) for ps, pe, _ in plane[1:]]
    friends += [(ps, y * 2 + other, pe) for ps, pe, _ in plane]
    friends += [up, down, far]
    for dev in friends:
        pl.semaphore_signal(barrier, inc=1, device_id=dev, device_id_type=MESH)

    lane = iota((TOKS, TOKS), 1)
    sub = iota((TOKS, TOKS), 0)
    hit = jnp.zeros((TOKS, TOKS), F32)
    for k in range(TOP):
        hit = hit + jnp.where(routes_ref[k : k + 1, :] == (sub >> 3), 1.0, 0.0)
    before = jnp.where(sub < lane, 1.0, 0.0).astype(BF16)
    rank = dot(hit.astype(BF16), before)
    place = jnp.where(rank == (sub & 7).astype(F32), hit, 0.0)
    disp[...] = place.astype(BF16)
    ghi[...] = place.T.astype(BF16)
    si, sl = iota((ROWS, TOKS), 0), iota((ROWS, TOKS), 1)
    sel[...] = jnp.where((si == (sl >> 3) * CAP + (sl & 7)) & ((sl & 7) < CAP), 1.0, 0.0).astype(BF16)
    ei, el = iota((TOKS, ROWS), 1), iota((TOKS, ROWS), 0)
    exd[...] = jnp.where((ei == (el >> 3) * CAP + (el & 7)) & ((el & 7) < CAP), 1.0, 0.0).astype(BF16)
    logits[...] = jnp.zeros_like(logits)
    accg[...] = jnp.zeros_like(accg)
    accu[...] = jnp.zeros_like(accu)

    with jax.named_scope("w_bar"):
        pl.semaphore_wait(barrier, len(friends))
        loads[0].wait()

    def a_copy(j, i):
        ps, pe, pm = plane[i]
        return rcopy(asend.at[j, pm], arecv.at[j, me], a_send, a_recv.at[j], (ps, cx, pe))

    def dispatch(j):
        cols = pl.ds(pl.multiple_of(j * C, 128), C)
        rows = dot(disp[...], tok[:, cols])
        asend[j] = rows.reshape(FLIGHT, PAD, C).astype(BF16)
        for i in range(1, 16):
            a_copy(j, i).start()
        arecv[j, me] = asend[j, me]

    def dispatch_first(j, carry):
        with jax.named_scope("disp"):
            dispatch(j)
        return carry

    hc = C // 2
    left, right = pl.ds(0, hc), pl.ds(hc, hc)

    def y_near(p, step):
        return rcopy(yb.at[p, 0], yb.at[p, 1 if step == 1 else 2], y_send.at[0], y1.at[p], up if step == 1 else down)

    def y_far(p, step):
        half, rel, dev = (left, 1, up) if step == 1 else (right, 2, down)
        return rcopy(yb.at[p, rel, :, half], yb.at[p, 3, :, half], y_send.at[0], y3.at[p], dev)

    with jax.named_scope("pre"):
        compact = dot(sel[...], disp[...]).astype(BF16)
        for p in range(NP):
            cols = slice((NR + p) * C, (NR + p + 1) * C)
            yb[p, 0] = dot(compact, tok[:, cols]).astype(BF16)
            y_near(p, 1).start()
            y_near(p, 3).start()

    lax.fori_loop(0, AHEAD, dispatch_first, 0)
    wdx = rcopy(wd_h.at[:, theirs], wd.at[core], wdx_sem.at[0], wdx_sem.at[1], peer)
    wdx.start()
    with jax.named_scope("w_wts"):
        for rel in range(4):
            q = iota((MSG * FLIGHT, ROWS), 1)
            q = ((q * 205) >> 10) * (MSG - CAP) + q + CAP * rel
            pack[rel] = jnp.where(q == iota((MSG * FLIGHT, ROWS), 0), 1.0, 0.0).astype(BF16)
            q = iota((ROWS, MSG * FLIGHT), 0)
            q = ((q * 205) >> 10) * (MSG - CAP) + q + CAP * rel
            unpack[rel] = jnp.where(q == iota((ROWS, MSG * FLIGHT), 1), 1.0, 0.0).astype(BF16)
        q = iota((ROWS, 8 * ROWS), 0)
        q = iota((ROWS, 8 * ROWS), 1) - ((q * 205) >> 10) * (PLACE - CAP) - q
        for rel in range(4):
            for c in range(2):
                at = slice(SLOT[rel][c] * ROWS, (SLOT[rel][c] + 1) * ROWS)
                sort[at, :] = jnp.where(q == (2 * rel + c) * CAP, 1.0, 0.0).astype(BF16)
        for cp in loads[1:4]:
            cp.wait()

    def y_relay(p):
        two = yb.at[p, pl.ds(0, 2)]
        rcopy(two, two, y_send.at[0], y1.at[p], peer).wait_recv()
        y_far(p, 1).start()
        y_far(p, 3).start()

    def y_message(p, i):
        ps, pe, pm = plane[i]
        return rcopy(ys.at[p, pm], yr.at[p, me], y_send.at[1], ym.at[p], (ps, cx, pe))

    def y_messages():
        for p in range(NP):
            with jax.named_scope("w_y3"):
                rcopy(yb.at[p, 0], yb.at[p, 0], y_send.at[0], y3.at[p], peer).wait_recv()
            v = dot(pack[0], yb[p, 0])
            for rel in range(1, 4):
                v = v + dot(pack[rel], yb[p, rel])
            ys[p] = v.reshape(FLIGHT, MSG, C).astype(BF16)
            for i in range(1, 16):
                y_message(p, i).start()
            yr[p, me] = ys[p, me]
            cols = slice((NR + p) * C, (NR + p + 1) * C)
            logits[...] += dot(tok[:, cols], rw[cols, :])

    def y_arrived():
        for p in range(NP):
            with jax.named_scope("w_ym"):
                most = yr.at[p, pl.ds(0, 15)]
                rcopy(most, most, y_send.at[1], ym.at[p], peer).wait_recv()
            got = yr[p].astype(F32).reshape(FLIGHT * MSG, C).astype(BF16)
            for rel in range(4):
                xb[NR + p, slot(rel, core)] = dot(unpack[rel], got).astype(BF16)
                g_peer(NR + p, rel).start()

    def slot(rel, c):
        return (c, 2 + 2 * c, 5 - 2 * c, 6 + c)[rel]

    def g_own_up(j):
        return rcopy(xb.at[j, core], xb.at[j, slot(1, core)], g_send.at[0], g1.at[j], up)

    def g_own_down(j):
        return rcopy(xb.at[j, core], xb.at[j, slot(2, core)], g_send.at[1], g1.at[j], down)

    def g_far_up(j):
        return rcopy(xb.at[j, slot(1, core), :, left], xb.at[j, 6 + core, :, left], g_send.at[2], g3.at[j], up)

    def g_far_down(j):
        return rcopy(xb.at[j, slot(2, core), :, right], xb.at[j, 6 + core, :, right], g_send.at[3], g3.at[j], down)

    def g_peer(j, rel):
        at = slot(rel, core)
        return rcopy(xb.at[j, at], xb.at[j, at], g_send.at[4 + rel], gd.at[rel // 3, j], peer)

    def g_peer_wait(j, rel):
        blocks = xb.at[j, pl.ds(0, 1 if rel == 3 else 3)]
        rcopy(blocks, blocks, g_send.at[4], gd.at[rel // 3, j], peer).wait_recv()

    def multiply(j, rel):
        rows = pl.ds(pl.multiple_of(j * C, 128), C)
        at = slice(rel * 2 * ROWS, (rel + 1) * 2 * ROWS)
        v = xb[j, 2 * rel : 2 * rel + 2].reshape(2 * ROWS, C)
        accg[at, :] += dot(v, wg[rows, :])
        accu[at, :] += dot(v, wu[rows, :])

    def relay(j):
        g_far_up(j).start()
        g_far_down(j).start()

    def relay_arrived(j):
        rcopy(xb.at[j, 0], xb.at[j, 0], g_send.at[0], g3.at[j], peer).wait_recv()
        g_peer(j, 3).start()

    def multiply_near(j):
        with jax.named_scope("w_d"):
            g_peer_wait(j, 0)
        for rel in range(3):
            multiply(j, rel)

    def multiply_far(j):
        g_peer_wait(j, 3)
        multiply(j, 3)

    def st_a(i, rel):
        ps, pe, pm = plane[i]
        cc = core if rel == 0 else other
        return rcopy(sta.at[0], str_.at[core * 16 + me], st_send.at[0], st_recv.at[0], (ps, y * 2 + cc, pe))

    def st_b(dev):
        return rcopy(sta.at[1], stb.at[y], st_send.at[1], st_recv.at[1], dev)

    all_a = rcopy(str_.at[pl.ds(0, 15)], str_.at[pl.ds(0, 15)], st_send.at[0], st_recv.at[0], peer)
    all_b = rcopy(stb.at[pl.ds(0, 3)], stb.at[pl.ds(0, 3)], st_send.at[1], st_recv.at[1], peer)

    def statistics():
        scores = jax.nn.sigmoid(logits[...])
        eye = iota((EXPERTS, TOKS), 0)
        named = jnp.zeros((EXPERTS, TOKS), F32)
        for k in range(TOP):
            named = named + jnp.where(routes_ref[k : k + 1, :] == eye, 1.0, 0.0)
        named = named.T
        affinity = scores / jnp.sum(scores, axis=1, keepdims=True)
        sta[0, 0:1, :] = jnp.sum(affinity, axis=0, keepdims=True)
        sta[0, 1:2, :] = jnp.sum(named, axis=0, keepdims=True)
        total = jnp.sum(jnp.where(named > 0.0, scores, 0.0), axis=1, keepdims=True)
        weights = scores / total * 2.5
        spread = jnp.where(iota((EXPERTS, TOKS), 0) == (iota((EXPERTS, TOKS), 1) >> 3), 1.0, 0.0)
        wide = jnp.dot(weights, spread, preferred_element_type=F32, precision=lax.Precision.HIGHEST)
        g = jnp.where(ghi[...].astype(F32) > 0.0, wide, 0.0)
        hi = g.astype(BF16)
        ghi[...] = hi
        lo = (g - hi.astype(F32)).astype(BF16)
        glo[...] = lo
        khi[...] = dot(hi, exd[...]).astype(BF16)
        klo[...] = dot(lo, exd[...]).astype(BF16)
        for rel in range(2):
            for i in range(0, 16, 2):
                if (rel, i) != (0, 0):
                    st_a(i, rel).start()

    def statistics_next():
        all_a.wait_recv()
        str_[core * 16 + me] = sta[0]
        acc = jnp.zeros((2, EXPERTS), F32)
        for cc in range(2):
            for e in range(8):
                acc = acc + str_[cc * 16 + s * 8 + e]
        sta[1] = acc
        stb[y] = acc
        for dev in (up, down, far):
            st_b(dev).start()

    def gather(i, carry):
        @stage(i + AHEAD < NR, "disp")
        def _():
            dispatch(i + AHEAD)

        @stage(i < NR, "fa")
        def _():
            j = i
            with jax.named_scope("w_a"):
                rcopy(
                    asend.at[j, pl.ds(0, 15)], arecv.at[j, pl.ds(0, 15)], a_send, a_recv.at[j], peer
                ).wait_recv()
            got = arecv[j].astype(F32).reshape(TOKS, C).astype(BF16)
            xb[j, core] = dot(sel[...], got).astype(BF16)
            g_own_up(j).start()
            g_own_down(j).start()
            g_peer(j, 0).start()
            cols = pl.ds(pl.multiple_of(j * C, 128), C)
            logits[...] += dot(tok[:, cols], rw[cols, :])

        @stage(i < NP, "w_y1")
        def _():
            y_relay(i)

        @stage((i >= LAG) & (i < NR), "ff")
        def _():
            relay(i - LAG)

        @stage((i >= NEAR) & (i < NR + NEAR), "fn")
        def _():
            j = i - NEAR
            with jax.named_scope("w_g1"):
                two = xb.at[j, pl.ds(0, 2)]
                rcopy(two, two, g_send.at[0], g1.at[j], peer).wait_recv()
            g_peer(j, 1).start()
            g_peer(j, 2).start()

        @stage(i == NR, "ff")
        def _():
            for j in range(NR - LAG, NR - NEAR + 1):
                relay(j)

        @stage(i == NR - AHEAD, "ymsg")
        def _():
            y_messages()

        @stage(i == NR, "yarr")
        def _():
            y_arrived()

        @stage(i == NR + 1, "stat")
        def _():
            statistics()

        @stage((i > NR) & (i < NR + NEAR), "ff")
        def _():
            relay(i - NEAR)

        @stage((i > NEAR) & (i < NR + NEAR), "fm")
        def _():
            multiply_near(i - NEAR - 1)

        @stage(i == NR + NEAR - 1, "fm")
        def _():
            for j in range(NR, NC):
                multiply_near(j)

        @stage(i == NR + NEAR, "fm")
        def _():
            multiply_near(NR - 1)

        @stage(i >= FAR, "fc")
        def _():
            with jax.named_scope("w_g3"):
                relay_arrived(i - FAR)

        @stage((i > FAR) & (i <= FAR + EARLY), "fmf")
        def _():
            multiply_far(i - FAR - 1)

        return carry

    lax.fori_loop(0, NR + NEAR + 1, gather, 0)

    def hidden(lo, n, k):
        at = pl.ds(lo, n)
        gate = accg[at, :]
        hb[core, at, :] = (gate * jax.nn.sigmoid(gate) * accu[at, :]).astype(BF16)
        h_copy(lo, n, k, core).start()

    def h_copy(lo, n, k, slot):
        at = pl.ds(lo, n)
        return rcopy(hb.at[core, at, :], hb.at[slot, at, :], h_sem.at[0, k], h_sem.at[1, k], peer)

    near_rows, far_rows = 6 * ROWS, 2 * ROWS
    with jax.named_scope("hn"):
        hidden(0, near_rows, 0)
    with jax.named_scope("w_h"):
        loads[4].wait()
        wdx.wait_recv()
        h_copy(0, near_rows, 0, other).wait_recv()

    def chunk(m):
        return pl.ds(pl.multiple_of(m * CM, 128), CM)

    def down_rows(lo, n, m):
        at = slice(lo * ROWS, (lo + n) * ROWS)
        cols = chunk(m)
        return dot(hb[0, at, :], wd[0, :, cols]) + dot(hb[1, at, :], wd[1, :, cols])

    def rows_of(slots, m):
        at = slice(slots * ROWS, (slots + 2) * ROWS)

        @pl.when(m < NB)
        def _():
            vbuf[...] = down_rows(slots, 2, m)

        @pl.when(m >= NB)
        def _():
            vbuf[...] = lp[m - NB, at, :].astype(F32)

        return vbuf[...]

    def l_copy(q, i):
        ps, pe, pm = plane[i]
        return rcopy(ls.at[q, pm], lr.at[q, me], l_send.at[0], lm.at[q], (ps, cx, pe))

    def reorder():
        q = iota((8 * ROWS, ROWS), 1)
        q = iota((8 * ROWS, ROWS), 0) - ((q * 205) >> 10) * (PLACE - CAP) - q
        for half in range(2):
            v = jnp.zeros((8 * ROWS, HID), F32)
            for rel in range(4):
                for c in range(2):
                    at = slice(SLOT[rel][c] * ROWS, (SLOT[rel][c] + 1) * ROWS)
                    take = jnp.where(q == (2 * rel + c) * CAP, 1.0, 0.0).astype(BF16)
                    v = v + dot(take, hb[half, at, :])
            hp[half] = v.astype(BF16)

    def go_home(q):
        cols = chunk(NB + q)
        v = dot(hp[0], wd[0, :, cols]) + dot(hp[1], wd[1, :, cols])
        ls[q] = v.reshape(FLIGHT, PLACE, CM).astype(BF16)
        for i in range(1, 16):
            l_copy(q, i).start()
        lr[q, me] = ls[q, me]

    def came_home(q):
        most = lr.at[q, pl.ds(0, 15)]
        rcopy(most, most, l_send.at[0], lm.at[q], peer).wait_recv()
        lp[q] = dot(sort[...], lr[q].reshape(8 * ROWS, CM)).astype(BF16)

    def h_share(q):
        return rcopy(hs.at[q], hr.at[q, core], l_send.at[1], lh.at[q], peer)

    def b_up(m, k):
        return rcopy(nu.at[m, k], f1.at[m, k], b_send.at[k], b_f.at[m], up)

    def b_down(m, k):
        return rcopy(nd.at[m, k], f2.at[m, k], b_send.at[2 + k], b_f.at[m], down)

    def b_far_up(m):
        return rcopy(t3.at[0, m], s3.at[0, m], b_send.at[4], b_s.at[m], up)

    def b_far_down(m):
        return rcopy(t3.at[1, m], s3.at[1, m], b_send.at[5], b_s.at[m], down)

    def independent(m):
        v = rows_of(2, m)
        nd[m, 0] = v[:ROWS].astype(BF16)
        b_down(m, 0).start()
        nu[m, 1] = v[ROWS:].astype(BF16)
        b_up(m, 1).start()

    def ind(q):
        with jax.named_scope("ind"):
            independent(q)

    waiting = [(j,) for j in range(NR + NEAR + 1 - FAR, NR)]
    ready = list(range(EARLY, NR + NEAR + 1 - FAR)) + list(range(NR, NC))
    ind(0)
    for q in range(1, FIRST):
        ind(q)
        if waiting:
            (j,) = waiting.pop(0)
            with jax.named_scope("w_g3"):
                relay_arrived(j)
            ready.append(j)
        with jax.named_scope("fmf"):
            for j in ready[:2] if len(ready) > 2 else []:
                multiply_far(j)
            if len(ready) > 2:
                ready = ready[2:]
    with jax.named_scope("fmf"):
        for (j,) in waiting:
            relay_arrived(j)
            ready.append(j)
        for j in ready:
            multiply_far(j)
    with jax.named_scope("hf"):
        hidden(near_rows, far_rows, 1)
    with jax.named_scope("w_hf"):
        h_copy(near_rows, far_rows, 1, other).wait_recv()

    def r_copy(m, rel, i):
        ps, pe, pm = plane[i]
        cc = core if rel == 0 else other
        return rcopy(rsend.at[m, cc, pm], rrecv.at[m, core * 16 + me], r_send.at[rel], r_recv.at[m], (ps, y * 2 + cc, pe))

    def backward(i, carry):
        @stage(i < NM, "bt")
        def _():
            m = i
            v = rows_of(6, m)
            t3[0, m] = v[:ROWS].astype(BF16)
            t3[1, m] = v[ROWS:].astype(BF16)
            b_far_up(m).start()
            b_far_down(m).start()

        @stage((lax.rem(i, 2) == 1) & (i < 2 * (NB - FIRST)), "bi")
        def _():
            independent(FIRST + lax.div(i, 2))

        @stage(i == 1, "home")
        def _():
            reorder()

        @stage((i >= 1) & (i <= NL), "home")
        def _():
            go_home(i - 1)

        @stage((i >= NB - NL) & (i < NB), "homew")
        def _():
            came_home(i - NB + NL)

        @stage((i >= NB + LEAD) & (i < NM + LEAD), "bi")
        def _():
            independent(i - LEAD)

        @stage((i >= LEAD) & (i < NM + LEAD), "bb")
        def _():
            m = i - LEAD
            v = rows_of(4, m)
            with jax.named_scope("w_s"):
                rcopy(nu.at[m], nu.at[m], b_send.at[0], b_s.at[m], peer).wait_recv()
            nu[m, 0] = (v[ROWS:] + s3[0, m].astype(F32)).astype(BF16)
            b_up(m, 0).start()
            nd[m, 1] = (v[:ROWS] + s3[1, m].astype(F32)).astype(BF16)
            b_down(m, 1).start()

        @stage(i == LEAD - 1, "stat")
        def _():
            statistics_next()

        @stage((i >= LEAD + SUM) & (i < NM + LEAD + SUM), "bc")
        def _():
            m = i - LEAD - SUM
            v = rows_of(0, m)
            with jax.named_scope("w_f"):
                four = nu.at[pl.ds(0, 2)]
                rcopy(four, four, b_send.at[0], b_f.at[m], peer).wait_recv()
            r = [
                (v[c * ROWS : (c + 1) * ROWS] + f1[m, c].astype(F32) + f2[m, c].astype(F32)).astype(BF16)
                for c in range(2)
            ]

            @pl.when(m < NB)
            def _():
                for c in range(2):
                    rsend[m, c] = dot(exd[...], r[c]).reshape(FLIGHT, PAD, CM).astype(BF16)
                for i2 in range(16):
                    for rel in range(2):
                        if (rel, i2) != (0, 0):
                            r_copy(m, rel, i2).start()
                rrecv[m, core * 16 + me] = rsend[m, core, me]

            @pl.when(m >= NB)
            def _():
                hs[m - NB] = jnp.where(core == 0, r[1], r[0])
                h_share(m - NB).start()
                hr[m - NB, core] = jnp.where(core == 0, r[0], r[1])

        @stage((i >= LEAD + BACK) & (i < NB + LEAD + BACK), "br")
        def _():
            m = i - LEAD - BACK
            with jax.named_scope("w_r"):
                most = rrecv.at[m, pl.ds(0, 31)]
                rcopy(most, most, r_send.at[0], r_recv.at[m], peer).wait_recv()
            for half in range(2):
                v = rrecv[m, half * 16 : half * 16 + 16].astype(F32).reshape(TOKS, CM).astype(BF16)
                cols = pl.ds(pl.multiple_of(half * HALF + m * CM, 128), CM)
                out_ref[:, cols] = (dot(ghi[...], v) + dot(glo[...], v)).astype(BF16)

        return carry

    lax.fori_loop(0, max(NB + LEAD + BACK, NM + LEAD + SUM), backward, 0)

    def last(q, carry):
        with jax.named_scope("w_l"):
            rcopy(hs.at[q], hr.at[q, other], l_send.at[1], lh.at[q], peer).wait_recv()
        for half in range(2):
            v = hr[q, half]
            cols = pl.ds(pl.multiple_of(half * HALF + (NB + q) * CM, 128), CM)
            out_ref[:, cols] = (dot(khi[...], v) + dot(klo[...], v)).astype(BF16)
        return carry

    lax.fori_loop(0, NL, last, 0)

    with jax.named_scope("fin"):
        all_b.wait_recv()
        tot = stb[0] + stb[1] + stb[2] + stb[3]
        bal_ref[...] = tot[1:2, :] * (EXPERTS / (TOP * LENGTH)) * (tot[0:1, :] / LENGTH) * EXPERTS

        wdx.wait_send()
        h_copy(0, near_rows, 0, core).wait_send()
        h_copy(near_rows, far_rows, 1, core).wait_send()
        all_a.wait_send()
        all_b.wait_send()

        def left_(src, sem):
            rcopy(src, src, sem, r_recv.at[0], peer).wait_send()

        left_(asend.at[:, pl.ds(0, 15)], a_send)
        some = pl.ds(0, NR)
        left_(xb.at[some, core], g_send.at[0])
        left_(xb.at[some, core], g_send.at[1])
        left_(xb.at[some, core, :, left], g_send.at[2])
        left_(xb.at[some, core, :, left], g_send.at[3])
        left_(yb.at[:, pl.ds(0, 3)], y_send.at[0])
        left_(ys.at[:, pl.ds(0, 15)], y_send.at[1])
        for rel in range(4):
            left_(xb.at[:, core], g_send.at[4 + rel])
        for k in range(6):
            left_(t3.at[0], b_send.at[k])
        left_(ls.at[:, pl.ds(0, 15)], l_send.at[0])
        left_(hs, l_send.at[1])
        left_(rsend.at[:, 0, pl.ds(0, 15)], r_send.at[0])
        left_(rsend.at[:, 0], r_send.at[1])


def on_device(tokens, routing, router_weight, w_gate, w_up, w_down):
    hbm = pl.BlockSpec(memory_space=pltpu.HBM)
    vmem = pl.BlockSpec(memory_space=pltpu.VMEM)
    V = pltpu.VMEM
    dma = pltpu.SemaphoreType.DMA
    out, bal = pl.pallas_call(
        kernel,
        out_shape=(
            jax.ShapeDtypeStruct((TOKS, D), BF16),
            jax.ShapeDtypeStruct((1, EXPERTS), F32),
        ),
        in_specs=[hbm, vmem, hbm, hbm, hbm, hbm],
        out_specs=(vmem, vmem),
        scratch_shapes=[
            V((TOKS, D), BF16),
            V((D, EXPERTS), BF16),
            V((D, HID), BF16),
            V((D, HID), BF16),
            V((2, HID, HALF), BF16),
            V((TOKS, TOKS), BF16),
            V((ROWS, TOKS), BF16),
            V((TOKS, ROWS), BF16),
            V((4, MSG * FLIGHT, ROWS), BF16),
            V((4, ROWS, MSG * FLIGHT), BF16),
            V((NP, 4, ROWS, C), BF16),
            V((NP, FLIGHT, MSG, C), BF16),
            V((NP, FLIGHT, MSG, C), BF16),
            V((TOKS, TOKS), BF16),
            V((TOKS, TOKS), BF16),
            V((TOKS, EXPERTS), F32),
            V((NR, FLIGHT, PAD, C), BF16),
            V((NR, FLIGHT, PAD, C), BF16),
            V((NC, 8, ROWS, C), BF16),
            V((8 * ROWS, HID), F32),
            V((8 * ROWS, HID), F32),
            V((2, 8 * ROWS, HID), BF16),
            V((2, NM, ROWS, CM), BF16),
            V((2, NM, ROWS, CM), BF16),
            V((NM, 2, ROWS, CM), BF16),
            V((NM, 2, ROWS, CM), BF16),
            V((NM, 2, ROWS, CM), BF16),
            V((NM, 2, ROWS, CM), BF16),
            V((NB, 2, FLIGHT, PAD, CM), BF16),
            V((NB, 2 * FLIGHT, PAD, CM), BF16),
            V((8 * ROWS, 8 * ROWS), BF16),
            V((2, 8 * ROWS, HID), BF16),
            V((NL, FLIGHT, PLACE, CM), BF16),
            V((NL, FLIGHT, PLACE, CM), BF16),
            V((NL, 8 * ROWS, CM), BF16),
            V((NL, ROWS, CM), BF16),
            V((NL, 2, ROWS, CM), BF16),
            V((2 * ROWS, CM), F32),
            V((TOKS, ROWS), BF16),
            V((TOKS, ROWS), BF16),
            V((2, 2, EXPERTS), F32),
            V((32, 2, EXPERTS), F32),
            V((4, 2, EXPERTS), F32),
            dma((5,)),
            dma((2,)),
            dma(()),
            dma((NR,)),
            dma((8,)),
            dma((NR,)),
            dma((NR,)),
            dma((2, NC)),
            dma((2, 2)),
            dma((6,)),
            dma((NM,)),
            dma((NM,)),
            dma((2,)),
            dma((NB,)),
            dma((2,)),
            dma((2,)),
            dma((2,)),
            dma((NP,)),
            dma((NP,)),
            dma((NP,)),
            dma((2,)),
            dma((NL,)),
            dma((NL,)),
        ],
        compiler_params=pltpu.CompilerParams(
            collective_id=0, has_side_effects=True, vmem_limit_bytes=52 * 1024 * 1024
        ),
    )(tokens[0], routing[0].T, router_weight, w_gate[0], w_up[0], w_down[0])
    return out[None], bal


def solution(mesh):
    placed = (
        P("seq", ("ctx", "exp"), None),
        P("seq", ("ctx", "exp"), None),
        P(),
        P(("seq", "exp"), None, "ctx"),
        P(("seq", "exp"), None, "ctx"),
        P(("seq", "exp"), "ctx", None),
    )
    return jax.shard_map(
        on_device,
        mesh=mesh,
        in_specs=placed,
        out_specs=(P("seq", ("ctx", "exp"), None), P("seq", None)),
        check_vma=False,
    )
```

```python
import jax
import jax.numpy as jnp
from jax import lax
from jax.experimental import pallas as pl
from jax.experimental.pallas import tpu as pltpu
from jax.sharding import PartitionSpec as P

MESH = pl.DeviceIdType.MESH
F32 = jnp.float32
BF16 = jnp.bfloat16

TOKS = 128
D = 7168
EXPERTS = 256
TOP = 8
FLIGHT = 16
CAP = 5
PAD = 8
HID = 256
ROWS = FLIGHT * CAP
LENGTH = 8192
HALF = D // 2

NC, C = 14, 512
NM, CM = 14, 256
NR = 12
NP = NC - NR
YPRE = 2
YARR = 0
MSG = 24
AHEAD = 6
NEAR = 3
LAG = 8
FAR = 12
EARLY = 2
NL = 3
NB = NM - NL
FIRST = 7
LEAD = 3
SUM = 3
BACK = 9


SLOT = ((0, 1), (2, 4), (5, 3), (6, 7))


def dot(a, b):
    return jnp.dot(a, b, preferred_element_type=F32)


def iota(shape, dim):
    return lax.broadcasted_iota(jnp.int32, shape, dim)


def stage(cond, name):
    def wrap(body):
        @pl.when(cond)
        def _():
            with jax.named_scope(name):
                body()

    return wrap


def kernel(
    tok_h, routes_ref, rw_h, wg_h, wu_h, wd_h,
    out_ref, bal_ref,
    tok, rw, wg, wu, wd, disp, sel, exd, pack, unpack, yb, ys, yr, ghi, glo, logits,
    asend, arecv, xb, accg, accu, hb,
    t3, s3, nu, nd, f1, f2, rsend, rrecv, hp, ls, lr, lp, hr, vbuf, khi, klo,
    sta, str_, stb,
    load_sem, wdx_sem, a_send, a_recv, g_send, g1, g3, gd,
    h_sem, b_send, b_s, b_f, r_send, r_recv, st_send, st_recv, y_send, y1, y3, ym, l_send, lm,
):
    s = lax.axis_index("seq")
    cx = lax.axis_index("ctx")
    ex = lax.axis_index("exp")
    core = lax.rem(cx, 2)
    other = 1 - core
    y = lax.div(cx, 2)
    zh = lax.div(ex, 4)
    xx = lax.rem(ex, 4)
    me = s * 8 + ex

    def at_y(step):
        return (s, lax.rem(y + step, 4) * 2 + core, ex)

    up, down, far = at_y(1), at_y(3), at_y(2)
    peer = (s, y * 2 + other, ex)

    plane = []
    for dx in range(4):
        for dh in range(2):
            for dl in range(2):
                ps = lax.rem(s + dl, 2)
                pe = lax.rem(zh + dh, 2) * 4 + lax.rem(xx + dx, 4)
                plane.append((ps, pe, ps * 8 + pe))

    def rcopy(src, dst, ssem, rsem, dev):
        return pltpu.make_async_remote_copy(
            src_ref=src, dst_ref=dst, send_sem=ssem, recv_sem=rsem, device_id=dev, device_id_type=MESH
        )

    mine = pl.ds(pl.multiple_of(core * HALF, 128), HALF)
    theirs = pl.ds(pl.multiple_of(other * HALF, 128), HALF)
    pairs = [(tok_h, tok), (rw_h, rw), (wg_h, wg), (wu_h, wu), (wd_h.at[:, mine], wd.at[core])]
    loads = [pltpu.make_async_copy(src, dst, load_sem.at[k]) for k, (src, dst) in enumerate(pairs)]
    for cp in loads:
        cp.start()

    barrier = pltpu.get_barrier_semaphore()
    friends = [(ps, y * 2 + core, pe) for ps, pe, _ in plane[1:]]
    friends += [(ps, y * 2 + other, pe) for ps, pe, _ in plane]
    friends += [up, down, far]
    for dev in friends:
        pl.semaphore_signal(barrier, inc=1, device_id=dev, device_id_type=MESH)

    lane = iota((TOKS, TOKS), 1)
    sub = iota((TOKS, TOKS), 0)
    hit = jnp.zeros((TOKS, TOKS), F32)
    for k in range(TOP):
        hit = hit + jnp.where(routes_ref[k : k + 1, :] == (sub >> 3), 1.0, 0.0)
    before = jnp.where(sub < lane, 1.0, 0.0).astype(BF16)
    rank = dot(hit.astype(BF16), before)
    place = jnp.where(rank == (sub & 7).astype(F32), hit, 0.0)
    disp[...] = place.astype(BF16)
    si, sl = iota((ROWS, TOKS), 0), iota((ROWS, TOKS), 1)
    sel[...] = jnp.where((si == (sl >> 3) * CAP + (sl & 7)) & ((sl & 7) < CAP), 1.0, 0.0).astype(BF16)

    with jax.named_scope("w_bar"):
        pl.semaphore_wait(barrier, len(friends))
        loads[0].wait()

    def a_copy(j, i):
        ps, pe, pm = plane[i]
        return rcopy(asend.at[j, pm], arecv.at[j, me], a_send, a_recv.at[j], (ps, cx, pe))

    def dispatch(j):
        cols = pl.ds(pl.multiple_of(j * C, 128), C)
        rows = dot(disp[...], tok[:, cols])
        asend[j] = rows.reshape(FLIGHT, PAD, C).astype(BF16)
        for i in range(1, 16):
            a_copy(j, i).start()
        arecv[j, me] = asend[j, me]

    def dispatch_first(j, carry):
        with jax.named_scope("disp"):
            dispatch(j)
        return carry

    hc = C // 2
    left, right = pl.ds(0, hc), pl.ds(hc, hc)

    def y_near(p, step):
        return rcopy(yb.at[p, 0], yb.at[p, 1 if step == 1 else 2], y_send.at[0], y1.at[p], up if step == 1 else down)

    def y_far(p, step):
        half, rel, dev = (left, 1, up) if step == 1 else (right, 2, down)
        return rcopy(yb.at[p, rel, :, half], yb.at[p, 3, :, half], y_send.at[0], y3.at[p], dev)

    with jax.named_scope("pre"):
        compact = dot(sel[...], disp[...]).astype(BF16)
        for p in range(NP):
            cols = slice((NR + p) * C, (NR + p + 1) * C)
            yb[p, 0] = dot(compact, tok[:, cols]).astype(BF16)
            y_near(p, 1).start()
            y_near(p, 3).start()

    lax.fori_loop(0, AHEAD, dispatch_first, 0)
    wdx = rcopy(wd_h.at[:, theirs], wd.at[core], wdx_sem.at[0], wdx_sem.at[1], peer)
    wdx.start()
    with jax.named_scope("w_wts"):
        for rel in range(4):
            q = iota((MSG * FLIGHT, ROWS), 1)
            q = ((q * 205) >> 10) * (MSG - CAP) + q + CAP * rel
            pack[rel] = jnp.where(q == iota((MSG * FLIGHT, ROWS), 0), 1.0, 0.0).astype(BF16)
            q = iota((ROWS, MSG * FLIGHT), 0)
            q = ((q * 205) >> 10) * (MSG - CAP) + q + CAP * rel
            unpack[rel] = jnp.where(q == iota((ROWS, MSG * FLIGHT), 1), 1.0, 0.0).astype(BF16)
        ei, el = iota((TOKS, ROWS), 1), iota((TOKS, ROWS), 0)
        exd[...] = jnp.where((ei == (el >> 3) * CAP + (el & 7)) & ((el & 7) < CAP), 1.0, 0.0).astype(BF16)
        logits[...] = jnp.zeros_like(logits)
        accg[...] = jnp.zeros_like(accg)
        accu[...] = jnp.zeros_like(accu)
        ghi[...] = disp[...].astype(F32).T.astype(BF16)
        for cp in loads[1:4]:
            cp.wait()

    def y_relay(p):
        two = yb.at[p, pl.ds(0, 2)]
        rcopy(two, two, y_send.at[0], y1.at[p], peer).wait_recv()
        y_far(p, 1).start()
        y_far(p, 3).start()

    with jax.named_scope("w_y1"):
        for p in range(YPRE):
            y_relay(p)

    def y_message(p, i):
        ps, pe, pm = plane[i]
        return rcopy(ys.at[p, pm], yr.at[p, me], y_send.at[1], ym.at[p], (ps, cx, pe))

    def y_messages(p):
        with jax.named_scope("w_y3"):
            rcopy(yb.at[p, 0], yb.at[p, 0], y_send.at[0], y3.at[p], peer).wait_recv()
        v = dot(pack[0], yb[p, 0])
        for rel in range(1, 4):
            v = v + dot(pack[rel], yb[p, rel])
        ys[p] = v.reshape(FLIGHT, MSG, C).astype(BF16)
        for i in range(1, 16):
            y_message(p, i).start()
        yr[p, me] = ys[p, me]
        cols = pl.ds(pl.multiple_of((NR + p) * C, 128), C)
        logits[...] += dot(tok[:, cols], rw[cols, :])

    def y_arrived(p):
        with jax.named_scope("w_ym"):
            most = yr.at[p, pl.ds(0, 15)]
            rcopy(most, most, y_send.at[1], ym.at[p], peer).wait_recv()
        got = yr[p].astype(F32).reshape(FLIGHT * MSG, C).astype(BF16)
        for rel in range(4):
            xb[NR + p, slot(rel, core)] = dot(unpack[rel], got).astype(BF16)
            g_peer(NR + p, rel).start()

    def slot(rel, c):
        return (c, 2 + 2 * c, 5 - 2 * c, 6 + c)[rel]

    def g_own_up(j):
        return rcopy(xb.at[j, core], xb.at[j, slot(1, core)], g_send.at[0], g1.at[j], up)

    def g_own_down(j):
        return rcopy(xb.at[j, core], xb.at[j, slot(2, core)], g_send.at[1], g1.at[j], down)

    def g_far_up(j):
        return rcopy(xb.at[j, slot(1, core), :, left], xb.at[j, 6 + core, :, left], g_send.at[2], g3.at[j], up)

    def g_far_down(j):
        return rcopy(xb.at[j, slot(2, core), :, right], xb.at[j, 6 + core, :, right], g_send.at[3], g3.at[j], down)

    def g_peer(j, rel):
        at = slot(rel, core)
        return rcopy(xb.at[j, at], xb.at[j, at], g_send.at[4 + rel], gd.at[rel // 3, j], peer)

    def g_peer_wait(j, rel):
        blocks = xb.at[j, pl.ds(0, 1 if rel == 3 else 3)]
        rcopy(blocks, blocks, g_send.at[4], gd.at[rel // 3, j], peer).wait_recv()

    def multiply(j, rel):
        rows = pl.ds(pl.multiple_of(j * C, 128), C)
        at = slice(rel * 2 * ROWS, (rel + 1) * 2 * ROWS)
        v = xb[j, 2 * rel : 2 * rel + 2].reshape(2 * ROWS, C)
        accg[at, :] += dot(v, wg[rows, :])
        accu[at, :] += dot(v, wu[rows, :])

    def relay(j):
        g_far_up(j).start()
        g_far_down(j).start()

    def relay_arrived(j):
        rcopy(xb.at[j, 0], xb.at[j, 0], g_send.at[0], g3.at[j], peer).wait_recv()
        g_peer(j, 3).start()

    def multiply_near(j):
        with jax.named_scope("w_d"):
            g_peer_wait(j, 0)
        for rel in range(3):
            multiply(j, rel)

    def multiply_far(j):
        g_peer_wait(j, 3)
        multiply(j, 3)

    def st_a(i, rel):
        ps, pe, pm = plane[i]
        cc = core if rel == 0 else other
        return rcopy(sta.at[0], str_.at[core * 16 + me], st_send.at[0], st_recv.at[0], (ps, y * 2 + cc, pe))

    def st_b(dev):
        return rcopy(sta.at[1], stb.at[y], st_send.at[1], st_recv.at[1], dev)

    all_a = rcopy(str_.at[pl.ds(0, 15)], str_.at[pl.ds(0, 15)], st_send.at[0], st_recv.at[0], peer)
    all_b = rcopy(stb.at[pl.ds(0, 3)], stb.at[pl.ds(0, 3)], st_send.at[1], st_recv.at[1], peer)

    def statistics():
        scores = jax.nn.sigmoid(logits[...])
        eye = iota((EXPERTS, TOKS), 0)
        named = jnp.zeros((EXPERTS, TOKS), F32)
        for k in range(TOP):
            named = named + jnp.where(routes_ref[k : k + 1, :] == eye, 1.0, 0.0)
        named = named.T
        affinity = scores / jnp.sum(scores, axis=1, keepdims=True)
        sta[0, 0:1, :] = jnp.sum(affinity, axis=0, keepdims=True)
        sta[0, 1:2, :] = jnp.sum(named, axis=0, keepdims=True)
        total = jnp.sum(jnp.where(named > 0.0, scores, 0.0), axis=1, keepdims=True)
        weights = scores / total * 2.5
        spread = jnp.where(iota((EXPERTS, TOKS), 0) == (iota((EXPERTS, TOKS), 1) >> 3), 1.0, 0.0)
        wide = jnp.dot(weights, spread, preferred_element_type=F32, precision=lax.Precision.HIGHEST)
        g = jnp.where(ghi[...].astype(F32) > 0.0, wide, 0.0)
        hi = g.astype(BF16)
        ghi[...] = hi
        lo = (g - hi.astype(F32)).astype(BF16)
        glo[...] = lo
        khi[...] = dot(hi, exd[...]).astype(BF16)
        klo[...] = dot(lo, exd[...]).astype(BF16)
        for rel in range(2):
            for i in range(0, 16, 2):
                if (rel, i) != (0, 0):
                    st_a(i, rel).start()

    def statistics_next():
        all_a.wait_recv()
        str_[core * 16 + me] = sta[0]
        acc = jnp.zeros((2, EXPERTS), F32)
        for cc in range(2):
            for e in range(8):
                acc = acc + str_[cc * 16 + s * 8 + e]
        sta[1] = acc
        stb[y] = acc
        for dev in (up, down, far):
            st_b(dev).start()

    def gather(i, carry):
        @stage(i + AHEAD < NR, "disp")
        def _():
            dispatch(i + AHEAD)

        @stage(i < NR, "fa")
        def _():
            j = i
            with jax.named_scope("w_a"):
                rcopy(
                    asend.at[j, pl.ds(0, 15)], arecv.at[j, pl.ds(0, 15)], a_send, a_recv.at[j], peer
                ).wait_recv()
            got = arecv[j].astype(F32).reshape(TOKS, C).astype(BF16)
            xb[j, core] = dot(sel[...], got).astype(BF16)
            g_own_up(j).start()
            g_own_down(j).start()
            g_peer(j, 0).start()
            cols = pl.ds(pl.multiple_of(j * C, 128), C)
            logits[...] += dot(tok[:, cols], rw[cols, :])

        @stage(i < NP - YPRE, "w_y1")
        def _():
            y_relay(i + YPRE)

        @stage((i >= LAG) & (i < NR), "ff")
        def _():
            relay(i - LAG)

        @stage((i >= NEAR) & (i < NR + NEAR), "fn")
        def _():
            j = i - NEAR
            with jax.named_scope("w_g1"):
                two = xb.at[j, pl.ds(0, 2)]
                rcopy(two, two, g_send.at[0], g1.at[j], peer).wait_recv()
            g_peer(j, 1).start()
            g_peer(j, 2).start()

        @stage(i == NR, "ff")
        def _():
            for j in range(NR - LAG, NR - NEAR + 1):
                relay(j)

        @stage((i >= NR - AHEAD) & (i < NC - AHEAD), "ymsg")
        def _():
            y_messages(i - NR + AHEAD)

        @stage((i >= NR - YARR) & (i < NC - YARR), "yarr")
        def _():
            y_arrived(i - NR + YARR)

        @stage(i == NR + 1, "stat")
        def _():
            statistics()

        @stage((i > NR) & (i < NR + NEAR), "ff")
        def _():
            relay(i - NEAR)

        @stage((i > NEAR) & (i < NR + NEAR), "fm")
        def _():
            multiply_near(i - NEAR - 1)

        @stage(i == NR + NEAR - 1, "fm")
        def _():
            for j in range(NR, NC):
                multiply_near(j)

        @stage(i == NR + NEAR, "fm")
        def _():
            multiply_near(NR - 1)

        @stage(i >= FAR, "fc")
        def _():
            with jax.named_scope("w_g3"):
                relay_arrived(i - FAR)

        @stage((i > FAR) & (i <= FAR + EARLY), "fmf")
        def _():
            multiply_far(i - FAR - 1)

        return carry

    lax.fori_loop(0, NR + NEAR + 1, gather, 0)

    def hidden(lo, n, k):
        at = pl.ds(lo, n)
        gate = accg[at, :]
        hb[core, at, :] = (gate * jax.nn.sigmoid(gate) * accu[at, :]).astype(BF16)
        h_copy(lo, n, k, core).start()

    def h_copy(lo, n, k, slot):
        at = pl.ds(lo, n)
        return rcopy(hb.at[core, at, :], hb.at[slot, at, :], h_sem.at[0, k], h_sem.at[1, k], peer)

    near_rows, far_rows = 6 * ROWS, 2 * ROWS
    with jax.named_scope("hn"):
        hidden(0, near_rows, 0)
    with jax.named_scope("w_h"):
        loads[4].wait()
        wdx.wait_recv()
        h_copy(0, near_rows, 0, other).wait_recv()

    def chunk(m):
        return pl.ds(pl.multiple_of(m * CM, 128), CM)

    def down_rows(lo, n, m):
        at = slice(lo * ROWS, (lo + n) * ROWS)
        cols = chunk(m)
        return dot(hb[0, at, :], wd[0, :, cols]) + dot(hb[1, at, :], wd[1, :, cols])

    def rows_of(slots, m):
        at = slice(slots * ROWS, (slots + 2) * ROWS)

        @pl.when(m < NB)
        def _():
            vbuf[...] = down_rows(slots, 2, m)

        @pl.when(m >= NB)
        def _():
            vbuf[...] = lp[m - NB, at, :].astype(F32)

        return vbuf[...]

    def l_copy(q, rel, i):
        ps, pe, pm = plane[i]
        cc = core if rel == 0 else other
        return rcopy(ls.at[q, cc, pm], lr.at[q, core * 16 + me], l_send, lm.at[q], (ps, y * 2 + cc, pe))

    def reorder():
        for half in range(2):
            for c in range(2):
                v = jnp.zeros((MSG * FLIGHT, HID), F32)
                for rel in range(4):
                    at = slice(SLOT[rel][c] * ROWS, (SLOT[rel][c] + 1) * ROWS)
                    v = v + dot(pack[rel], hb[half, at, :])
                hp[half, c * MSG * FLIGHT : (c + 1) * MSG * FLIGHT, :] = v.astype(BF16)

    def go_home(q):
        cols = chunk(NB + q)
        v = dot(hp[0], wd[0, :, cols]) + dot(hp[1], wd[1, :, cols])
        ls[q] = v.reshape(2, FLIGHT, MSG, CM).astype(BF16)
        for i in range(16):
            for rel in range(2):
                if (rel, i) != (0, 0):
                    l_copy(q, rel, i).start()
        lr[q, core * 16 + me] = ls[q, core, me]

    def came_home(q):
        most = lr.at[q, pl.ds(0, 31)]
        rcopy(most, most, l_send, lm.at[q], peer).wait_recv()
        for half in range(2):
            got = lr[q, half * 16 : half * 16 + 16].astype(F32).reshape(FLIGHT * MSG, CM).astype(BF16)
            for rel in range(4):
                at = slice(SLOT[rel][half] * ROWS, (SLOT[rel][half] + 1) * ROWS)
                lp[q, at, :] = dot(unpack[rel], got).astype(BF16)

    def b_up(m, k):
        return rcopy(nu.at[m, k], f1.at[m, k], b_send.at[k], b_f.at[m], up)

    def b_down(m, k):
        return rcopy(nd.at[m, k], f2.at[m, k], b_send.at[2 + k], b_f.at[m], down)

    def b_far_up(m):
        return rcopy(t3.at[0, m], s3.at[0, m], b_send.at[4], b_s.at[m], up)

    def b_far_down(m):
        return rcopy(t3.at[1, m], s3.at[1, m], b_send.at[5], b_s.at[m], down)

    def independent(m):
        v = rows_of(2, m)
        nd[m, 0] = v[:ROWS].astype(BF16)
        b_down(m, 0).start()
        nu[m, 1] = v[ROWS:].astype(BF16)
        b_up(m, 1).start()

    def ind(q):
        with jax.named_scope("ind"):
            independent(q)

    waiting = list(range(NR + NEAR + 1 - FAR, NR))
    ready = list(range(EARLY, NR + NEAR + 1 - FAR)) + list(range(NR, NC))
    ind(0)
    for q in range(1, FIRST):
        ind(q)
        for j in waiting[: 1 + (q > 2)]:
            with jax.named_scope("w_g3"):
                relay_arrived(j)
            ready.append(j)
        waiting = waiting[1 + (q > 2) :]
        with jax.named_scope("fmf"):
            for j in ready[:2] if len(ready) > 2 else []:
                multiply_far(j)
            if len(ready) > 2:
                ready = ready[2:]
    with jax.named_scope("fmf"):
        for j in waiting:
            relay_arrived(j)
            ready.append(j)
        for j in ready:
            multiply_far(j)
    with jax.named_scope("hf"):
        hidden(near_rows, far_rows, 1)
    with jax.named_scope("w_hf"):
        h_copy(near_rows, far_rows, 1, other).wait_recv()

    def r_copy(m, rel, i):
        ps, pe, pm = plane[i]
        cc = core if rel == 0 else other
        return rcopy(rsend.at[m, cc, pm], rrecv.at[m, core * 16 + me], r_send.at[rel], r_recv.at[m], (ps, y * 2 + cc, pe))

    def last(q):
        for half in range(2):
            v = hr[q, half]
            cols = pl.ds(pl.multiple_of(half * HALF + (NB + q) * CM, 128), CM)
            out_ref[:, cols] = (dot(khi[...], v) + dot(klo[...], v)).astype(BF16)

    def backward(i, carry):
        @stage((i >= NB) & (i < NM), "homew")
        def _():
            came_home(i - NB)

        @stage(i < NM, "bt")
        def _():
            m = i
            v = rows_of(6, m)
            t3[0, m] = v[:ROWS].astype(BF16)
            t3[1, m] = v[ROWS:].astype(BF16)
            b_far_up(m).start()
            b_far_down(m).start()

        @stage((lax.rem(i, 2) == 1) & (i < 2 * (NB - FIRST)), "bi")
        def _():
            independent(FIRST + lax.div(i, 2))

        @stage(i == 1, "home")
        def _():
            reorder()

        @stage((i >= 1) & (i <= NL), "home")
        def _():
            go_home(i - 1)

        @stage((i >= NB + LEAD) & (i < NM + LEAD), "bi")
        def _():
            independent(i - LEAD)

        @stage((i >= LEAD) & (i < NM + LEAD), "bb")
        def _():
            m = i - LEAD
            v = rows_of(4, m)
            with jax.named_scope("w_s"):
                rcopy(nu.at[m], nu.at[m], b_send.at[0], b_s.at[m], peer).wait_recv()
            nu[m, 0] = (v[ROWS:] + s3[0, m].astype(F32)).astype(BF16)
            b_up(m, 0).start()
            nd[m, 1] = (v[:ROWS] + s3[1, m].astype(F32)).astype(BF16)
            b_down(m, 1).start()

        @stage(i == LEAD - 1, "stat")
        def _():
            statistics_next()

        @stage((i >= LEAD + SUM) & (i < NM + LEAD + SUM), "bc")
        def _():
            m = i - LEAD - SUM
            v = rows_of(0, m)
            with jax.named_scope("w_f"):
                four = nu.at[pl.ds(0, 2)]
                rcopy(four, four, b_send.at[0], b_f.at[m], peer).wait_recv()
            r = [
                (v[c * ROWS : (c + 1) * ROWS] + f1[m, c].astype(F32) + f2[m, c].astype(F32)).astype(BF16)
                for c in range(2)
            ]

            @pl.when(m < NB)
            def _():
                for c in range(2):
                    rsend[m, c] = dot(exd[...], r[c]).reshape(FLIGHT, PAD, CM).astype(BF16)
                for i2 in range(16):
                    for rel in range(2):
                        if (rel, i2) != (0, 0):
                            r_copy(m, rel, i2).start()
                rrecv[m, core * 16 + me] = rsend[m, core, me]

            @pl.when(m >= NB)
            def _():
                for c in range(2):
                    hr[m - NB, c] = r[c]

        @stage((i >= NB + LEAD + SUM + 1) & (i < NM + LEAD + SUM), "last")
        def _():
            last(i - NB - LEAD - SUM - 1)

        @stage((i >= LEAD + BACK) & (i < NB + LEAD + BACK), "br")
        def _():
            m = i - LEAD - BACK
            with jax.named_scope("w_r"):
                most = rrecv.at[m, pl.ds(0, 31)]
                rcopy(most, most, r_send.at[0], r_recv.at[m], peer).wait_recv()
            for half in range(2):
                v = rrecv[m, half * 16 : half * 16 + 16].astype(F32).reshape(TOKS, CM).astype(BF16)
                cols = pl.ds(pl.multiple_of(half * HALF + m * CM, 128), CM)
                out_ref[:, cols] = (dot(ghi[...], v) + dot(glo[...], v)).astype(BF16)

        return carry

    lax.fori_loop(0, max(NB + LEAD + BACK, NM + LEAD + SUM), backward, 0)

    last(NL - 1)

    with jax.named_scope("fin"):
        all_b.wait_recv()
        tot = stb[0] + stb[1] + stb[2] + stb[3]
        bal_ref[...] = tot[1:2, :] * (EXPERTS / (TOP * LENGTH)) * (tot[0:1, :] / LENGTH) * EXPERTS

        wdx.wait_send()
        h_copy(0, near_rows, 0, core).wait_send()
        h_copy(near_rows, far_rows, 1, core).wait_send()
        all_a.wait_send()
        all_b.wait_send()

        def left_(src, sem):
            rcopy(src, src, sem, r_recv.at[0], peer).wait_send()

        left_(asend.at[:, pl.ds(0, 15)], a_send)
        some = pl.ds(0, NR)
        left_(xb.at[some, core], g_send.at[0])
        left_(xb.at[some, core], g_send.at[1])
        left_(xb.at[some, core, :, left], g_send.at[2])
        left_(xb.at[some, core, :, left], g_send.at[3])
        left_(yb.at[:, pl.ds(0, 3)], y_send.at[0])
        left_(ys.at[:, pl.ds(0, 15)], y_send.at[1])
        for rel in range(4):
            left_(xb.at[:, core], g_send.at[4 + rel])
        for k in range(6):
            left_(t3.at[0], b_send.at[k])
        left_(lr.at[:, pl.ds(0, 31)], l_send)
        left_(rsend.at[:, 0, pl.ds(0, 15)], r_send.at[0])
        left_(rsend.at[:, 0], r_send.at[1])


def on_device(tokens, routing, router_weight, w_gate, w_up, w_down):
    hbm = pl.BlockSpec(memory_space=pltpu.HBM)
    vmem = pl.BlockSpec(memory_space=pltpu.VMEM)
    V = pltpu.VMEM
    dma = pltpu.SemaphoreType.DMA
    out, bal = pl.pallas_call(
        kernel,
        out_shape=(
            jax.ShapeDtypeStruct((TOKS, D), BF16),
            jax.ShapeDtypeStruct((1, EXPERTS), F32),
        ),
        in_specs=[hbm, vmem, hbm, hbm, hbm, hbm],
        out_specs=(vmem, vmem),
        scratch_shapes=[
            V((TOKS, D), BF16),
            V((D, EXPERTS), BF16),
            V((D, HID), BF16),
            V((D, HID), BF16),
            V((2, HID, HALF), BF16),
            V((TOKS, TOKS), BF16),
            V((ROWS, TOKS), BF16),
            V((TOKS, ROWS), BF16),
            V((4, MSG * FLIGHT, ROWS), BF16),
            V((4, ROWS, MSG * FLIGHT), BF16),
            V((NP, 4, ROWS, C), BF16),
            V((NP, FLIGHT, MSG, C), BF16),
            V((NP, FLIGHT, MSG, C), BF16),
            V((TOKS, TOKS), BF16),
            V((TOKS, TOKS), BF16),
            V((TOKS, EXPERTS), F32),
            V((NR, FLIGHT, PAD, C), BF16),
            V((NR, FLIGHT, PAD, C), BF16),
            V((NC, 8, ROWS, C), BF16),
            V((8 * ROWS, HID), F32),
            V((8 * ROWS, HID), F32),
            V((2, 8 * ROWS, HID), BF16),
            V((2, NM, ROWS, CM), BF16),
            V((2, NM, ROWS, CM), BF16),
            V((NM, 2, ROWS, CM), BF16),
            V((NM, 2, ROWS, CM), BF16),
            V((NM, 2, ROWS, CM), BF16),
            V((NM, 2, ROWS, CM), BF16),
            V((NB, 2, FLIGHT, PAD, CM), BF16),
            V((NB, 2 * FLIGHT, PAD, CM), BF16),
            V((2, 2 * MSG * FLIGHT, HID), BF16),
            V((NL, 2, FLIGHT, MSG, CM), BF16),
            V((NL, 2 * FLIGHT, MSG, CM), BF16),
            V((NL, 8 * ROWS, CM), BF16),
            V((NL, 2, ROWS, CM), BF16),
            V((2 * ROWS, CM), F32),
            V((TOKS, ROWS), BF16),
            V((TOKS, ROWS), BF16),
            V((2, 2, EXPERTS), F32),
            V((32, 2, EXPERTS), F32),
            V((4, 2, EXPERTS), F32),
            dma((5,)),
            dma((2,)),
            dma(()),
            dma((NR,)),
            dma((8,)),
            dma((NR,)),
            dma((NR,)),
            dma((2, NC)),
            dma((2, 2)),
            dma((6,)),
            dma((NM,)),
            dma((NM,)),
            dma((2,)),
            dma((NB,)),
            dma((2,)),
            dma((2,)),
            dma((2,)),
            dma((NP,)),
            dma((NP,)),
            dma((NP,)),
            dma(()),
            dma((NL,)),
        ],
        compiler_params=pltpu.CompilerParams(
            collective_id=0, has_side_effects=True, vmem_limit_bytes=52 * 1024 * 1024
        ),
    )(tokens[0], routing[0].T, router_weight, w_gate[0], w_up[0], w_down[0])
    return out[None], bal


def solution(mesh):
    placed = (
        P("seq", ("ctx", "exp"), None),
        P("seq", ("ctx", "exp"), None),
        P(),
        P(("seq", "exp"), None, "ctx"),
        P(("seq", "exp"), None, "ctx"),
        P(("seq", "exp"), "ctx", None),
    )
    return jax.shard_map(
        on_device,
        mesh=mesh,
        in_specs=placed,
        out_specs=(P("seq", ("ctx", "exp"), None), P("seq", None)),
        check_vma=False,
    )
```

```python
import jax
import jax.numpy as jnp
from jax import lax
from jax.experimental import pallas as pl
from jax.experimental.pallas import tpu as pltpu
from jax.sharding import PartitionSpec as P

MESH = pl.DeviceIdType.MESH
F32 = jnp.float32
BF16 = jnp.bfloat16

TOKS = 128
D = 7168
EXPERTS = 256
TOP = 8
FLIGHT = 16
CAP = 5
PAD = 8
HID = 256
ROWS = FLIGHT * CAP
LENGTH = 8192
HALF = D // 2

NC, C = 14, 512
NM, CM = 14, 256
NR = 12
NP = NC - NR
YPRE = 2
YARR = 0
MSG = 24
AHEAD = 6
NEAR = 3
LAG = 8
FAR = 12
EARLY = 2
NL = 3
NB = NM - NL
FIRST = 7
LEAD = 3
SUM = 3
BACK = 8


SLOT = ((0, 1), (2, 4), (5, 3), (6, 7))


def dot(a, b):
    return jnp.dot(a, b, preferred_element_type=F32)


def iota(shape, dim):
    return lax.broadcasted_iota(jnp.int32, shape, dim)


def stage(cond, name):
    def wrap(body):
        @pl.when(cond)
        def _():
            with jax.named_scope(name):
                body()

    return wrap


def kernel(
    tok_h, routes_ref, rw_h, wg_h, wu_h, wd_h,
    out_ref, bal_ref,
    tok, rw, wg, wu, wd, disp, sel, exd, pack, unpack, yb, ys, yr, ghi, glo, logits,
    asend, arecv, xb, accg, accu, hb,
    t3, s3, nu, nd, f1, f2, rsend, rrecv, hp, ls, lr, lp, hr, vbuf, khi, klo,
    sta, str_, stb,
    load_sem, wdx_sem, a_send, a_recv, g_send, g1, g3, gd,
    h_sem, b_send, b_s, b_f, r_send, r_recv, st_send, st_recv, y_send, y1, y3, ym, l_send, lm,
):
    s = lax.axis_index("seq")
    cx = lax.axis_index("ctx")
    ex = lax.axis_index("exp")
    core = lax.rem(cx, 2)
    other = 1 - core
    y = lax.div(cx, 2)
    zh = lax.div(ex, 4)
    xx = lax.rem(ex, 4)
    me = s * 8 + ex

    def at_y(step):
        return (s, lax.rem(y + step, 4) * 2 + core, ex)

    up, down, far = at_y(1), at_y(3), at_y(2)
    peer = (s, y * 2 + other, ex)

    plane = []
    for dx in range(4):
        for dh in range(2):
            for dl in range(2):
                ps = lax.rem(s + dl, 2)
                pe = lax.rem(zh + dh, 2) * 4 + lax.rem(xx + dx, 4)
                plane.append((ps, pe, ps * 8 + pe))

    def rcopy(src, dst, ssem, rsem, dev):
        return pltpu.make_async_remote_copy(
            src_ref=src, dst_ref=dst, send_sem=ssem, recv_sem=rsem, device_id=dev, device_id_type=MESH
        )

    mine = pl.ds(pl.multiple_of(core * HALF, 128), HALF)
    theirs = pl.ds(pl.multiple_of(other * HALF, 128), HALF)
    pairs = [(tok_h, tok), (rw_h, rw), (wg_h, wg), (wu_h, wu), (wd_h.at[:, mine], wd.at[core])]
    loads = [pltpu.make_async_copy(src, dst, load_sem.at[k]) for k, (src, dst) in enumerate(pairs)]
    for cp in loads:
        cp.start()

    barrier = pltpu.get_barrier_semaphore()
    away = sorted(range(16), key=lambda i: -(min(i // 4, 4 - i // 4) + 2 * (i // 2 % 2)))
    friends = [(plane[i][0], y * 2 + c, plane[i][1]) for i in away for c in (other, core) if i or c is other]
    friends += [far, up, down]
    for dev in friends:
        pl.semaphore_signal(barrier, inc=1, device_id=dev, device_id_type=MESH)

    lane = iota((TOKS, TOKS), 1)
    sub = iota((TOKS, TOKS), 0)
    hit = jnp.zeros((TOKS, TOKS), F32)
    for k in range(TOP):
        hit = hit + jnp.where(routes_ref[k : k + 1, :] == (sub >> 3), 1.0, 0.0)
    before = jnp.where(sub < lane, 1.0, 0.0).astype(BF16)
    rank = dot(hit.astype(BF16), before)
    place = jnp.where(rank == (sub & 7).astype(F32), hit, 0.0)
    disp[...] = place.astype(BF16)
    si, sl = iota((ROWS, TOKS), 0), iota((ROWS, TOKS), 1)
    sel[...] = jnp.where((si == (sl >> 3) * CAP + (sl & 7)) & ((sl & 7) < CAP), 1.0, 0.0).astype(BF16)

    with jax.named_scope("w_bar"):
        pl.semaphore_wait(barrier, len(friends))
        loads[0].wait()

    def a_copy(j, i):
        ps, pe, pm = plane[i]
        return rcopy(asend.at[j, pm], arecv.at[j, me], a_send, a_recv.at[j], (ps, cx, pe))

    def dispatch(j):
        cols = pl.ds(pl.multiple_of(j * C, 128), C)
        rows = dot(disp[...], tok[:, cols])
        asend[j] = rows.reshape(FLIGHT, PAD, C).astype(BF16)
        for i in range(1, 16):
            a_copy(j, i).start()
        arecv[j, me] = asend[j, me]

    def dispatch_first(j, carry):
        with jax.named_scope("disp"):
            dispatch(j)
        return carry

    hc = C // 2
    left, right = pl.ds(0, hc), pl.ds(hc, hc)

    def y_near(p, step):
        return rcopy(yb.at[p, 0], yb.at[p, 1 if step == 1 else 2], y_send.at[0], y1.at[p], up if step == 1 else down)

    def y_far(p, step):
        half, rel, dev = (left, 1, up) if step == 1 else (right, 2, down)
        return rcopy(yb.at[p, rel, :, half], yb.at[p, 3, :, half], y_send.at[0], y3.at[p], dev)

    with jax.named_scope("pre"):
        compact = dot(sel[...], disp[...]).astype(BF16)
        for p in range(NP):
            cols = slice((NR + p) * C, (NR + p + 1) * C)
            yb[p, 0] = dot(compact, tok[:, cols]).astype(BF16)
            y_near(p, 1).start()
            y_near(p, 3).start()

    lax.fori_loop(0, AHEAD, dispatch_first, 0)
    wdx = rcopy(wd_h.at[:, theirs], wd.at[core], wdx_sem.at[0], wdx_sem.at[1], peer)
    wdx.start()
    with jax.named_scope("w_wts"):
        for rel in range(4):
            q = iota((MSG * FLIGHT, ROWS), 1)
            q = ((q * 205) >> 10) * (MSG - CAP) + q + CAP * rel
            pack[rel] = jnp.where(q == iota((MSG * FLIGHT, ROWS), 0), 1.0, 0.0).astype(BF16)
            q = iota((ROWS, MSG * FLIGHT), 0)
            q = ((q * 205) >> 10) * (MSG - CAP) + q + CAP * rel
            unpack[rel] = jnp.where(q == iota((ROWS, MSG * FLIGHT), 1), 1.0, 0.0).astype(BF16)
        ei, el = iota((TOKS, ROWS), 1), iota((TOKS, ROWS), 0)
        exd[...] = jnp.where((ei == (el >> 3) * CAP + (el & 7)) & ((el & 7) < CAP), 1.0, 0.0).astype(BF16)
        logits[...] = jnp.zeros_like(logits)
        accg[...] = jnp.zeros_like(accg)
        accu[...] = jnp.zeros_like(accu)
        ghi[...] = disp[...].astype(F32).T.astype(BF16)
        for cp in loads[1:4]:
            cp.wait()

    def y_relay(p):
        two = yb.at[p, pl.ds(0, 2)]
        rcopy(two, two, y_send.at[0], y1.at[p], peer).wait_recv()
        y_far(p, 1).start()
        y_far(p, 3).start()

    with jax.named_scope("w_y1"):
        for p in range(YPRE):
            y_relay(p)

    def y_message(p, i):
        ps, pe, pm = plane[i]
        return rcopy(ys.at[p, pm], yr.at[p, me], y_send.at[1], ym.at[p], (ps, cx, pe))

    def y_messages(p):
        with jax.named_scope("w_y3"):
            rcopy(yb.at[p, 0], yb.at[p, 0], y_send.at[0], y3.at[p], peer).wait_recv()
        v = dot(pack[0], yb[p, 0])
        for rel in range(1, 4):
            v = v + dot(pack[rel], yb[p, rel])
        ys[p] = v.reshape(FLIGHT, MSG, C).astype(BF16)
        for i in range(1, 16):
            y_message(p, i).start()
        yr[p, me] = ys[p, me]
        cols = pl.ds(pl.multiple_of((NR + p) * C, 128), C)
        logits[...] += dot(tok[:, cols], rw[cols, :])

    def y_arrived(p):
        with jax.named_scope("w_ym"):
            most = yr.at[p, pl.ds(0, 15)]
            rcopy(most, most, y_send.at[1], ym.at[p], peer).wait_recv()
        got = yr[p].astype(F32).reshape(FLIGHT * MSG, C).astype(BF16)
        for rel in range(4):
            xb[NR + p, slot(rel, core)] = dot(unpack[rel], got).astype(BF16)
            g_peer(NR + p, rel).start()

    def slot(rel, c):
        return (c, 2 + 2 * c, 5 - 2 * c, 6 + c)[rel]

    def g_own_up(j):
        return rcopy(xb.at[j, core], xb.at[j, slot(1, core)], g_send.at[0], g1.at[j], up)

    def g_own_down(j):
        return rcopy(xb.at[j, core], xb.at[j, slot(2, core)], g_send.at[0], g1.at[j], down)

    def g_far_up(j):
        return rcopy(xb.at[j, slot(1, core), :, left], xb.at[j, 6 + core, :, left], g_send.at[0], g3.at[j], up)

    def g_far_down(j):
        return rcopy(xb.at[j, slot(2, core), :, right], xb.at[j, 6 + core, :, right], g_send.at[0], g3.at[j], down)

    def g_peer(j, rel):
        at = slot(rel, core)
        return rcopy(xb.at[j, at], xb.at[j, at], g_send.at[1], gd.at[rel // 3, j], peer)

    def g_peer_wait(j, rel):
        blocks = xb.at[j, pl.ds(0, 1 if rel == 3 else 3)]
        rcopy(blocks, blocks, g_send.at[1], gd.at[rel // 3, j], peer).wait_recv()

    def multiply(j, rel):
        rows = pl.ds(pl.multiple_of(j * C, 128), C)
        at = slice(rel * 2 * ROWS, (rel + 1) * 2 * ROWS)
        v = xb[j, 2 * rel : 2 * rel + 2].reshape(2 * ROWS, C)
        accg[at, :] += dot(v, wg[rows, :])
        accu[at, :] += dot(v, wu[rows, :])

    def relay(j):
        g_far_up(j).start()
        g_far_down(j).start()

    def relay_arrived(j):
        rcopy(xb.at[j, 0], xb.at[j, 0], g_send.at[0], g3.at[j], peer).wait_recv()
        g_peer(j, 3).start()

    def multiply_near(j):
        with jax.named_scope("w_d"):
            g_peer_wait(j, 0)
        for rel in range(3):
            multiply(j, rel)

    def multiply_far(j):
        g_peer_wait(j, 3)
        multiply(j, 3)

    def st_a(i, rel):
        ps, pe, pm = plane[i]
        cc = core if rel == 0 else other
        return rcopy(sta.at[0], str_.at[core * 16 + me], st_send.at[0], st_recv.at[0], (ps, y * 2 + cc, pe))

    def st_b(dev):
        return rcopy(sta.at[1], stb.at[y], st_send.at[1], st_recv.at[1], dev)

    all_a = rcopy(str_.at[pl.ds(0, 15)], str_.at[pl.ds(0, 15)], st_send.at[0], st_recv.at[0], peer)
    all_b = rcopy(stb.at[pl.ds(0, 3)], stb.at[pl.ds(0, 3)], st_send.at[1], st_recv.at[1], peer)

    def statistics():
        scores = jax.nn.sigmoid(logits[...])
        eye = iota((EXPERTS, TOKS), 0)
        named = jnp.zeros((EXPERTS, TOKS), F32)
        for k in range(TOP):
            named = named + jnp.where(routes_ref[k : k + 1, :] == eye, 1.0, 0.0)
        named = named.T
        affinity = scores / jnp.sum(scores, axis=1, keepdims=True)
        sta[0, 0:1, :] = jnp.sum(affinity, axis=0, keepdims=True)
        sta[0, 1:2, :] = jnp.sum(named, axis=0, keepdims=True)
        total = jnp.sum(jnp.where(named > 0.0, scores, 0.0), axis=1, keepdims=True)
        weights = scores / total * 2.5
        spread = jnp.where(iota((EXPERTS, TOKS), 0) == (iota((EXPERTS, TOKS), 1) >> 3), 1.0, 0.0)
        wide = jnp.dot(weights, spread, preferred_element_type=F32, precision=lax.Precision.HIGHEST)
        g = jnp.where(ghi[...].astype(F32) > 0.0, wide, 0.0)
        hi = g.astype(BF16)
        ghi[...] = hi
        lo = (g - hi.astype(F32)).astype(BF16)
        glo[...] = lo
        khi[...] = dot(hi, exd[...]).astype(BF16)
        klo[...] = dot(lo, exd[...]).astype(BF16)
        for rel in range(2):
            for i in range(0, 16, 2):
                if (rel, i) != (0, 0):
                    st_a(i, rel).start()

    def statistics_next():
        all_a.wait_recv()
        str_[core * 16 + me] = sta[0]
        acc = jnp.zeros((2, EXPERTS), F32)
        for cc in range(2):
            for e in range(8):
                acc = acc + str_[cc * 16 + s * 8 + e]
        sta[1] = acc
        stb[y] = acc
        for dev in (up, down, far):
            st_b(dev).start()

    def gather(i, carry):
        @stage(i + AHEAD < NR, "disp")
        def _():
            dispatch(i + AHEAD)

        @stage(i < NR, "fa")
        def _():
            j = i
            with jax.named_scope("w_a"):
                rcopy(
                    asend.at[j, pl.ds(0, 15)], arecv.at[j, pl.ds(0, 15)], a_send, a_recv.at[j], peer
                ).wait_recv()
            got = arecv[j].astype(F32).reshape(TOKS, C).astype(BF16)
            xb[j, core] = dot(sel[...], got).astype(BF16)
            g_own_up(j).start()
            g_own_down(j).start()
            g_peer(j, 0).start()
            cols = pl.ds(pl.multiple_of(j * C, 128), C)
            logits[...] += dot(tok[:, cols], rw[cols, :])

        @stage(i < NP - YPRE, "w_y1")
        def _():
            y_relay(i + YPRE)

        @stage((i >= LAG) & (i < NR), "ff")
        def _():
            relay(i - LAG)

        @stage((i >= NEAR) & (i < NR + NEAR), "fn")
        def _():
            j = i - NEAR
            with jax.named_scope("w_g1"):
                two = xb.at[j, pl.ds(0, 2)]
                rcopy(two, two, g_send.at[0], g1.at[j], peer).wait_recv()
            g_peer(j, 1).start()
            g_peer(j, 2).start()

        @stage(i == NR, "ff")
        def _():
            for j in range(NR - LAG, NR - NEAR + 1):
                relay(j)

        @stage((i >= NR - AHEAD) & (i < NC - AHEAD), "ymsg")
        def _():
            y_messages(i - NR + AHEAD)

        @stage((i >= NR - YARR) & (i < NC - YARR), "yarr")
        def _():
            y_arrived(i - NR + YARR)

        @stage(i == NR + 1, "stat")
        def _():
            statistics()

        @stage((i > NR) & (i < NR + NEAR), "ff")
        def _():
            relay(i - NEAR)

        @stage((i > NEAR) & (i < NR + NEAR), "fm")
        def _():
            multiply_near(i - NEAR - 1)

        @stage(i == NR + NEAR - 1, "fm")
        def _():
            for j in range(NR, NC):
                multiply_near(j)

        @stage(i == NR + NEAR, "fm")
        def _():
            multiply_near(NR - 1)

        @stage(i >= FAR, "fc")
        def _():
            with jax.named_scope("w_g3"):
                relay_arrived(i - FAR)

        @stage((i > FAR) & (i <= FAR + EARLY), "fmf")
        def _():
            multiply_far(i - FAR - 1)

        return carry

    lax.fori_loop(0, NR + NEAR + 1, gather, 0)

    def hidden(lo, n, k):
        at = pl.ds(lo, n)
        gate = accg[at, :]
        hb[core, at, :] = (gate * jax.nn.sigmoid(gate) * accu[at, :]).astype(BF16)
        h_copy(lo, n, k, core).start()

    def h_copy(lo, n, k, slot):
        at = pl.ds(lo, n)
        return rcopy(hb.at[core, at, :], hb.at[slot, at, :], h_sem.at[0, k], h_sem.at[1, k], peer)

    near_rows, far_rows = 6 * ROWS, 2 * ROWS
    with jax.named_scope("hn"):
        hidden(0, near_rows, 0)
    with jax.named_scope("w_h"):
        loads[4].wait()
        wdx.wait_recv()
        h_copy(0, near_rows, 0, other).wait_recv()

    def chunk(m):
        return pl.ds(pl.multiple_of(m * CM, 128), CM)

    def down_rows(lo, n, m):
        at = slice(lo * ROWS, (lo + n) * ROWS)
        cols = chunk(m)
        return dot(hb[0, at, :], wd[0, :, cols]) + dot(hb[1, at, :], wd[1, :, cols])

    def rows_of(slots, m):
        at = slice(slots * ROWS, (slots + 2) * ROWS)

        @pl.when(m < NB)
        def _():
            vbuf[...] = down_rows(slots, 2, m)

        @pl.when(m >= NB)
        def _():
            vbuf[...] = lp[m - NB, at, :].astype(F32)

        return vbuf[...]

    def l_copy(q, rel, i):
        ps, pe, pm = plane[i]
        cc = core if rel == 0 else other
        return rcopy(ls.at[q, cc, pm], lr.at[q, core * 16 + me], l_send, lm.at[q], (ps, y * 2 + cc, pe))

    def reorder():
        for half in range(2):
            for c in range(2):
                v = jnp.zeros((MSG * FLIGHT, HID), F32)
                for rel in range(4):
                    at = slice(SLOT[rel][c] * ROWS, (SLOT[rel][c] + 1) * ROWS)
                    v = v + dot(pack[rel], hb[half, at, :])
                hp[half, c * MSG * FLIGHT : (c + 1) * MSG * FLIGHT, :] = v.astype(BF16)

    def go_home(q):
        cols = chunk(NB + q)
        v = dot(hp[0], wd[0, :, cols]) + dot(hp[1], wd[1, :, cols])
        ls[q] = v.reshape(2, FLIGHT, MSG, CM).astype(BF16)
        for i in range(16):
            for rel in range(2):
                if (rel, i) != (0, 0):
                    l_copy(q, rel, i).start()
        lr[q, core * 16 + me] = ls[q, core, me]

    def came_home(q):
        most = lr.at[q, pl.ds(0, 31)]
        rcopy(most, most, l_send, lm.at[q], peer).wait_recv()
        for half in range(2):
            got = lr[q, half * 16 : half * 16 + 16].astype(F32).reshape(FLIGHT * MSG, CM).astype(BF16)
            for rel in range(4):
                at = slice(SLOT[rel][half] * ROWS, (SLOT[rel][half] + 1) * ROWS)
                lp[q, at, :] = dot(unpack[rel], got).astype(BF16)

    def b_up(m, k):
        return rcopy(nu.at[m, k], f1.at[m, k], b_send, b_f.at[m], up)

    def b_down(m, k):
        return rcopy(nd.at[m, k], f2.at[m, k], b_send, b_f.at[m], down)

    def b_far_up(m):
        return rcopy(t3.at[0, m], s3.at[0, m], b_send, b_s.at[m], up)

    def b_far_down(m):
        return rcopy(t3.at[1, m], s3.at[1, m], b_send, b_s.at[m], down)

    def independent(m):
        v = rows_of(2, m)
        nd[m, 0] = v[:ROWS].astype(BF16)
        b_down(m, 0).start()
        nu[m, 1] = v[ROWS:].astype(BF16)
        b_up(m, 1).start()

    def ind(q):
        with jax.named_scope("ind"):
            independent(q)

    waiting = list(range(NR + NEAR + 1 - FAR, NR))
    ready = list(range(EARLY, NR + NEAR + 1 - FAR)) + list(range(NR, NC))
    ind(0)
    for q in range(1, FIRST):
        ind(q)
        for j in waiting[: 1 + (q > 2)]:
            with jax.named_scope("w_g3"):
                relay_arrived(j)
            ready.append(j)
        waiting = waiting[1 + (q > 2) :]
        with jax.named_scope("fmf"):
            for j in ready[:2] if len(ready) > 2 else []:
                multiply_far(j)
            if len(ready) > 2:
                ready = ready[2:]
    with jax.named_scope("fmf"):
        for j in waiting:
            relay_arrived(j)
            ready.append(j)
        for j in ready:
            multiply_far(j)
    with jax.named_scope("hf"):
        hidden(near_rows, far_rows, 1)
    with jax.named_scope("w_hf"):
        h_copy(near_rows, far_rows, 1, other).wait_recv()

    def r_copy(m, rel, i):
        ps, pe, pm = plane[i]
        cc = core if rel == 0 else other
        return rcopy(rsend.at[m, cc, pm], rrecv.at[m, core * 16 + me], r_send.at[rel], r_recv.at[m], (ps, y * 2 + cc, pe))

    def last(q):
        for half in range(2):
            v = hr[q, half]
            cols = pl.ds(pl.multiple_of(half * HALF + (NB + q) * CM, 128), CM)
            out_ref[:, cols] = (dot(khi[...], v) + dot(klo[...], v)).astype(BF16)

    def backward(i, carry):
        @stage((i >= NB) & (i < NM), "homew")
        def _():
            came_home(i - NB)

        @stage(i < NM, "bt")
        def _():
            m = i
            v = rows_of(6, m)
            t3[0, m] = v[:ROWS].astype(BF16)
            t3[1, m] = v[ROWS:].astype(BF16)
            b_far_up(m).start()
            b_far_down(m).start()

        @stage((lax.rem(i, 2) == 1) & (i < 2 * (NB - FIRST)), "bi")
        def _():
            independent(FIRST + lax.div(i, 2))

        @stage(i == 1, "home")
        def _():
            reorder()

        @stage((i >= 1) & (i <= NL), "home")
        def _():
            go_home(i - 1)

        @stage((i >= NB + LEAD) & (i < NM + LEAD), "bi")
        def _():
            independent(i - LEAD)

        @stage((i >= LEAD) & (i < NM + LEAD), "bb")
        def _():
            m = i - LEAD
            v = rows_of(4, m)
            with jax.named_scope("w_s"):
                rcopy(nu.at[m], nu.at[m], b_send, b_s.at[m], peer).wait_recv()
            nu[m, 0] = (v[ROWS:] + s3[0, m].astype(F32)).astype(BF16)
            b_up(m, 0).start()
            nd[m, 1] = (v[:ROWS] + s3[1, m].astype(F32)).astype(BF16)
            b_down(m, 1).start()

        @stage(i == LEAD - 1, "stat")
        def _():
            statistics_next()

        @stage((i >= LEAD + SUM) & (i < NM + LEAD + SUM), "bc")
        def _():
            m = i - LEAD - SUM
            v = rows_of(0, m)
            with jax.named_scope("w_f"):
                four = nu.at[pl.ds(0, 2)]
                rcopy(four, four, b_send, b_f.at[m], peer).wait_recv()
            r = [
                (v[c * ROWS : (c + 1) * ROWS] + f1[m, c].astype(F32) + f2[m, c].astype(F32)).astype(BF16)
                for c in range(2)
            ]

            @pl.when(m < NB)
            def _():
                for c in range(2):
                    rsend[m, c] = dot(exd[...], r[c]).reshape(FLIGHT, PAD, CM).astype(BF16)
                for i2 in range(16):
                    for rel in range(2):
                        if (rel, i2) != (0, 0):
                            r_copy(m, rel, i2).start()
                rrecv[m, core * 16 + me] = rsend[m, core, me]

            @pl.when(m >= NB)
            def _():
                for c in range(2):
                    hr[m - NB, c] = r[c]

        @stage((i >= NB + LEAD + SUM + 1) & (i < NM + LEAD + SUM), "last")
        def _():
            last(i - NB - LEAD - SUM - 1)

        @stage((i >= LEAD + BACK) & (i < NB + LEAD + BACK), "br")
        def _():
            m = i - LEAD - BACK
            with jax.named_scope("w_r"):
                most = rrecv.at[m, pl.ds(0, 31)]
                rcopy(most, most, r_send.at[0], r_recv.at[m], peer).wait_recv()
            for half in range(2):
                v = rrecv[m, half * 16 : half * 16 + 16].astype(F32).reshape(TOKS, CM).astype(BF16)
                cols = pl.ds(pl.multiple_of(half * HALF + m * CM, 128), CM)
                out_ref[:, cols] = (dot(ghi[...], v) + dot(glo[...], v)).astype(BF16)

        return carry

    lax.fori_loop(0, max(NB + LEAD + BACK, NM + LEAD + SUM), backward, 0)

    last(NL - 1)

    with jax.named_scope("fin"):
        all_b.wait_recv()
        tot = stb[0] + stb[1] + stb[2] + stb[3]
        bal_ref[...] = tot[1:2, :] * (EXPERTS / (TOP * LENGTH)) * (tot[0:1, :] / LENGTH) * EXPERTS

        wdx.wait_send()
        h_copy(0, near_rows, 0, core).wait_send()
        h_copy(near_rows, far_rows, 1, core).wait_send()
        all_a.wait_send()
        all_b.wait_send()

        def left_(src, sem):
            rcopy(src, src, sem, r_recv.at[0], peer).wait_send()

        left_(asend.at[:, pl.ds(0, 15)], a_send)
        left_(xb.at[pl.ds(0, NR // 2), pl.ds(0, 6)], g_send.at[0])
        left_(xb.at[:, pl.ds(0, 4)], g_send.at[1])
        left_(yb.at[:, pl.ds(0, 3)], y_send.at[0])
        left_(ys.at[:, pl.ds(0, 15)], y_send.at[1])
        left_(xb.at[pl.ds(0, NM // 2), pl.ds(0, 6)], b_send)
        left_(lr.at[:, pl.ds(0, 31)], l_send)
        left_(rsend.at[:, 0, pl.ds(0, 15)], r_send.at[0])
        left_(rsend.at[:, 0], r_send.at[1])


def put_out(out_v, bal_v, out_h, bal_h, sem):
    parts = [pl.ds(k * 16, 16) for k in range(TOKS // 16)]
    copies = [pltpu.make_async_copy(out_v.at[p], out_h.at[p], sem.at[k]) for k, p in enumerate(parts)]
    copies.append(pltpu.make_async_copy(bal_v, bal_h, sem.at[len(parts)]))
    for cp in copies:
        cp.start()
    for cp in copies:
        cp.wait()


def on_device(tokens, routing, router_weight, w_gate, w_up, w_down):
    hbm = pl.BlockSpec(memory_space=pltpu.HBM)
    vmem = pl.BlockSpec(memory_space=pltpu.VMEM)
    V = pltpu.VMEM
    dma = pltpu.SemaphoreType.DMA
    out, bal = pl.pallas_call(
        kernel,
        out_shape=(
            jax.ShapeDtypeStruct((TOKS, D), BF16),
            jax.ShapeDtypeStruct((1, EXPERTS), F32),
        ),
        in_specs=[hbm, vmem, hbm, hbm, hbm, hbm],
        out_specs=(vmem, vmem),
        scratch_shapes=[
            V((TOKS, D), BF16),
            V((D, EXPERTS), BF16),
            V((D, HID), BF16),
            V((D, HID), BF16),
            V((2, HID, HALF), BF16),
            V((TOKS, TOKS), BF16),
            V((ROWS, TOKS), BF16),
            V((TOKS, ROWS), BF16),
            V((4, MSG * FLIGHT, ROWS), BF16),
            V((4, ROWS, MSG * FLIGHT), BF16),
            V((NP, 4, ROWS, C), BF16),
            V((NP, FLIGHT, MSG, C), BF16),
            V((NP, FLIGHT, MSG, C), BF16),
            V((TOKS, TOKS), BF16),
            V((TOKS, TOKS), BF16),
            V((TOKS, EXPERTS), F32),
            V((NR, FLIGHT, PAD, C), BF16),
            V((NR, FLIGHT, PAD, C), BF16),
            V((NC, 8, ROWS, C), BF16),
            V((8 * ROWS, HID), F32),
            V((8 * ROWS, HID), F32),
            V((2, 8 * ROWS, HID), BF16),
            V((2, NM, ROWS, CM), BF16),
            V((2, NM, ROWS, CM), BF16),
            V((NM, 2, ROWS, CM), BF16),
            V((NM, 2, ROWS, CM), BF16),
            V((NM, 2, ROWS, CM), BF16),
            V((NM, 2, ROWS, CM), BF16),
            V((NB, 2, FLIGHT, PAD, CM), BF16),
            V((NB, 2 * FLIGHT, PAD, CM), BF16),
            V((2, 2 * MSG * FLIGHT, HID), BF16),
            V((NL, 2, FLIGHT, MSG, CM), BF16),
            V((NL, 2 * FLIGHT, MSG, CM), BF16),
            V((NL, 8 * ROWS, CM), BF16),
            V((NL, 2, ROWS, CM), BF16),
            V((2 * ROWS, CM), F32),
            V((TOKS, ROWS), BF16),
            V((TOKS, ROWS), BF16),
            V((2, 2, EXPERTS), F32),
            V((32, 2, EXPERTS), F32),
            V((4, 2, EXPERTS), F32),
            dma((5,)),
            dma((2,)),
            dma(()),
            dma((NR,)),
            dma((2,)),
            dma((NR,)),
            dma((NR,)),
            dma((2, NC)),
            dma((2, 2)),
            dma(()),
            dma((NM,)),
            dma((NM,)),
            dma((2,)),
            dma((NB,)),
            dma((2,)),
            dma((2,)),
            dma((2,)),
            dma((NP,)),
            dma((NP,)),
            dma((NP,)),
            dma(()),
            dma((NL,)),
        ],
        compiler_params=pltpu.CompilerParams(
            collective_id=0, has_side_effects=True, vmem_limit_bytes=52 * 1024 * 1024
        ),
    )(tokens[0], routing[0].T, router_weight, w_gate[0], w_up[0], w_down[0])
    out, bal = pl.pallas_call(
        put_out,
        out_shape=(
            jax.ShapeDtypeStruct((TOKS, D), BF16),
            jax.ShapeDtypeStruct((1, EXPERTS), F32),
        ),
        in_specs=[vmem, vmem],
        out_specs=(hbm, hbm),
        scratch_shapes=[dma((TOKS // 16 + 1,))],
        compiler_params=pltpu.CompilerParams(vmem_limit_bytes=8 * 1024 * 1024),
    )(out, bal)
    return out[None], bal


def solution(mesh):
    placed = (
        P("seq", ("ctx", "exp"), None),
        P("seq", ("ctx", "exp"), None),
        P(),
        P(("seq", "exp"), None, "ctx"),
        P(("seq", "exp"), None, "ctx"),
        P(("seq", "exp"), "ctx", None),
    )
    return jax.shard_map(
        on_device,
        mesh=mesh,
        in_specs=placed,
        out_specs=(P("seq", ("ctx", "exp"), None), P("seq", None)),
        check_vma=False,
    )
```

```python
import jax
import jax.numpy as jnp
from jax import lax
from jax.experimental import pallas as pl
from jax.experimental.pallas import tpu as pltpu
from jax.sharding import PartitionSpec as P

MESH = pl.DeviceIdType.MESH
F32 = jnp.float32
BF16 = jnp.bfloat16

TOKS = 128
D = 7168
EXPERTS = 256
TOP = 8
FLIGHT = 16
CAP = 5
PAD = 8
HID = 256
ROWS = FLIGHT * CAP
LENGTH = 8192
HALF = D // 2

NC, C = 14, 512
NM, CM = 14, 256
NR = 12
NP = NC - NR
YPRE = 2
YARR = 0
MSG = 24
AHEAD = 6
NEAR = 3
LAG = 8
FAR = 12
EARLY = 2
NL = 3
NB = NM - NL
FIRST = 7
LEAD = 3
SUM = 3
BACK = 8


SLOT = ((0, 1), (2, 4), (5, 3), (6, 7))


def dot(a, b):
    return jnp.dot(a, b, preferred_element_type=F32)


def iota(shape, dim):
    return lax.broadcasted_iota(jnp.int32, shape, dim)


def stage(cond, name):
    def wrap(body):
        @pl.when(cond)
        def _():
            with jax.named_scope(name):
                body()

    return wrap


def kernel(
    tok_h, routes_ref, rw_h, wg_h, wu_h, wd_h,
    out_ref, bal_ref,
    tok, rw, wg, wu, wd, disp, sel, exd, pack, unpack, yb, ys, yr, ghi, both, logits,
    asend, arecv, xb, accg, accu, hb,
    t3, s3, nu, nd, f1, f2, rsend, rrecv, hp, ls, lr, lp, hr, vbuf, khi, klo,
    sta, str_, stb,
    load_sem, wdx_sem, a_send, a_recv, g_send, g1, g3, gd,
    h_sem, b_send, b_s, b_f, r_send, r_recv, st_send, st_recv, y_send, y1, y3, ym, l_send, lm,
):
    s = lax.axis_index("seq")
    cx = lax.axis_index("ctx")
    ex = lax.axis_index("exp")
    core = lax.rem(cx, 2)
    other = 1 - core
    y = lax.div(cx, 2)
    zh = lax.div(ex, 4)
    xx = lax.rem(ex, 4)
    me = s * 8 + ex

    def at_y(step):
        return (s, lax.rem(y + step, 4) * 2 + core, ex)

    up, down, far = at_y(1), at_y(3), at_y(2)
    peer = (s, y * 2 + other, ex)

    plane = []
    for dx in range(4):
        for dh in range(2):
            for dl in range(2):
                ps = lax.rem(s + dl, 2)
                pe = lax.rem(zh + dh, 2) * 4 + lax.rem(xx + dx, 4)
                plane.append((ps, pe, ps * 8 + pe))

    def rcopy(src, dst, ssem, rsem, dev):
        return pltpu.make_async_remote_copy(
            src_ref=src, dst_ref=dst, send_sem=ssem, recv_sem=rsem, device_id=dev, device_id_type=MESH
        )

    mine = pl.ds(pl.multiple_of(core * HALF, 128), HALF)
    theirs = pl.ds(pl.multiple_of(other * HALF, 128), HALF)
    pairs = [(tok_h, tok), (rw_h, rw), (wg_h, wg), (wu_h, wu), (wd_h.at[:, mine], wd.at[core])]
    loads = [pltpu.make_async_copy(src, dst, load_sem.at[k]) for k, (src, dst) in enumerate(pairs)]
    for cp in loads:
        cp.start()

    barrier = pltpu.get_barrier_semaphore()
    away = sorted(range(16), key=lambda i: -(min(i // 4, 4 - i // 4) + 2 * (i // 2 % 2)))
    friends = [(plane[i][0], y * 2 + c, plane[i][1]) for i in away for c in (other, core) if i or c is other]
    friends += [far, up, down]
    for dev in friends:
        pl.semaphore_signal(barrier, inc=1, device_id=dev, device_id_type=MESH)

    lane = iota((TOKS, TOKS), 1)
    sub = iota((TOKS, TOKS), 0)
    hit = jnp.zeros((TOKS, TOKS), F32)
    for k in range(TOP):
        hit = hit + jnp.where(routes_ref[k : k + 1, :] == (sub >> 3), 1.0, 0.0)
    before = jnp.where(sub < lane, 1.0, 0.0).astype(BF16)
    rank = dot(hit.astype(BF16), before)
    place = jnp.where(rank == (sub & 7).astype(F32), hit, 0.0)
    disp[...] = place.astype(BF16)
    si, sl = iota((ROWS, TOKS), 0), iota((ROWS, TOKS), 1)
    sel[...] = jnp.where((si == (sl >> 3) * CAP + (sl & 7)) & ((sl & 7) < CAP), 1.0, 0.0).astype(BF16)

    with jax.named_scope("w_bar"):
        pl.semaphore_wait(barrier, len(friends))
        loads[0].wait()

    def a_copy(j, i):
        ps, pe, pm = plane[i]
        return rcopy(asend.at[j, pm], arecv.at[j, me], a_send, a_recv.at[j], (ps, cx, pe))

    def dispatch(j):
        cols = pl.ds(pl.multiple_of(j * C, 128), C)
        rows = dot(disp[...], tok[:, cols])
        asend[j] = rows.reshape(FLIGHT, PAD, C).astype(BF16)
        for i in range(1, 16):
            a_copy(j, i).start()
        arecv[j, me] = asend[j, me]

    def dispatch_first(j, carry):
        with jax.named_scope("disp"):
            dispatch(j)
        return carry

    hc = C // 2
    left, right = pl.ds(0, hc), pl.ds(hc, hc)

    def y_near(p, step):
        return rcopy(yb.at[p, 0], yb.at[p, 1 if step == 1 else 2], y_send.at[0], y1.at[p], up if step == 1 else down)

    def y_far(p, step):
        half, rel, dev = (left, 1, up) if step == 1 else (right, 2, down)
        return rcopy(yb.at[p, rel, :, half], yb.at[p, 3, :, half], y_send.at[0], y3.at[p], dev)

    with jax.named_scope("pre"):
        compact = dot(sel[...], disp[...]).astype(BF16)
        for p in range(NP):
            cols = slice((NR + p) * C, (NR + p + 1) * C)
            yb[p, 0] = dot(compact, tok[:, cols]).astype(BF16)
            y_near(p, 1).start()
            y_near(p, 3).start()

    lax.fori_loop(0, AHEAD, dispatch_first, 0)
    wdx = rcopy(wd_h.at[:, theirs], wd.at[core], wdx_sem.at[0], wdx_sem.at[1], peer)
    wdx.start()
    with jax.named_scope("w_wts"):
        for rel in range(4):
            q = iota((MSG * FLIGHT, ROWS), 1)
            q = ((q * 205) >> 10) * (MSG - CAP) + q + CAP * rel
            pack[rel] = jnp.where(q == iota((MSG * FLIGHT, ROWS), 0), 1.0, 0.0).astype(BF16)
            q = iota((ROWS, MSG * FLIGHT), 0)
            q = ((q * 205) >> 10) * (MSG - CAP) + q + CAP * rel
            unpack[rel] = jnp.where(q == iota((ROWS, MSG * FLIGHT), 1), 1.0, 0.0).astype(BF16)
        ei, el = iota((TOKS, ROWS), 1), iota((TOKS, ROWS), 0)
        exd[...] = jnp.where((ei == (el >> 3) * CAP + (el & 7)) & ((el & 7) < CAP), 1.0, 0.0).astype(BF16)
        logits[...] = jnp.zeros_like(logits)
        accg[...] = jnp.zeros_like(accg)
        accu[...] = jnp.zeros_like(accu)
        ghi[...] = disp[...].astype(F32).T.astype(BF16)
        for cp in loads[1:4]:
            cp.wait()

    def y_relay(p):
        two = yb.at[p, pl.ds(0, 2)]
        rcopy(two, two, y_send.at[0], y1.at[p], peer).wait_recv()
        y_far(p, 1).start()
        y_far(p, 3).start()

    with jax.named_scope("w_y1"):
        for p in range(YPRE):
            y_relay(p)

    def y_message(p, i):
        ps, pe, pm = plane[i]
        return rcopy(ys.at[p, pm], yr.at[p, me], y_send.at[1], ym.at[p], (ps, cx, pe))

    def y_messages(p):
        with jax.named_scope("w_y3"):
            rcopy(yb.at[p, 0], yb.at[p, 0], y_send.at[0], y3.at[p], peer).wait_recv()
        v = dot(pack[0], yb[p, 0])
        for rel in range(1, 4):
            v = v + dot(pack[rel], yb[p, rel])
        ys[p] = v.reshape(FLIGHT, MSG, C).astype(BF16)
        for i in range(1, 16):
            y_message(p, i).start()
        yr[p, me] = ys[p, me]
        cols = pl.ds(pl.multiple_of((NR + p) * C, 128), C)
        logits[...] += dot(tok[:, cols], rw[cols, :])

    def y_arrived(p):
        with jax.named_scope("w_ym"):
            most = yr.at[p, pl.ds(0, 15)]
            rcopy(most, most, y_send.at[1], ym.at[p], peer).wait_recv()
        got = yr[p].astype(F32).reshape(FLIGHT * MSG, C).astype(BF16)
        for rel in range(4):
            xb[NR + p, slot(rel, core)] = dot(unpack[rel], got).astype(BF16)
            g_peer(NR + p, rel).start()

    def slot(rel, c):
        return (c, 2 + 2 * c, 5 - 2 * c, 6 + c)[rel]

    def g_own_up(j):
        return rcopy(xb.at[j, core], xb.at[j, slot(1, core)], g_send.at[0], g1.at[j], up)

    def g_own_down(j):
        return rcopy(xb.at[j, core], xb.at[j, slot(2, core)], g_send.at[0], g1.at[j], down)

    def g_far_up(j):
        return rcopy(xb.at[j, slot(1, core), :, left], xb.at[j, 6 + core, :, left], g_send.at[0], g3.at[j], up)

    def g_far_down(j):
        return rcopy(xb.at[j, slot(2, core), :, right], xb.at[j, 6 + core, :, right], g_send.at[0], g3.at[j], down)

    def g_peer(j, rel):
        at = slot(rel, core)
        return rcopy(xb.at[j, at], xb.at[j, at], g_send.at[1], gd.at[rel // 3, j], peer)

    def g_peer_wait(j, rel):
        blocks = xb.at[j, pl.ds(0, 1 if rel == 3 else 3)]
        rcopy(blocks, blocks, g_send.at[1], gd.at[rel // 3, j], peer).wait_recv()

    def multiply(j, rel):
        rows = pl.ds(pl.multiple_of(j * C, 128), C)
        at = slice(rel * 2 * ROWS, (rel + 1) * 2 * ROWS)
        v = xb[j, 2 * rel : 2 * rel + 2].reshape(2 * ROWS, C)
        accg[at, :] += dot(v, wg[rows, :])
        accu[at, :] += dot(v, wu[rows, :])

    def relay(j):
        g_far_up(j).start()
        g_far_down(j).start()

    def relay_arrived(j):
        rcopy(xb.at[j, 0], xb.at[j, 0], g_send.at[0], g3.at[j], peer).wait_recv()
        g_peer(j, 3).start()

    def multiply_near(j):
        with jax.named_scope("w_d"):
            g_peer_wait(j, 0)
        for rel in range(3):
            multiply(j, rel)

    def multiply_far(j):
        g_peer_wait(j, 3)
        multiply(j, 3)

    def st_a(i, rel):
        ps, pe, pm = plane[i]
        cc = core if rel == 0 else other
        return rcopy(sta.at[0], str_.at[core * 16 + me], st_send.at[0], st_recv.at[0], (ps, y * 2 + cc, pe))

    def st_b(dev):
        return rcopy(sta.at[1], stb.at[y], st_send.at[1], st_recv.at[1], dev)

    all_a = rcopy(str_.at[pl.ds(0, 15)], str_.at[pl.ds(0, 15)], st_send.at[0], st_recv.at[0], peer)
    all_b = rcopy(stb.at[pl.ds(0, 3)], stb.at[pl.ds(0, 3)], st_send.at[1], st_recv.at[1], peer)

    def statistics():
        scores = jax.nn.sigmoid(logits[...])
        eye = iota((EXPERTS, TOKS), 0)
        named = jnp.zeros((EXPERTS, TOKS), F32)
        for k in range(TOP):
            named = named + jnp.where(routes_ref[k : k + 1, :] == eye, 1.0, 0.0)
        named = named.T
        affinity = scores / jnp.sum(scores, axis=1, keepdims=True)
        sta[0, 0:1, :] = jnp.sum(affinity, axis=0, keepdims=True)
        sta[0, 1:2, :] = jnp.sum(named, axis=0, keepdims=True)
        total = jnp.sum(jnp.where(named > 0.0, scores, 0.0), axis=1, keepdims=True)
        weights = scores / total * 2.5
        spread = jnp.where(iota((EXPERTS, TOKS), 0) == (iota((EXPERTS, TOKS), 1) >> 3), 1.0, 0.0)
        wide = jnp.dot(weights, spread, preferred_element_type=F32, precision=lax.Precision.HIGHEST)
        g = jnp.where(ghi[...].astype(F32) > 0.0, wide, 0.0)
        hi = g.astype(BF16)
        both[:, :TOKS] = hi
        lo = (g - hi.astype(F32)).astype(BF16)
        both[:, TOKS:] = lo
        khi[...] = dot(hi, exd[...]).astype(BF16)
        klo[...] = dot(lo, exd[...]).astype(BF16)
        for rel in range(2):
            for i in range(0, 16, 2):
                if (rel, i) != (0, 0):
                    st_a(i, rel).start()

    def statistics_next():
        all_a.wait_recv()
        str_[core * 16 + me] = sta[0]
        acc = jnp.zeros((2, EXPERTS), F32)
        for cc in range(2):
            for e in range(8):
                acc = acc + str_[cc * 16 + s * 8 + e]
        sta[1] = acc
        stb[y] = acc
        for dev in (up, down, far):
            st_b(dev).start()

    def gather(i, carry):
        @stage(i + AHEAD < NR, "disp")
        def _():
            dispatch(i + AHEAD)

        @stage(i < NR, "fa")
        def _():
            j = i
            with jax.named_scope("w_a"):
                rcopy(
                    asend.at[j, pl.ds(0, 15)], arecv.at[j, pl.ds(0, 15)], a_send, a_recv.at[j], peer
                ).wait_recv()
            got = arecv[j].astype(F32).reshape(TOKS, C).astype(BF16)
            xb[j, core] = dot(sel[...], got).astype(BF16)
            g_own_up(j).start()
            g_own_down(j).start()
            g_peer(j, 0).start()
            cols = pl.ds(pl.multiple_of(j * C, 128), C)
            logits[...] += dot(tok[:, cols], rw[cols, :])

        @stage(i < NP - YPRE, "w_y1")
        def _():
            y_relay(i + YPRE)

        @stage((i >= LAG) & (i < NR), "ff")
        def _():
            relay(i - LAG)

        @stage((i >= NEAR) & (i < NR + NEAR), "fn")
        def _():
            j = i - NEAR
            with jax.named_scope("w_g1"):
                two = xb.at[j, pl.ds(0, 2)]
                rcopy(two, two, g_send.at[0], g1.at[j], peer).wait_recv()
            g_peer(j, 1).start()
            g_peer(j, 2).start()

        @stage(i == NR, "ff")
        def _():
            for j in range(NR - LAG, NR - NEAR + 1):
                relay(j)

        @stage((i >= NR - AHEAD) & (i < NC - AHEAD), "ymsg")
        def _():
            y_messages(i - NR + AHEAD)

        @stage((i >= NR - YARR) & (i < NC - YARR), "yarr")
        def _():
            y_arrived(i - NR + YARR)

        @stage(i == NR + 1, "stat")
        def _():
            statistics()

        @stage((i > NR) & (i < NR + NEAR), "ff")
        def _():
            relay(i - NEAR)

        @stage((i > NEAR) & (i < NR + NEAR), "fm")
        def _():
            multiply_near(i - NEAR - 1)

        @stage(i == NR + NEAR - 1, "fm")
        def _():
            for j in range(NR, NC):
                multiply_near(j)

        @stage(i == NR + NEAR, "fm")
        def _():
            multiply_near(NR - 1)

        @stage(i >= FAR, "fc")
        def _():
            with jax.named_scope("w_g3"):
                relay_arrived(i - FAR)

        @stage((i > FAR) & (i <= FAR + EARLY), "fmf")
        def _():
            multiply_far(i - FAR - 1)

        return carry

    lax.fori_loop(0, NR + NEAR + 1, gather, 0)

    def hidden(lo, n, k):
        at = pl.ds(lo, n)
        gate = accg[at, :]
        hb[core, at, :] = (gate * jax.nn.sigmoid(gate) * accu[at, :]).astype(BF16)
        h_copy(lo, n, k, core).start()

    def h_copy(lo, n, k, slot):
        at = pl.ds(lo, n)
        return rcopy(hb.at[core, at, :], hb.at[slot, at, :], h_sem.at[0, k], h_sem.at[1, k], peer)

    near_rows, far_rows = 6 * ROWS, 2 * ROWS
    with jax.named_scope("hn"):
        hidden(0, near_rows, 0)
    with jax.named_scope("w_h"):
        loads[4].wait()
        wdx.wait_recv()
        h_copy(0, near_rows, 0, other).wait_recv()

    def chunk(m):
        return pl.ds(pl.multiple_of(m * CM, 128), CM)

    def down_rows(lo, n, m):
        at = slice(lo * ROWS, (lo + n) * ROWS)
        cols = chunk(m)
        return dot(hb[0, at, :], wd[0, :, cols]) + dot(hb[1, at, :], wd[1, :, cols])

    def rows_of(slots, m):
        at = slice(slots * ROWS, (slots + 2) * ROWS)

        @pl.when(m < NB)
        def _():
            vbuf[...] = down_rows(slots, 2, m)

        @pl.when(m >= NB)
        def _():
            vbuf[...] = lp[m - NB, at, :].astype(F32)

        return vbuf[...]

    def l_copy(q, rel, i):
        ps, pe, pm = plane[i]
        cc = core if rel == 0 else other
        return rcopy(ls.at[q, cc, pm], lr.at[q, core * 16 + me], l_send, lm.at[q], (ps, y * 2 + cc, pe))

    def reorder():
        for half in range(2):
            for c in range(2):
                v = jnp.zeros((MSG * FLIGHT, HID), F32)
                for rel in range(4):
                    at = slice(SLOT[rel][c] * ROWS, (SLOT[rel][c] + 1) * ROWS)
                    v = v + dot(pack[rel], hb[half, at, :])
                hp[half, c * MSG * FLIGHT : (c + 1) * MSG * FLIGHT, :] = v.astype(BF16)

    def go_home(q):
        cols = chunk(NB + q)
        v = dot(hp[0], wd[0, :, cols]) + dot(hp[1], wd[1, :, cols])
        ls[q] = v.reshape(2, FLIGHT, MSG, CM).astype(BF16)
        for i in range(16):
            for rel in range(2):
                if (rel, i) != (0, 0):
                    l_copy(q, rel, i).start()
        lr[q, core * 16 + me] = ls[q, core, me]

    def came_home(q):
        most = lr.at[q, pl.ds(0, 31)]
        rcopy(most, most, l_send, lm.at[q], peer).wait_recv()
        for half in range(2):
            got = lr[q, half * 16 : half * 16 + 16].astype(F32).reshape(FLIGHT * MSG, CM).astype(BF16)
            for rel in range(4):
                at = slice(SLOT[rel][half] * ROWS, (SLOT[rel][half] + 1) * ROWS)
                lp[q, at, :] = dot(unpack[rel], got).astype(BF16)

    def b_up(m, k):
        return rcopy(nu.at[m, k], f1.at[m, k], b_send, b_f.at[m], up)

    def b_down(m, k):
        return rcopy(nd.at[m, k], f2.at[m, k], b_send, b_f.at[m], down)

    def b_far_up(m):
        return rcopy(t3.at[0, m], s3.at[0, m], b_send, b_s.at[m], up)

    def b_far_down(m):
        return rcopy(t3.at[1, m], s3.at[1, m], b_send, b_s.at[m], down)

    def independent(m):
        v = rows_of(2, m)
        nd[m, 0] = v[:ROWS].astype(BF16)
        b_down(m, 0).start()
        nu[m, 1] = v[ROWS:].astype(BF16)
        b_up(m, 1).start()

    def ind(q):
        with jax.named_scope("ind"):
            independent(q)

    waiting = list(range(NR + NEAR + 1 - FAR, NR))
    ready = list(range(EARLY, NR + NEAR + 1 - FAR)) + list(range(NR, NC))
    ind(0)
    for q in range(1, FIRST):
        ind(q)
        for j in waiting[: 1 + (q > 2)]:
            with jax.named_scope("w_g3"):
                relay_arrived(j)
            ready.append(j)
        waiting = waiting[1 + (q > 2) :]
        with jax.named_scope("fmf"):
            for j in ready[:2] if len(ready) > 2 else []:
                multiply_far(j)
            if len(ready) > 2:
                ready = ready[2:]
    with jax.named_scope("fmf"):
        for j in waiting:
            relay_arrived(j)
            ready.append(j)
        for j in ready:
            multiply_far(j)
    with jax.named_scope("hf"):
        hidden(near_rows, far_rows, 1)
    with jax.named_scope("w_hf"):
        h_copy(near_rows, far_rows, 1, other).wait_recv()

    def r_copy(m, rel, i):
        ps, pe, pm = plane[i]
        cc = core if rel == 0 else other
        return rcopy(rsend.at[m, cc, pm], rrecv.at[m, core * 16 + me], r_send.at[rel], r_recv.at[m], (ps, y * 2 + cc, pe))

    def last(q):
        for half in range(2):
            v = hr[q, half]
            cols = pl.ds(pl.multiple_of(half * HALF + (NB + q) * CM, 128), CM)
            out_ref[:, cols] = (dot(khi[...], v) + dot(klo[...], v)).astype(BF16)

    def backward(i, carry):
        @stage((i >= NB) & (i < NM), "homew")
        def _():
            came_home(i - NB)

        @stage(i < NM, "bt")
        def _():
            m = i
            v = rows_of(6, m)
            t3[0, m] = v[:ROWS].astype(BF16)
            t3[1, m] = v[ROWS:].astype(BF16)
            b_far_up(m).start()
            b_far_down(m).start()

        @stage((lax.rem(i, 2) == 1) & (i < 2 * (NB - FIRST)), "bi")
        def _():
            independent(FIRST + lax.div(i, 2))

        @stage(i == 1, "home")
        def _():
            reorder()

        @stage((i >= 1) & (i <= NL), "home")
        def _():
            go_home(i - 1)

        @stage((i >= NB + LEAD) & (i < NM + LEAD), "bi")
        def _():
            independent(i - LEAD)

        @stage((i >= LEAD) & (i < NM + LEAD), "bb")
        def _():
            m = i - LEAD
            v = rows_of(4, m)
            with jax.named_scope("w_s"):
                rcopy(nu.at[m], nu.at[m], b_send, b_s.at[m], peer).wait_recv()
            nu[m, 0] = (v[ROWS:] + s3[0, m].astype(F32)).astype(BF16)
            b_up(m, 0).start()
            nd[m, 1] = (v[:ROWS] + s3[1, m].astype(F32)).astype(BF16)
            b_down(m, 1).start()

        @stage(i == LEAD - 1, "stat")
        def _():
            statistics_next()

        @stage((i >= LEAD + SUM) & (i < NM + LEAD + SUM), "bc")
        def _():
            m = i - LEAD - SUM
            v = rows_of(0, m)
            with jax.named_scope("w_f"):
                four = nu.at[pl.ds(0, 2)]
                rcopy(four, four, b_send, b_f.at[m], peer).wait_recv()
            r = [
                (v[c * ROWS : (c + 1) * ROWS] + f1[m, c].astype(F32) + f2[m, c].astype(F32)).astype(BF16)
                for c in range(2)
            ]

            @pl.when(m < NB)
            def _():
                for c in range(2):
                    rsend[m, c] = dot(exd[...], r[c]).reshape(FLIGHT, PAD, CM).astype(BF16)
                for i2 in range(16):
                    for rel in range(2):
                        if (rel, i2) != (0, 0):
                            r_copy(m, rel, i2).start()
                rrecv[m, core * 16 + me] = rsend[m, core, me]

            @pl.when(m >= NB)
            def _():
                for c in range(2):
                    hr[m - NB, c] = r[c]

        @stage((i >= NB + LEAD + SUM + 1) & (i < NM + LEAD + SUM), "last")
        def _():
            last(i - NB - LEAD - SUM - 1)

        @stage((i >= LEAD + BACK) & (i < NB + LEAD + BACK), "br")
        def _():
            m = i - LEAD - BACK
            with jax.named_scope("w_r"):
                most = rrecv.at[m, pl.ds(0, 31)]
                rcopy(most, most, r_send.at[0], r_recv.at[m], peer).wait_recv()
            for half in range(2):
                v = rrecv[m, half * 16 : half * 16 + 16].astype(F32).reshape(TOKS, CM).astype(BF16)
                cols = pl.ds(pl.multiple_of(half * HALF + m * CM, 128), CM)
                out_ref[:, cols] = dot(both[...], jnp.concatenate([v, v], axis=0)).astype(BF16)

        return carry

    lax.fori_loop(0, max(NB + LEAD + BACK, NM + LEAD + SUM), backward, 0)

    last(NL - 1)

    with jax.named_scope("fin"):
        all_b.wait_recv()
        tot = stb[0] + stb[1] + stb[2] + stb[3]
        bal_ref[...] = tot[1:2, :] * (EXPERTS / (TOP * LENGTH)) * (tot[0:1, :] / LENGTH) * EXPERTS

        wdx.wait_send()
        h_copy(0, near_rows, 0, core).wait_send()
        h_copy(near_rows, far_rows, 1, core).wait_send()
        all_a.wait_send()
        all_b.wait_send()

        def left_(src, sem):
            rcopy(src, src, sem, r_recv.at[0], peer).wait_send()

        left_(asend.at[:, pl.ds(0, 15)], a_send)
        left_(xb.at[pl.ds(0, NR // 2), pl.ds(0, 6)], g_send.at[0])
        left_(xb.at[:, pl.ds(0, 4)], g_send.at[1])
        left_(yb.at[:, pl.ds(0, 3)], y_send.at[0])
        left_(ys.at[:, pl.ds(0, 15)], y_send.at[1])
        left_(xb.at[pl.ds(0, NM // 2), pl.ds(0, 6)], b_send)
        left_(lr.at[:, pl.ds(0, 31)], l_send)
        left_(rsend.at[:, 0, pl.ds(0, 15)], r_send.at[0])
        left_(rsend.at[:, 0], r_send.at[1])


def put_out(out_v, bal_v, out_h, bal_h, sem):
    parts = [pl.ds(k * 16, 16) for k in range(TOKS // 16)]
    copies = [pltpu.make_async_copy(out_v.at[p], out_h.at[p], sem.at[k]) for k, p in enumerate(parts)]
    copies.append(pltpu.make_async_copy(bal_v, bal_h, sem.at[len(parts)]))
    for cp in copies:
        cp.start()
    for cp in copies:
        cp.wait()


def on_device(tokens, routing, router_weight, w_gate, w_up, w_down):
    hbm = pl.BlockSpec(memory_space=pltpu.HBM)
    vmem = pl.BlockSpec(memory_space=pltpu.VMEM)
    V = pltpu.VMEM
    dma = pltpu.SemaphoreType.DMA
    out, bal = pl.pallas_call(
        kernel,
        out_shape=(
            jax.ShapeDtypeStruct((TOKS, D), BF16),
            jax.ShapeDtypeStruct((1, EXPERTS), F32),
        ),
        in_specs=[hbm, vmem, hbm, hbm, hbm, hbm],
        out_specs=(vmem, vmem),
        scratch_shapes=[
            V((TOKS, D), BF16),
            V((D, EXPERTS), BF16),
            V((D, HID), BF16),
            V((D, HID), BF16),
            V((2, HID, HALF), BF16),
            V((TOKS, TOKS), BF16),
            V((ROWS, TOKS), BF16),
            V((TOKS, ROWS), BF16),
            V((4, MSG * FLIGHT, ROWS), BF16),
            V((4, ROWS, MSG * FLIGHT), BF16),
            V((NP, 4, ROWS, C), BF16),
            V((NP, FLIGHT, MSG, C), BF16),
            V((NP, FLIGHT, MSG, C), BF16),
            V((TOKS, TOKS), BF16),
            V((TOKS, 2 * TOKS), BF16),
            V((TOKS, EXPERTS), F32),
            V((NR, FLIGHT, PAD, C), BF16),
            V((NR, FLIGHT, PAD, C), BF16),
            V((NC, 8, ROWS, C), BF16),
            V((8 * ROWS, HID), F32),
            V((8 * ROWS, HID), F32),
            V((2, 8 * ROWS, HID), BF16),
            V((2, NM, ROWS, CM), BF16),
            V((2, NM, ROWS, CM), BF16),
            V((NM, 2, ROWS, CM), BF16),
            V((NM, 2, ROWS, CM), BF16),
            V((NM, 2, ROWS, CM), BF16),
            V((NM, 2, ROWS, CM), BF16),
            V((NB, 2, FLIGHT, PAD, CM), BF16),
            V((NB, 2 * FLIGHT, PAD, CM), BF16),
            V((2, 2 * MSG * FLIGHT, HID), BF16),
            V((NL, 2, FLIGHT, MSG, CM), BF16),
            V((NL, 2 * FLIGHT, MSG, CM), BF16),
            V((NL, 8 * ROWS, CM), BF16),
            V((NL, 2, ROWS, CM), BF16),
            V((2 * ROWS, CM), F32),
            V((TOKS, ROWS), BF16),
            V((TOKS, ROWS), BF16),
            V((2, 2, EXPERTS), F32),
            V((32, 2, EXPERTS), F32),
            V((4, 2, EXPERTS), F32),
            dma((5,)),
            dma((2,)),
            dma(()),
            dma((NR,)),
            dma((2,)),
            dma((NR,)),
            dma((NR,)),
            dma((2, NC)),
            dma((2, 2)),
            dma(()),
            dma((NM,)),
            dma((NM,)),
            dma((2,)),
            dma((NB,)),
            dma((2,)),
            dma((2,)),
            dma((2,)),
            dma((NP,)),
            dma((NP,)),
            dma((NP,)),
            dma(()),
            dma((NL,)),
        ],
        compiler_params=pltpu.CompilerParams(
            collective_id=0, has_side_effects=True, vmem_limit_bytes=52 * 1024 * 1024
        ),
    )(tokens[0], routing[0].T, router_weight, w_gate[0], w_up[0], w_down[0])
    out, bal = pl.pallas_call(
        put_out,
        out_shape=(
            jax.ShapeDtypeStruct((TOKS, D), BF16),
            jax.ShapeDtypeStruct((1, EXPERTS), F32),
        ),
        in_specs=[vmem, vmem],
        out_specs=(hbm, hbm),
        scratch_shapes=[dma((TOKS // 16 + 1,))],
        compiler_params=pltpu.CompilerParams(vmem_limit_bytes=8 * 1024 * 1024),
    )(out, bal)
    return out[None], bal


def solution(mesh):
    placed = (
        P("seq", ("ctx", "exp"), None),
        P("seq", ("ctx", "exp"), None),
        P(),
        P(("seq", "exp"), None, "ctx"),
        P(("seq", "exp"), None, "ctx"),
        P(("seq", "exp"), "ctx", None),
    )
    return jax.shard_map(
        on_device,
        mesh=mesh,
        in_specs=placed,
        out_specs=(P("seq", ("ctx", "exp"), None), P("seq", None)),
        check_vma=False,
    )
```

```python
import jax
import jax.numpy as jnp
from jax import lax
from jax.experimental import pallas as pl
from jax.experimental.pallas import tpu as pltpu
from jax.sharding import PartitionSpec as P

MESH = pl.DeviceIdType.MESH
F32 = jnp.float32
BF16 = jnp.bfloat16

TOKS = 128
D = 7168
EXPERTS = 256
TOP = 8
FLIGHT = 16
CAP = 5
PAD = 8
HID = 256
ROWS = FLIGHT * CAP
LENGTH = 8192
HALF = D // 2

NC, C = 14, 512
NM, CM = 14, 256
NR = 12
NP = NC - NR
YPRE = 2
YARR = 0
MSG = 24
AHEAD = 6
NEAR = 3
LAG = 8
FAR = 12
EARLY = 2
NL = 3
NB = NM - NL
FIRST = 7
LEAD = 3
SUM = 3
BACK = 8


SLOT = ((0, 1), (2, 4), (5, 3), (6, 7))


def dot(a, b):
    return jnp.dot(a, b, preferred_element_type=F32)


def iota(shape, dim):
    return lax.broadcasted_iota(jnp.int32, shape, dim)


def stage(cond, name):
    def wrap(body):
        @pl.when(cond)
        def _():
            with jax.named_scope(name):
                body()

    return wrap


def kernel(
    tok_h, routes_ref, rw_h, wg_h, wu_h, wd_h,
    out_ref, bal_ref,
    tok, rw, wg, wu, wd, disp, sel, exd, pack, unpack, yb, ys, yr, ghi, both, logits,
    asend, arecv, xb, accg, accu, hb,
    t3, s3, nu, nd, f1, f2, rsend, rrecv, hp, ls, lr, lp, hr, vbuf, khi, klo,
    sta, str_, stb,
    load_sem, wdx_sem, a_send, a_recv, g_send, g1, g3, gd,
    h_sem, b_send, b_s, b_f, r_send, r_recv, st_send, st_recv, y_send, y1, y3, ym, l_send, lm,
):
    s = lax.axis_index("seq")
    cx = lax.axis_index("ctx")
    ex = lax.axis_index("exp")
    core = lax.rem(cx, 2)
    other = 1 - core
    y = lax.div(cx, 2)
    zh = lax.div(ex, 4)
    xx = lax.rem(ex, 4)
    me = s * 8 + ex

    def at_y(step):
        return (s, lax.rem(y + step, 4) * 2 + core, ex)

    up, down, far = at_y(1), at_y(3), at_y(2)
    peer = (s, y * 2 + other, ex)

    plane = []
    for dx in range(4):
        for dh in range(2):
            for dl in range(2):
                ps = lax.rem(s + dl, 2)
                pe = lax.rem(zh + dh, 2) * 4 + lax.rem(xx + dx, 4)
                plane.append((ps, pe, ps * 8 + pe))

    def rcopy(src, dst, ssem, rsem, dev):
        return pltpu.make_async_remote_copy(
            src_ref=src, dst_ref=dst, send_sem=ssem, recv_sem=rsem, device_id=dev, device_id_type=MESH
        )

    mine = pl.ds(pl.multiple_of(core * HALF, 128), HALF)
    theirs = pl.ds(pl.multiple_of(other * HALF, 128), HALF)
    pairs = [(tok_h, tok), (rw_h, rw), (wg_h, wg), (wu_h, wu), (wd_h.at[:, mine], wd.at[core])]
    loads = [pltpu.make_async_copy(src, dst, load_sem.at[k]) for k, (src, dst) in enumerate(pairs)]
    for cp in loads:
        cp.start()

    barrier = pltpu.get_barrier_semaphore()
    away = sorted(range(16), key=lambda i: -(min(i // 4, 4 - i // 4) + 2 * (i // 2 % 2)))
    friends = [(plane[i][0], y * 2 + c, plane[i][1]) for i in away for c in (other, core) if i or c is other]
    friends += [far, up, down]
    for dev in friends:
        pl.semaphore_signal(barrier, inc=1, device_id=dev, device_id_type=MESH)

    lane = iota((TOKS, TOKS), 1)
    sub = iota((TOKS, TOKS), 0)
    hit = jnp.zeros((TOKS, TOKS), F32)
    for k in range(TOP):
        hit = hit + jnp.where(routes_ref[k : k + 1, :] == (sub >> 3), 1.0, 0.0)
    before = jnp.where(sub < lane, 1.0, 0.0).astype(BF16)
    rank = dot(hit.astype(BF16), before)
    place = jnp.where(rank == (sub & 7).astype(F32), hit, 0.0)
    disp[...] = place.astype(BF16)
    si, sl = iota((ROWS, TOKS), 0), iota((ROWS, TOKS), 1)
    sel[...] = jnp.where((si == (sl >> 3) * CAP + (sl & 7)) & ((sl & 7) < CAP), 1.0, 0.0).astype(BF16)

    with jax.named_scope("w_bar"):
        pl.semaphore_wait(barrier, len(friends))
        loads[0].wait()

    def a_copy(j, i):
        ps, pe, pm = plane[i]
        return rcopy(asend.at[j, pm], arecv.at[j, me], a_send, a_recv.at[j], (ps, cx, pe))

    def dispatch(j):
        cols = pl.ds(pl.multiple_of(j * C, 128), C)
        rows = dot(disp[...], tok[:, cols])
        asend[j] = rows.reshape(FLIGHT, PAD, C).astype(BF16)
        for i in away:
            if i:
                a_copy(j, i).start()
        arecv[j, me] = asend[j, me]

    def dispatch_first(j, carry):
        with jax.named_scope("disp"):
            dispatch(j)
        return carry

    hc = C // 2
    left, right = pl.ds(0, hc), pl.ds(hc, hc)

    def y_near(p, step):
        return rcopy(yb.at[p, 0], yb.at[p, 1 if step == 1 else 2], y_send.at[0], y1.at[p], up if step == 1 else down)

    def y_far(p, step):
        half, rel, dev = (left, 1, up) if step == 1 else (right, 2, down)
        return rcopy(yb.at[p, rel, :, half], yb.at[p, 3, :, half], y_send.at[0], y3.at[p], dev)

    with jax.named_scope("pre"):
        compact = dot(sel[...], disp[...]).astype(BF16)
        for p in range(NP):
            cols = slice((NR + p) * C, (NR + p + 1) * C)
            yb[p, 0] = dot(compact, tok[:, cols]).astype(BF16)
            y_near(p, 1).start()
            y_near(p, 3).start()

    lax.fori_loop(0, AHEAD, dispatch_first, 0)
    wdx = rcopy(wd_h.at[:, theirs], wd.at[core], wdx_sem.at[0], wdx_sem.at[1], peer)
    wdx.start()
    with jax.named_scope("w_wts"):
        for rel in range(4):
            q = iota((MSG * FLIGHT, ROWS), 1)
            q = ((q * 205) >> 10) * (MSG - CAP) + q + CAP * rel
            pack[rel] = jnp.where(q == iota((MSG * FLIGHT, ROWS), 0), 1.0, 0.0).astype(BF16)
            q = iota((ROWS, MSG * FLIGHT), 0)
            q = ((q * 205) >> 10) * (MSG - CAP) + q + CAP * rel
            unpack[rel] = jnp.where(q == iota((ROWS, MSG * FLIGHT), 1), 1.0, 0.0).astype(BF16)
        ei, el = iota((TOKS, ROWS), 1), iota((TOKS, ROWS), 0)
        exd[...] = jnp.where((ei == (el >> 3) * CAP + (el & 7)) & ((el & 7) < CAP), 1.0, 0.0).astype(BF16)
        logits[...] = jnp.zeros_like(logits)
        accg[...] = jnp.zeros_like(accg)
        accu[...] = jnp.zeros_like(accu)
        ghi[...] = disp[...].astype(F32).T.astype(BF16)
        for cp in loads[1:4]:
            cp.wait()

    def y_relay(p):
        two = yb.at[p, pl.ds(0, 2)]
        rcopy(two, two, y_send.at[0], y1.at[p], peer).wait_recv()
        y_far(p, 1).start()
        y_far(p, 3).start()

    with jax.named_scope("w_y1"):
        for p in range(YPRE):
            y_relay(p)

    def y_message(p, i):
        ps, pe, pm = plane[i]
        return rcopy(ys.at[p, pm], yr.at[p, me], y_send.at[1], ym.at[p], (ps, cx, pe))

    def y_messages(p):
        with jax.named_scope("w_y3"):
            rcopy(yb.at[p, 0], yb.at[p, 0], y_send.at[0], y3.at[p], peer).wait_recv()
        v = dot(pack[0], yb[p, 0])
        for rel in range(1, 4):
            v = v + dot(pack[rel], yb[p, rel])
        ys[p] = v.reshape(FLIGHT, MSG, C).astype(BF16)
        for i in range(1, 16):
            y_message(p, i).start()
        yr[p, me] = ys[p, me]
        cols = pl.ds(pl.multiple_of((NR + p) * C, 128), C)
        logits[...] += dot(tok[:, cols], rw[cols, :])

    def y_arrived(p):
        with jax.named_scope("w_ym"):
            most = yr.at[p, pl.ds(0, 15)]
            rcopy(most, most, y_send.at[1], ym.at[p], peer).wait_recv()
        got = yr[p].astype(F32).reshape(FLIGHT * MSG, C).astype(BF16)
        for rel in range(4):
            xb[NR + p, slot(rel, core)] = dot(unpack[rel], got).astype(BF16)
            g_peer(NR + p, rel).start()

    def slot(rel, c):
        return (c, 2 + 2 * c, 5 - 2 * c, 6 + c)[rel]

    def g_own_up(j):
        return rcopy(xb.at[j, core], xb.at[j, slot(1, core)], g_send.at[0], g1.at[j], up)

    def g_own_down(j):
        return rcopy(xb.at[j, core], xb.at[j, slot(2, core)], g_send.at[0], g1.at[j], down)

    def g_far_up(j):
        return rcopy(xb.at[j, slot(1, core), :, left], xb.at[j, 6 + core, :, left], g_send.at[0], g3.at[j], up)

    def g_far_down(j):
        return rcopy(xb.at[j, slot(2, core), :, right], xb.at[j, 6 + core, :, right], g_send.at[0], g3.at[j], down)

    def g_peer(j, rel):
        at = slot(rel, core)
        return rcopy(xb.at[j, at], xb.at[j, at], g_send.at[1], gd.at[rel // 3, j], peer)

    def g_peer_wait(j, rel):
        blocks = xb.at[j, pl.ds(0, 1 if rel == 3 else 3)]
        rcopy(blocks, blocks, g_send.at[1], gd.at[rel // 3, j], peer).wait_recv()

    def multiply(j, rel):
        rows = pl.ds(pl.multiple_of(j * C, 128), C)
        at = slice(rel * 2 * ROWS, (rel + 1) * 2 * ROWS)
        v = xb[j, 2 * rel : 2 * rel + 2].reshape(2 * ROWS, C)
        accg[at, :] += dot(v, wg[rows, :])
        accu[at, :] += dot(v, wu[rows, :])

    def relay(j):
        g_far_up(j).start()
        g_far_down(j).start()

    def relay_arrived(j):
        rcopy(xb.at[j, 0], xb.at[j, 0], g_send.at[0], g3.at[j], peer).wait_recv()
        g_peer(j, 3).start()

    def multiply_near(j):
        with jax.named_scope("w_d"):
            g_peer_wait(j, 0)
        for rel in range(3):
            multiply(j, rel)

    def multiply_far(j):
        g_peer_wait(j, 3)
        multiply(j, 3)

    def st_a(i, rel):
        ps, pe, pm = plane[i]
        cc = core if rel == 0 else other
        return rcopy(sta.at[0], str_.at[core * 16 + me], st_send.at[0], st_recv.at[0], (ps, y * 2 + cc, pe))

    def st_b(dev):
        return rcopy(sta.at[1], stb.at[y], st_send.at[1], st_recv.at[1], dev)

    all_a = rcopy(str_.at[pl.ds(0, 15)], str_.at[pl.ds(0, 15)], st_send.at[0], st_recv.at[0], peer)
    all_b = rcopy(stb.at[pl.ds(0, 3)], stb.at[pl.ds(0, 3)], st_send.at[1], st_recv.at[1], peer)

    def statistics():
        scores = jax.nn.sigmoid(logits[...])
        eye = iota((EXPERTS, TOKS), 0)
        named = jnp.zeros((EXPERTS, TOKS), F32)
        for k in range(TOP):
            named = named + jnp.where(routes_ref[k : k + 1, :] == eye, 1.0, 0.0)
        named = named.T
        affinity = scores / jnp.sum(scores, axis=1, keepdims=True)
        sta[0, 0:1, :] = jnp.sum(affinity, axis=0, keepdims=True)
        sta[0, 1:2, :] = jnp.sum(named, axis=0, keepdims=True)
        total = jnp.sum(jnp.where(named > 0.0, scores, 0.0), axis=1, keepdims=True)
        weights = scores / total * 2.5
        spread = jnp.where(iota((EXPERTS, TOKS), 0) == (iota((EXPERTS, TOKS), 1) >> 3), 1.0, 0.0)
        wide = jnp.dot(weights, spread, preferred_element_type=F32, precision=lax.Precision.HIGHEST)
        g = jnp.where(ghi[...].astype(F32) > 0.0, wide, 0.0)
        hi = g.astype(BF16)
        both[:, :TOKS] = hi
        lo = (g - hi.astype(F32)).astype(BF16)
        both[:, TOKS:] = lo
        khi[...] = dot(hi, exd[...]).astype(BF16)
        klo[...] = dot(lo, exd[...]).astype(BF16)
        for rel in range(2):
            for i in range(0, 16, 2):
                if (rel, i) != (0, 0):
                    st_a(i, rel).start()

    def statistics_next():
        all_a.wait_recv()
        str_[core * 16 + me] = sta[0]
        acc = jnp.zeros((2, EXPERTS), F32)
        for cc in range(2):
            for e in range(8):
                acc = acc + str_[cc * 16 + s * 8 + e]
        sta[1] = acc
        stb[y] = acc
        for dev in (up, down, far):
            st_b(dev).start()

    def gather(i, carry):
        @stage(i + AHEAD < NR, "disp")
        def _():
            dispatch(i + AHEAD)

        @stage(i < NR, "fa")
        def _():
            j = i
            with jax.named_scope("w_a"):
                rcopy(
                    asend.at[j, pl.ds(0, 15)], arecv.at[j, pl.ds(0, 15)], a_send, a_recv.at[j], peer
                ).wait_recv()
            got = arecv[j].astype(F32).reshape(TOKS, C).astype(BF16)
            xb[j, core] = dot(sel[...], got).astype(BF16)
            g_own_up(j).start()
            g_own_down(j).start()
            g_peer(j, 0).start()
            cols = pl.ds(pl.multiple_of(j * C, 128), C)
            logits[...] += dot(tok[:, cols], rw[cols, :])

        @stage(i < NP - YPRE, "w_y1")
        def _():
            y_relay(i + YPRE)

        @stage((i >= LAG) & (i < NR), "ff")
        def _():
            relay(i - LAG)

        @stage((i >= NEAR) & (i < NR + NEAR), "fn")
        def _():
            j = i - NEAR
            with jax.named_scope("w_g1"):
                two = xb.at[j, pl.ds(0, 2)]
                rcopy(two, two, g_send.at[0], g1.at[j], peer).wait_recv()
            g_peer(j, 1).start()
            g_peer(j, 2).start()

        @stage(i == NR, "ff")
        def _():
            for j in range(NR - LAG, NR - NEAR + 1):
                relay(j)

        @stage((i >= NR - AHEAD) & (i < NC - AHEAD), "ymsg")
        def _():
            y_messages(i - NR + AHEAD)

        @stage((i >= NR - YARR) & (i < NC - YARR), "yarr")
        def _():
            y_arrived(i - NR + YARR)

        @stage(i == NR + 1, "stat")
        def _():
            statistics()

        @stage((i > NR) & (i < NR + NEAR), "ff")
        def _():
            relay(i - NEAR)

        @stage((i > NEAR) & (i < NR + NEAR), "fm")
        def _():
            multiply_near(i - NEAR - 1)

        @stage(i == NR + NEAR - 1, "fm")
        def _():
            for j in range(NR, NC):
                multiply_near(j)

        @stage(i == NR + NEAR, "fm")
        def _():
            multiply_near(NR - 1)

        @stage(i >= FAR, "fc")
        def _():
            with jax.named_scope("w_g3"):
                relay_arrived(i - FAR)

        @stage((i > FAR) & (i <= FAR + EARLY), "fmf")
        def _():
            multiply_far(i - FAR - 1)

        return carry

    lax.fori_loop(0, NR + NEAR + 1, gather, 0)

    def hidden(lo, n, k):
        at = pl.ds(lo, n)
        gate = accg[at, :]
        hb[core, at, :] = (gate * jax.nn.sigmoid(gate) * accu[at, :]).astype(BF16)
        h_copy(lo, n, k, core).start()

    def h_copy(lo, n, k, slot):
        at = pl.ds(lo, n)
        return rcopy(hb.at[core, at, :], hb.at[slot, at, :], h_sem.at[0, k], h_sem.at[1, k], peer)

    near_rows, far_rows = 6 * ROWS, 2 * ROWS
    with jax.named_scope("hn"):
        hidden(0, near_rows, 0)
    with jax.named_scope("w_h"):
        loads[4].wait()
        wdx.wait_recv()
        h_copy(0, near_rows, 0, other).wait_recv()

    def chunk(m):
        return pl.ds(pl.multiple_of(m * CM, 128), CM)

    def down_rows(lo, n, m):
        at = slice(lo * ROWS, (lo + n) * ROWS)
        cols = chunk(m)
        return dot(hb[0, at, :], wd[0, :, cols]) + dot(hb[1, at, :], wd[1, :, cols])

    def rows_of(slots, m):
        at = slice(slots * ROWS, (slots + 2) * ROWS)

        @pl.when(m < NB)
        def _():
            vbuf[...] = down_rows(slots, 2, m)

        @pl.when(m >= NB)
        def _():
            vbuf[...] = lp[m - NB, at, :].astype(F32)

        return vbuf[...]

    def l_copy(q, rel, i):
        ps, pe, pm = plane[i]
        cc = core if rel == 0 else other
        return rcopy(ls.at[q, cc, pm], lr.at[q, core * 16 + me], l_send, lm.at[q], (ps, y * 2 + cc, pe))

    def reorder():
        for half in range(2):
            for c in range(2):
                v = jnp.zeros((MSG * FLIGHT, HID), F32)
                for rel in range(4):
                    at = slice(SLOT[rel][c] * ROWS, (SLOT[rel][c] + 1) * ROWS)
                    v = v + dot(pack[rel], hb[half, at, :])
                hp[half, c * MSG * FLIGHT : (c + 1) * MSG * FLIGHT, :] = v.astype(BF16)

    def go_home(q):
        cols = chunk(NB + q)
        v = dot(hp[0], wd[0, :, cols]) + dot(hp[1], wd[1, :, cols])
        ls[q] = v.reshape(2, FLIGHT, MSG, CM).astype(BF16)
        for i in range(16):
            for rel in range(2):
                if (rel, i) != (0, 0):
                    l_copy(q, rel, i).start()
        lr[q, core * 16 + me] = ls[q, core, me]

    def came_home(q):
        most = lr.at[q, pl.ds(0, 31)]
        rcopy(most, most, l_send, lm.at[q], peer).wait_recv()
        for half in range(2):
            got = lr[q, half * 16 : half * 16 + 16].astype(F32).reshape(FLIGHT * MSG, CM).astype(BF16)
            for rel in range(4):
                at = slice(SLOT[rel][half] * ROWS, (SLOT[rel][half] + 1) * ROWS)
                lp[q, at, :] = dot(unpack[rel], got).astype(BF16)

    def b_up(m, k):
        return rcopy(nu.at[m, k], f1.at[m, k], b_send, b_f.at[m], up)

    def b_down(m, k):
        return rcopy(nd.at[m, k], f2.at[m, k], b_send, b_f.at[m], down)

    def b_far_up(m):
        return rcopy(t3.at[0, m], s3.at[0, m], b_send, b_s.at[m], up)

    def b_far_down(m):
        return rcopy(t3.at[1, m], s3.at[1, m], b_send, b_s.at[m], down)

    def independent(m):
        v = rows_of(2, m)
        nd[m, 0] = v[:ROWS].astype(BF16)
        b_down(m, 0).start()
        nu[m, 1] = v[ROWS:].astype(BF16)
        b_up(m, 1).start()

    def ind(q):
        with jax.named_scope("ind"):
            independent(q)

    waiting = list(range(NR + NEAR + 1 - FAR, NR))
    ready = list(range(EARLY, NR + NEAR + 1 - FAR)) + list(range(NR, NC))
    ind(0)
    for q in range(1, FIRST):
        ind(q)
        for j in waiting[: 1 + (q > 2)]:
            with jax.named_scope("w_g3"):
                relay_arrived(j)
            ready.append(j)
        waiting = waiting[1 + (q > 2) :]
        with jax.named_scope("fmf"):
            for j in ready[:2] if len(ready) > 2 else []:
                multiply_far(j)
            if len(ready) > 2:
                ready = ready[2:]
    with jax.named_scope("fmf"):
        for j in waiting:
            relay_arrived(j)
            ready.append(j)
        for j in ready:
            multiply_far(j)
    with jax.named_scope("hf"):
        hidden(near_rows, far_rows, 1)
    with jax.named_scope("w_hf"):
        h_copy(near_rows, far_rows, 1, other).wait_recv()

    def r_copy(m, rel, i):
        ps, pe, pm = plane[i]
        cc = core if rel == 0 else other
        return rcopy(rsend.at[m, cc, pm], rrecv.at[m, core * 16 + me], r_send.at[rel], r_recv.at[m], (ps, y * 2 + cc, pe))

    def last(q):
        for half in range(2):
            v = hr[q, half]
            cols = pl.ds(pl.multiple_of(half * HALF + (NB + q) * CM, 128), CM)
            out_ref[:, cols] = (dot(khi[...], v) + dot(klo[...], v)).astype(BF16)

    def backward(i, carry):
        @stage((i >= NB) & (i < NM), "homew")
        def _():
            came_home(i - NB)

        @stage(i < NM, "bt")
        def _():
            m = i
            v = rows_of(6, m)
            t3[0, m] = v[:ROWS].astype(BF16)
            t3[1, m] = v[ROWS:].astype(BF16)
            b_far_up(m).start()
            b_far_down(m).start()

        @stage((lax.rem(i, 2) == 1) & (i < 2 * (NB - FIRST)), "bi")
        def _():
            independent(FIRST + lax.div(i, 2))

        @stage(i == 1, "home")
        def _():
            reorder()

        @stage((i >= 1) & (i <= NL), "home")
        def _():
            go_home(i - 1)

        @stage((i >= NB + LEAD) & (i < NM + LEAD), "bi")
        def _():
            independent(i - LEAD)

        @stage((i >= LEAD) & (i < NM + LEAD), "bb")
        def _():
            m = i - LEAD
            v = rows_of(4, m)
            with jax.named_scope("w_s"):
                rcopy(nu.at[m], nu.at[m], b_send, b_s.at[m], peer).wait_recv()
            nu[m, 0] = (v[ROWS:] + s3[0, m].astype(F32)).astype(BF16)
            b_up(m, 0).start()
            nd[m, 1] = (v[:ROWS] + s3[1, m].astype(F32)).astype(BF16)
            b_down(m, 1).start()

        @stage(i == LEAD - 1, "stat")
        def _():
            statistics_next()

        @stage((i >= LEAD + SUM) & (i < NM + LEAD + SUM), "bc")
        def _():
            m = i - LEAD - SUM
            v = rows_of(0, m)
            with jax.named_scope("w_f"):
                four = nu.at[pl.ds(0, 2)]
                rcopy(four, four, b_send, b_f.at[m], peer).wait_recv()
            r = [
                (v[c * ROWS : (c + 1) * ROWS] + f1[m, c].astype(F32) + f2[m, c].astype(F32)).astype(BF16)
                for c in range(2)
            ]

            @pl.when(m < NB)
            def _():
                for c in range(2):
                    rsend[m, c] = dot(exd[...], r[c]).reshape(FLIGHT, PAD, CM).astype(BF16)
                for i2 in away:
                    for rel in range(2):
                        if (rel, i2) != (0, 0):
                            r_copy(m, rel, i2).start()
                rrecv[m, core * 16 + me] = rsend[m, core, me]

            @pl.when(m >= NB)
            def _():
                for c in range(2):
                    hr[m - NB, c] = r[c]

        @stage((i >= NB + LEAD + SUM + 1) & (i < NM + LEAD + SUM), "last")
        def _():
            last(i - NB - LEAD - SUM - 1)

        @stage((i >= LEAD + BACK) & (i < NB + LEAD + BACK), "br")
        def _():
            m = i - LEAD - BACK
            with jax.named_scope("w_r"):
                most = rrecv.at[m, pl.ds(0, 31)]
                rcopy(most, most, r_send.at[0], r_recv.at[m], peer).wait_recv()
            for half in range(2):
                v = rrecv[m, half * 16 : half * 16 + 16].astype(F32).reshape(TOKS, CM).astype(BF16)
                cols = pl.ds(pl.multiple_of(half * HALF + m * CM, 128), CM)
                out_ref[:, cols] = dot(both[...], jnp.concatenate([v, v], axis=0)).astype(BF16)

        return carry

    lax.fori_loop(0, max(NB + LEAD + BACK, NM + LEAD + SUM), backward, 0)

    last(NL - 1)

    with jax.named_scope("fin"):
        all_b.wait_recv()
        tot = stb[0] + stb[1] + stb[2] + stb[3]
        bal_ref[...] = tot[1:2, :] * (EXPERTS / (TOP * LENGTH)) * (tot[0:1, :] / LENGTH) * EXPERTS

        wdx.wait_send()
        h_copy(0, near_rows, 0, core).wait_send()
        h_copy(near_rows, far_rows, 1, core).wait_send()
        all_a.wait_send()
        all_b.wait_send()

        def left_(src, sem):
            rcopy(src, src, sem, r_recv.at[0], peer).wait_send()

        left_(asend.at[:, pl.ds(0, 15)], a_send)
        left_(xb.at[pl.ds(0, NR // 2), pl.ds(0, 6)], g_send.at[0])
        left_(xb.at[:, pl.ds(0, 4)], g_send.at[1])
        left_(yb.at[:, pl.ds(0, 3)], y_send.at[0])
        left_(ys.at[:, pl.ds(0, 15)], y_send.at[1])
        left_(xb.at[pl.ds(0, NM // 2), pl.ds(0, 6)], b_send)
        left_(lr.at[:, pl.ds(0, 31)], l_send)
        left_(rsend.at[:, 0, pl.ds(0, 15)], r_send.at[0])
        left_(rsend.at[:, 0], r_send.at[1])


def put_out(out_v, bal_v, out_h, bal_h, sem):
    parts = [pl.ds(k * 16, 16) for k in range(TOKS // 16)]
    copies = [pltpu.make_async_copy(out_v.at[p], out_h.at[p], sem.at[k]) for k, p in enumerate(parts)]
    copies.append(pltpu.make_async_copy(bal_v, bal_h, sem.at[len(parts)]))
    for cp in copies:
        cp.start()
    for cp in copies:
        cp.wait()


def on_device(tokens, routing, router_weight, w_gate, w_up, w_down):
    hbm = pl.BlockSpec(memory_space=pltpu.HBM)
    vmem = pl.BlockSpec(memory_space=pltpu.VMEM)
    V = pltpu.VMEM
    dma = pltpu.SemaphoreType.DMA
    out, bal = pl.pallas_call(
        kernel,
        out_shape=(
            jax.ShapeDtypeStruct((TOKS, D), BF16),
            jax.ShapeDtypeStruct((1, EXPERTS), F32),
        ),
        in_specs=[hbm, vmem, hbm, hbm, hbm, hbm],
        out_specs=(vmem, vmem),
        scratch_shapes=[
            V((TOKS, D), BF16),
            V((D, EXPERTS), BF16),
            V((D, HID), BF16),
            V((D, HID), BF16),
            V((2, HID, HALF), BF16),
            V((TOKS, TOKS), BF16),
            V((ROWS, TOKS), BF16),
            V((TOKS, ROWS), BF16),
            V((4, MSG * FLIGHT, ROWS), BF16),
            V((4, ROWS, MSG * FLIGHT), BF16),
            V((NP, 4, ROWS, C), BF16),
            V((NP, FLIGHT, MSG, C), BF16),
            V((NP, FLIGHT, MSG, C), BF16),
            V((TOKS, TOKS), BF16),
            V((TOKS, 2 * TOKS), BF16),
            V((TOKS, EXPERTS), F32),
            V((NR, FLIGHT, PAD, C), BF16),
            V((NR, FLIGHT, PAD, C), BF16),
            V((NC, 8, ROWS, C), BF16),
            V((8 * ROWS, HID), F32),
            V((8 * ROWS, HID), F32),
            V((2, 8 * ROWS, HID), BF16),
            V((2, NM, ROWS, CM), BF16),
            V((2, NM, ROWS, CM), BF16),
            V((NM, 2, ROWS, CM), BF16),
            V((NM, 2, ROWS, CM), BF16),
            V((NM, 2, ROWS, CM), BF16),
            V((NM, 2, ROWS, CM), BF16),
            V((NB, 2, FLIGHT, PAD, CM), BF16),
            V((NB, 2 * FLIGHT, PAD, CM), BF16),
            V((2, 2 * MSG * FLIGHT, HID), BF16),
            V((NL, 2, FLIGHT, MSG, CM), BF16),
            V((NL, 2 * FLIGHT, MSG, CM), BF16),
            V((NL, 8 * ROWS, CM), BF16),
            V((NL, 2, ROWS, CM), BF16),
            V((2 * ROWS, CM), F32),
            V((TOKS, ROWS), BF16),
            V((TOKS, ROWS), BF16),
            V((2, 2, EXPERTS), F32),
            V((32, 2, EXPERTS), F32),
            V((4, 2, EXPERTS), F32),
            dma((5,)),
            dma((2,)),
            dma(()),
            dma((NR,)),
            dma((2,)),
            dma((NR,)),
            dma((NR,)),
            dma((2, NC)),
            dma((2, 2)),
            dma(()),
            dma((NM,)),
            dma((NM,)),
            dma((2,)),
            dma((NB,)),
            dma((2,)),
            dma((2,)),
            dma((2,)),
            dma((NP,)),
            dma((NP,)),
            dma((NP,)),
            dma(()),
            dma((NL,)),
        ],
        compiler_params=pltpu.CompilerParams(
            collective_id=0, has_side_effects=True, vmem_limit_bytes=52 * 1024 * 1024
        ),
    )(tokens[0], routing[0].T, router_weight, w_gate[0], w_up[0], w_down[0])
    out, bal = pl.pallas_call(
        put_out,
        out_shape=(
            jax.ShapeDtypeStruct((TOKS, D), BF16),
            jax.ShapeDtypeStruct((1, EXPERTS), F32),
        ),
        in_specs=[vmem, vmem],
        out_specs=(hbm, hbm),
        scratch_shapes=[dma((TOKS // 16 + 1,))],
        compiler_params=pltpu.CompilerParams(vmem_limit_bytes=8 * 1024 * 1024),
    )(out, bal)
    return out[None], bal


def solution(mesh):
    placed = (
        P("seq", ("ctx", "exp"), None),
        P("seq", ("ctx", "exp"), None),
        P(),
        P(("seq", "exp"), None, "ctx"),
        P(("seq", "exp"), None, "ctx"),
        P(("seq", "exp"), "ctx", None),
    )
    return jax.shard_map(
        on_device,
        mesh=mesh,
        in_specs=placed,
        out_specs=(P("seq", ("ctx", "exp"), None), P("seq", None)),
        check_vma=False,
    )
```
